32 devices in a mesh: member: 2 (over y), tx: 4 (over z), ty: 4 (over x, core).
Axes of the slice: x: 2, y: 2, z: 4, core: 2. Of those that a mesh axis runs over, the one named last changes fastest.
Arguments:
- tracers: float32 [80, 3, 128, 512], P('member', None, 'tx', 'ty'), parts along dimension 0, may hold values from 0.05 to 2
- velocity: float32 [2, 3, 128, 512], P(None, None, 'tx', 'ty'), may hold values from -0.4 to 0.4
- land_mask: int32 [3, 128, 512], P(None, 'tx', 'ty'), may hold values 0 or 1
- sunlight: float32 [128, 512], P('tx', 'ty'), may hold values from 0.3 to 3
- growth_max: float32 [52], P('member'), parts along dimension 0, may hold values from 0.2 to 1.5
- half_sat: float32 [8, 26], P('member'), parts along dimension 0, may hold values from 0.05 to 1
- light_half: float32 [52], P('member'), parts along dimension 0, may hold values from 0.1 to 1
- graze_max: float32 [20], P('member'), parts along dimension 0, may hold values from 0.2 to 1.5
- graze_half: float32 [20], P('member'), parts along dimension 0, may hold values from 0.2 to 2
- palatable: int32 [20, 26], P('member'), parts along dimension 0, may hold values 0 or 1
- stoichiometry: float32 [4], replicated, may hold values from 0.05 to 1
Outputs:
- updated: float32 [80, 3, 128, 512], P('member', None, 'tx', 'ty'), parts along dimension 0
The draws below stay inside these ranges and needn't reach their ends.
There are 2 independent parts, one for each index of `member`. The reference program is written for one: setup_inputs(seed, part) draws one part's arguments, and reference() takes and returns one part's arrays. A program takes and returns all parts, laid end to end along the dimension named above; an argument that names none is the same for every part. Nothing has to cross between parts.
All inputs are finite; a program needn't handle non-finite values. No bound on the sum of `land_mask` on one device may be relied on, other than what follows from the above.
Results may differ from the reference program's by a relative error of at most 0.000064.
Values sent between devices are 32-bit elements; how exact they have to be, the bound alone decides.
A program may use at most 64 MiB of HBM per device.

```python
import math
import jax
import jax.numpy as jnp
from jax import lax

NNUT = 4
NPHY = 26
NZOO = 10
NR = 3
NTR = 40
NX = 128
NY = 512


def with_ends(entries, rng, least, high):
    dims = entries.shape
    spot = [jax.random.randint(jax.random.fold_in(rng, axis), (), 0, dims[axis]) for axis in range(len(dims))]
    entries = entries.at[tuple(spot)].set(least)
    longest = dims.index(max(dims))
    spot[longest] = (spot[longest] + 1) % dims[longest]
    return entries.at[tuple(spot)].set(high)


def block_scale(own_key, dims, cuts, low, largest):
    loudness = 1.0
    for dim, blocks in cuts:
        steps = jax.random.uniform(jax.random.fold_in(jax.random.fold_in(own_key, 6), dim), (blocks,), jnp.float32, low / len(cuts), largest / len(cuts))
        loudness = loudness * jnp.repeat(jnp.exp(steps), dims[dim] // blocks).reshape((-1,) + (1,) * (len(dims) - 1 - dim))
    return loudness


def setup_inputs(seed: int = 0, part: int = 0) -> dict:
    keys = jax.random.split(jax.random.key(seed), 12)
    own_keys = jax.random.split(jax.random.fold_in(keys[11], part), 12)
    tracers = jnp.clip(jnp.exp(math.log(2.0) - 3.6888794 * jax.random.uniform(own_keys[0], (NTR, NR, NX, NY), jnp.float32) ** block_scale(own_keys[0], (NTR, NR, NX, NY), ((2, 4), (3, 4)), -0.2, 0.2)), 0.05, 2.0)
    velocity = jnp.clip(jax.random.uniform(keys[1], (2, NR, NX, NY), jnp.float32, -0.4, 0.4) * block_scale(keys[1], (2, NR, NX, NY), ((2, 4), (3, 4)), -0.4, 0.0), -0.4, 0.4)
    land_mask = with_ends((jax.random.randint(keys[2], (NR, NX, NY), 0, 5) < 4).astype(jnp.int32), jax.random.fold_in(keys[2], 1), 0, 1)
    sunlight = jnp.clip(jnp.exp(math.log(3.0) - 2.3025851 * jax.random.uniform(keys[3], (NX, NY), jnp.float32) ** block_scale(keys[3], (NX, NY), ((0, 4), (1, 4)), -0.2, 0.2)), 0.3, 3.0)
    growth_max = jnp.clip(jnp.exp(jax.random.uniform(own_keys[4], (NPHY,), jnp.float32, math.log(0.2), math.log(1.5))), 0.2, 1.5)
    half_sat = jnp.clip(jnp.exp(jax.random.uniform(own_keys[5], (NNUT, NPHY), jnp.float32, math.log(0.05), math.log(1.0))), 0.05, 1.0)
    light_half = jnp.clip(jnp.exp(jax.random.uniform(own_keys[6], (NPHY,), jnp.float32, math.log(0.1), math.log(1.0))), 0.1, 1.0)
    graze_max = jnp.clip(jnp.exp(jax.random.uniform(own_keys[7], (NZOO,), jnp.float32, math.log(0.2), math.log(1.5))), 0.2, 1.5)
    graze_half = jnp.clip(jnp.exp(jax.random.uniform(own_keys[8], (NZOO,), jnp.float32, math.log(0.2), math.log(2.0))), 0.2, 2.0)
    palatable = with_ends((jax.random.randint(own_keys[9], (NZOO, NPHY), 0, 2) < 1).astype(jnp.int32), jax.random.fold_in(own_keys[9], 1), 0, 1)
    stoichiometry = jnp.clip(jnp.exp(jax.random.uniform(keys[10], (NNUT,), jnp.float32, math.log(0.05), math.log(1.0))), 0.05, 1.0)
    return dict(tracers=tracers, velocity=velocity, land_mask=land_mask, sunlight=sunlight, growth_max=growth_max, half_sat=half_sat, light_half=light_half, graze_max=graze_max, graze_half=graze_half, palatable=palatable, stoichiometry=stoichiometry)


plankton_mortality = 0.05
grazer_mortality = 0.3
assimilation = 0.3
attenuation = 0.4


def window(values, offset, amount, axis_dim):
    return lax.slice_in_dim(values, offset, offset + amount, axis=axis_dim)


def advect(padded, courant, wet_mask, axis_dim, length):
    face_count = length + 1
    far_left = window(padded, 0, face_count, axis_dim)
    near_left = window(padded, 1, face_count, axis_dim)
    near_right = window(padded, 2, face_count, axis_dim)
    far_right = window(padded, 3, face_count, axis_dim)
    opened = window(wet_mask, 1, face_count, axis_dim) * window(wet_mask, 2, face_count, axis_dim)
    transport = window(courant, 2, face_count, axis_dim) * opened
    face_flux = transport * ((7.0 / 12.0) * (near_left + near_right) - (1.0 / 12.0) * (far_left + far_right))
    face_flux = face_flux + jnp.abs(transport) * (1.0 / 12.0) * (far_right - 3.0 * near_right + 3.0 * near_left - far_left)
    centre = window(padded, 2, length, axis_dim)
    outflow = window(face_flux, 1, length, axis_dim) - window(face_flux, 0, length, axis_dim)
    spread = window(transport, 1, length, axis_dim) - window(transport, 0, length, axis_dim)
    return centre - outflow + centre * spread


def ecology(concentration, irradiance, growth_max, half_sat, light_half, graze_max, graze_half, palatable, stoichiometry):
    nutrients = concentration[:NNUT]
    phytoplankton = concentration[NNUT:NNUT + NPHY]
    zooplankton = concentration[NNUT + NPHY:]
    saturation = nutrients[:, None, :] / (nutrients[:, None, :] + half_sat[:, :, None])
    nutrient_limit = jnp.min(saturation, axis=0)
    light_limit = irradiance[None, :] / (irradiance[None, :] + light_half[:, None])
    growth = growth_max[:, None] * nutrient_limit * light_limit * phytoplankton
    prey_weights = palatable.astype(jnp.float32)
    available = jnp.dot(prey_weights, phytoplankton, precision=lax.Precision.HIGHEST)
    grazing_rate = graze_max[:, None] * zooplankton / (graze_half[:, None] + available)
    grazed = phytoplankton * jnp.dot(prey_weights.T, grazing_rate, precision=lax.Precision.HIGHEST)
    ingested = grazing_rate * available
    plankton_loss = plankton_mortality * phytoplankton
    grazer_loss = grazer_mortality * zooplankton * zooplankton
    phyto_change = growth - grazed - plankton_loss
    grazer_change = assimilation * ingested - grazer_loss
    recycled = jnp.sum(plankton_loss, axis=0) + jnp.sum(grazer_loss, axis=0) + (1.0 - assimilation) * jnp.sum(ingested, axis=0) - jnp.sum(growth, axis=0)
    nutrient_change = stoichiometry[:, None] * recycled[None, :]
    return jnp.concatenate([nutrient_change, phyto_change, grazer_change], axis=0)


def reference(tracers, velocity, land_mask, sunlight, growth_max, half_sat, light_half, graze_max, graze_half, palatable, stoichiometry):
    def pad_along(values):
        return jnp.pad(values, ((0, 0), (0, 0), (2, 2), (0, 0)), mode="wrap")

    def pad_across(values):
        return jnp.pad(values, ((0, 0), (0, 0), (0, 0), (2, 2)))

    def one_layer(layer_index):
        concentration = lax.dynamic_slice_in_dim(tracers, layer_index, 1, 1)
        flow = lax.dynamic_slice_in_dim(velocity, layer_index, 1, 1)
        wet_mask = lax.dynamic_slice_in_dim(land_mask, layer_index, 1, 0).astype(jnp.float32)[None]
        after_along = advect(pad_along(concentration), pad_along(flow[0:1]), pad_along(wet_mask), 2, NX)
        advected = advect(pad_across(after_along), pad_across(flow[1:2]), pad_across(wet_mask), 3, NY)
        depth_factor = jnp.exp(-attenuation * (layer_index.astype(jnp.float32) + 0.5))
        irradiance = (sunlight * depth_factor).reshape(-1)
        tendency = ecology(concentration.reshape(NTR, -1), irradiance, growth_max, half_sat, light_half, graze_max, graze_half, palatable, stoichiometry)
        return advected + wet_mask * tendency.reshape(concentration.shape)

    layers = lax.map(one_layer, jnp.arange(NR, dtype=jnp.int32))
    return jnp.moveaxis(layers[:, :, 0], 0, 1)
```

```python
import functools

import jax
import jax.numpy as jnp
from jax import lax
from jax.experimental import pallas as pl
from jax.experimental.pallas import tpu as pltpu
from jax.sharding import PartitionSpec as P

NNUT = 4
plankton_mortality = 0.05
grazer_mortality = 0.3
assimilation = 0.3
attenuation = 0.4

ROWS = 8
LANES = 128
FIRST = 8
GROUP = 4
PER = LANES // GROUP
BATCH = 8
MESH = pl.DeviceIdType.MESH


def stencil_weights(here, after):
    hp, hm = jnp.maximum(here, 0.0), jnp.minimum(here, 0.0)
    ap, am = jnp.maximum(after, 0.0), jnp.minimum(after, 0.0)
    sixth = 1.0 / 6.0
    return (
        -sixth * hp,
        5.0 * sixth * hp + 2.0 * sixth * hm + sixth * ap,
        1.0 - 4.0 * sixth * hp - sixth * hm + sixth * ap + 4.0 * sixth * am,
        -sixth * hm - 2.0 * sixth * ap - 5.0 * sixth * am,
        sixth * am,
    )


def exchange_kernel(
    dims,
    tracers,
    velocity,
    land_mask,
    sunlight,
    *refs,
):
    sources, (swept, tend, halo), tables, buffers = refs[:7], refs[7:10], refs[10:17], refs[17:]
    growth_max, half_sat, light_half, graze_max, graze_half, palatable, stoichiometry = tables
    (
    pad,
    mask_buf,
    sun_buf,
    send_lo,
    send_hi,
    recv_lo,
    recv_hi,
    pack_in,
    pack_out,
    left_in,
    left_out,
    right_in,
    right_out,
    prey,
    load_sems,
    row_sems,
    col_sems,
    ) = buffers
    count, levels, along, nphy, nzoo = dims
    fields = count + 2
    tiles = along // ROWS
    inner = tiles - 2
    last = FIRST + along - ROWS
    tx_size, ty_size = lax.axis_size("tx"), lax.axis_size("ty")
    tx, ty = lax.axis_index("tx"), lax.axis_index("ty")
    up, down = lax.rem(tx + 1, tx_size), lax.rem(tx + tx_size - 1, tx_size)
    right, left = lax.rem(ty + 1, ty_size), lax.rem(ty + ty_size - 1, ty_size)

    def load(slot, src, dst):
        copy = pltpu.make_async_copy(src, dst, load_sems.at[slot])
        copy.start()
        return copy

    own = pl.ds(0, count)
    loads = [
        load(0, land_mask, mask_buf),
        load(1, velocity.at[0], pad.at[count, :, pl.ds(FIRST, along), :]),
        load(2, tracers.at[:, :, pl.ds(0, ROWS), :], pad.at[own, :, pl.ds(FIRST, ROWS), :]),
        load(3, tracers.at[:, :, pl.ds(along - ROWS, ROWS), :], pad.at[own, :, pl.ds(last, ROWS), :]),
        load(4, tracers.at[:, :, pl.ds(ROWS, along - 2 * ROWS), :],
             pad.at[own, :, pl.ds(FIRST + ROWS, along - 2 * ROWS), :]),
        load(5, velocity.at[1], pad.at[count + 2, :, pl.ds(FIRST, along), :]),
        load(6, sunlight, sun_buf),
    ]
    small = [load(7 + i, src, dst) for i, (src, dst) in enumerate(zip(sources, tables))]

    barrier = pltpu.get_barrier_semaphore()
    for target in ({"tx": up}, {"tx": down}, {"ty": right}, {"ty": left}):
        pl.semaphore_signal(barrier, inc=1, device_id=target, device_id_type=MESH)

    def to_float(z, carry):
        for k in range(nphy):
            prey[z, k] = palatable[z, k].astype(jnp.float32)
        return carry

    for copy in small:
        copy.wait()
    lax.fori_loop(0, nzoo, to_float, 0)

    loads[0].wait()
    pad[count + 1, :, FIRST:FIRST + along, :] = mask_buf[...].astype(jnp.float32)
    for slot in (1, 2, 3):
        loads[slot].wait()
    send_lo[...] = pad[0:fields, :, FIRST:FIRST + 2, :]
    send_hi[...] = pad[0:fields, :, FIRST + along - 2:FIRST + along, :]

    pl.semaphore_wait(barrier, 4)

    def remote(src, dst, sems, slot, target):
        return pltpu.make_async_remote_copy(
            src_ref=src, dst_ref=dst, send_sem=sems.at[slot, 0], recv_sem=sems.at[slot, 1],
            device_id=target, device_id_type=MESH,
        )

    to_down = remote(send_lo, recv_hi, row_sems, 0, {"tx": down})
    to_up = remote(send_hi, recv_lo, row_sems, 1, {"tx": up})
    to_up.start()
    to_down.start()
    for slot in (4, 5, 6):
        loads[slot].wait()

    lane_group = lax.broadcasted_iota(jnp.int32, (ROWS, LANES), 1) // GROUP

    def sweep(level, tile, pack, spot):
        base = FIRST + tile * ROWS

        def at(field, shift):
            return pad[field, level, pl.ds(base + shift, ROWS), :]

        wet = at(count + 1, 0)
        here = at(count, 0) * at(count + 1, -1) * wet
        after = at(count, 1) * wet * at(count + 1, 1)
        weights = stencil_weights(here, after)
        packed = [None] * (-(-fields // PER))
        for begin in range(0, fields, BATCH):
            batch = range(begin, min(begin + BATCH, fields))
            values = []
            for field in batch:
                if field < count:
                    value = at(field, -2) * weights[0]
                    for shift in range(-1, 3):
                        value = value + at(field, shift) * weights[shift + 2]
                elif field == count:
                    value = at(count + 2, 0)
                else:
                    value = wet
                values.append(value)
            for field, value in zip(batch, values):
                group, place = divmod(field, PER)
                turned = pltpu.roll(value, (GROUP * place + 2) % LANES, 1)
                if place == 0:
                    packed[group] = turned
                else:
                    packed[group] = jnp.where(lane_group == place, turned, packed[group])
            for field, value in zip(batch, values):
                swept[field, level, pl.ds(tile * ROWS, ROWS), :] = value
        for group, value in enumerate(packed):
            pack[level, spot, group] = value

    def sides(slot, pack, from_left, from_right):
        to_right = remote(pack, from_left, col_sems, slot, {"ty": right})
        to_left = remote(pack, from_right, col_sems, slot + 1, {"ty": left})
        return to_right, to_left

    has_left, has_right = ty > 0, ty < ty_size - 1

    def start(pair):
        pl.when(has_right)(pair[0].start)
        pl.when(has_left)(pair[1].start)

    def inner_level(level, carry):
        for tile in range(1, tiles - 1):
            sweep(level, tile, pack_in, tile - 1)
        return carry

    lax.fori_loop(0, levels, inner_level, 0)
    early = sides(0, pack_in, left_in, right_in)
    start(early)

    def ecology(level, carry):
        def field(index):
            return pad[index, level, pl.ds(FIRST, along), :]

        wet = field(count + 1)
        depth = jnp.full((along, LANES), -attenuation * (level.astype(jnp.float32) + 0.5), jnp.float32)
        light = sun_buf[...] * jnp.exp(depth)
        inverse = [1.0 / field(j) for j in range(NNUT)]
        recycled = jnp.zeros((along, LANES), jnp.float32)
        for k in range(nphy):
            phyto = field(NNUT + k)
            worst = inverse[0] * half_sat[0, k]
            for j in range(1, NNUT):
                worst = jnp.maximum(worst, inverse[j] * half_sat[j, k])
            growth = growth_max[k] * light * phyto / ((1.0 + worst) * (light + light_half[k]))
            loss = plankton_mortality * phyto
            change = growth - loss
            recycled = recycled - change
            tend[NNUT + k, level] = change
        available = [None] * nzoo
        for k in range(nphy):
            phyto = field(NNUT + k)
            for z in range(nzoo):
                term = prey[z, k] * phyto
                available[z] = term if k == 0 else available[z] + term
        rates = []
        for z in range(nzoo):
            zoo = field(NNUT + nphy + z)
            rate = graze_max[z] * zoo / (graze_half[z] + available[z])
            ingested = rate * available[z]
            loss = grazer_mortality * zoo * zoo
            tend[NNUT + nphy + z, level] = wet * (assimilation * ingested - loss)
            recycled = recycled + loss + (1.0 - assimilation) * ingested
            rates.append(rate)
        for k in range(nphy):
            eaten = prey[0, k] * rates[0]
            for z in range(1, nzoo):
                eaten = eaten + prey[z, k] * rates[z]
            tend[NNUT + k, level] = wet * (tend[NNUT + k, level] - field(NNUT + k) * eaten)
        recycled = wet * recycled
        for j in range(NNUT):
            tend[j, level] = stoichiometry[j] * recycled
        return carry

    lax.fori_loop(0, levels, ecology, 0)

    to_down.wait()
    to_up.wait()
    pad[0:fields, :, FIRST - 2:FIRST, :] = recv_lo[...]
    pad[0:fields, :, FIRST + along:FIRST + along + 2, :] = recv_hi[...]

    def outer_level(level, carry):
        sweep(level, 0, pack_out, 0)
        sweep(level, tiles - 1, pack_out, 1)
        return carry

    lax.fori_loop(0, levels, outer_level, 0)
    late = sides(2, pack_out, left_out, right_out)
    start(late)

    @pl.when(jnp.logical_not(has_left))
    def _():
        left_in[...] = jnp.zeros_like(left_in)
        left_out[...] = jnp.zeros_like(left_out)

    @pl.when(jnp.logical_not(has_right))
    def _():
        right_in[...] = jnp.zeros_like(right_in)
        right_out[...] = jnp.zeros_like(right_out)

    def finish(pair):
        @pl.when(has_right)
        def _():
            pair[0].wait_send()
            pair[1].wait_recv()

        @pl.when(has_left)
        def _():
            pair[1].wait_send()
            pair[0].wait_recv()

    finish(early)
    lane = lax.broadcasted_iota(jnp.int32, (ROWS, LANES), 1)
    from_left = (lane % GROUP) < 2

    def across_level(level, carry):
        for tile in range(1, tiles - 1):
            packs = [
                jnp.where(from_left, left_in[level, tile - 1, g], right_in[level, tile - 1, g])
                for g in range(halo.shape[2])
            ]
            across_tile(count, level, tile, packs, swept, tend, tend)
        return carry

    lax.fori_loop(0, levels, across_level, 0)
    finish(late)
    halo[...] = jnp.where(from_left, left_out[...], right_out[...])


def across_tile(count, level, tile, packs, swept, tend, result):
    lane = lax.broadcasted_iota(jnp.int32, (ROWS, LANES), 1)
    low, high = lane < 2, lane >= LANES - 2
    first, final = lane == 0, lane == LANES - 1
    rows = pl.ds(tile * ROWS, ROWS)

    def parts(field):
        group, place = divmod(field, PER)
        value = swept[field, level, rows, :]
        ends = pltpu.roll(packs[group], (-GROUP * place - 2) % LANES, 1)
        return value, ends

    def below(value, ends):
        return pltpu.roll(jnp.where(final, ends, value), 1, 1)

    def above(value, ends):
        return pltpu.roll(jnp.where(first, ends, value), LANES - 1, 1)

    flow, flow_ends = parts(count)
    wet, wet_ends = parts(count + 1)
    here = flow * below(wet, wet_ends) * wet
    after = above(flow, flow_ends) * wet * above(wet, wet_ends)
    weights = stencil_weights(here, after)
    for begin in range(0, count, BATCH):
        batch = range(begin, min(begin + BATCH, count))
        pairs = [parts(field) for field in batch]
        far_before = [pltpu.roll(jnp.where(high, e, v), 2, 1) for v, e in pairs]
        near_before = [below(v, e) for v, e in pairs]
        near_behind = [above(v, e) for v, e in pairs]
        far_behind = [pltpu.roll(jnp.where(low, e, v), LANES - 2, 1) for v, e in pairs]
        totals = []
        for i, field in enumerate(batch):
            total = tend[field, level, rows, :] + pairs[i][0] * weights[2]
            total = total + far_before[i] * weights[0] + near_before[i] * weights[1]
            total = total + near_behind[i] * weights[3] + far_behind[i] * weights[4]
            totals.append(total)
        for i, field in enumerate(batch):
            result[field, level, rows, :] = totals[i]


def across_kernel(dims, swept, tend, halo, updated, result, sems):
    count, levels, along = dims
    tiles = along // ROWS
    inner = pl.ds(ROWS, along - 2 * ROWS)
    copies = [pltpu.make_async_copy(tend.at[:, :, inner, :], updated.at[:, :, inner, :], sems.at[0])]
    copies[0].start()
    for spot, tile in enumerate((0, tiles - 1)):
        def step(level, carry):
            packs = [halo[level, spot, g] for g in range(halo.shape[2])]
            across_tile(count, level, tile, packs, swept, tend, result)
            return carry

        lax.fori_loop(0, levels, step, 0)
        rows = pl.ds(tile * ROWS, ROWS)
        copy = pltpu.make_async_copy(result.at[:, :, rows, :], updated.at[:, :, rows, :], sems.at[spot + 1])
        copy.start()
        copies.append(copy)
    for copy in copies:
        copy.wait()


def shards(
    tracers,
    velocity,
    land_mask,
    sunlight,
    growth_max,
    half_sat,
    light_half,
    graze_max,
    graze_half,
    palatable,
    stoichiometry,
):
    count, levels, along, across = tracers.shape
    assert across == LANES and along % ROWS == 0 and along >= 3 * ROWS
    nphy, nzoo = growth_max.shape[0], graze_max.shape[0]
    fields = count + 2
    groups = -(-fields // PER)
    tiles = along // ROWS
    f32 = jnp.float32
    any_space = pl.BlockSpec(memory_space=pl.ANY)
    hbm = pl.BlockSpec(memory_space=pltpu.HBM)
    vmem = pl.BlockSpec(memory_space=pltpu.VMEM)
    small = (growth_max, half_sat, light_half, graze_max, graze_half, palatable, stoichiometry)
    inner_shape = (levels, tiles - 2, groups, ROWS, LANES)
    outer_shape = (levels, 2, groups, ROWS, LANES)
    edge = (fields, levels, 2, LANES)
    swept, tend, halo = pl.pallas_call(
        functools.partial(exchange_kernel, (count, levels, along, nphy, nzoo)),
        out_shape=(
            jax.ShapeDtypeStruct((fields, levels, along, across), f32),
            jax.ShapeDtypeStruct(tracers.shape, f32),
            jax.ShapeDtypeStruct(outer_shape, f32),
        ),
        in_specs=[hbm] * 11,
        out_specs=(vmem, vmem, vmem),
        scratch_shapes=[pltpu.SMEM(x.shape, x.dtype) for x in small] + [
            pltpu.VMEM((count + 3, levels, FIRST + along + ROWS, LANES), f32),
            pltpu.VMEM(land_mask.shape, jnp.int32),
            pltpu.VMEM(sunlight.shape, f32),
            pltpu.VMEM(edge, f32),
            pltpu.VMEM(edge, f32),
            pltpu.VMEM(edge, f32),
            pltpu.VMEM(edge, f32),
            pltpu.VMEM(inner_shape, f32),
            pltpu.VMEM(outer_shape, f32),
            pltpu.VMEM(inner_shape, f32),
            pltpu.VMEM(outer_shape, f32),
            pltpu.VMEM(inner_shape, f32),
            pltpu.VMEM(outer_shape, f32),
            pltpu.SMEM(palatable.shape, f32),
            pltpu.SemaphoreType.DMA((14,)),
            pltpu.SemaphoreType.DMA((2, 2)),
            pltpu.SemaphoreType.DMA((4, 2)),
        ],
        compiler_params=pltpu.CompilerParams(
            collective_id=0, has_side_effects=True, vmem_limit_bytes=24 * 2**20
        ),
        name="exchange",
    )(*[
        pltpu.with_memory_space_constraint(x, pltpu.HBM)
        for x in (tracers, velocity, land_mask, sunlight) + small
    ])
    return pl.pallas_call(
        functools.partial(across_kernel, (count, levels, along)),
        out_shape=jax.ShapeDtypeStruct(tracers.shape, f32),
        in_specs=[vmem] * 3,
        out_specs=any_space,
        scratch_shapes=[pltpu.VMEM(tracers.shape, f32), pltpu.SemaphoreType.DMA((3,))],
        compiler_params=pltpu.CompilerParams(vmem_limit_bytes=24 * 2**20),
        name="across",
    )(swept, tend, halo)


def solution(mesh):
    return jax.shard_map(
        shards,
        mesh=mesh,
        in_specs=(
            P("member", None, "tx", "ty"),
            P(None, None, "tx", "ty"),
            P(None, "tx", "ty"),
            P("tx", "ty"),
            P("member"),
            P("member", None),
            P("member"),
            P("member"),
            P("member"),
            P("member", None),
            P(),
        ),
        out_specs=P("member", None, "tx", "ty"),
        check_vma=False,
    )
```

```python
import functools

import jax
import jax.numpy as jnp
from jax import lax
from jax.experimental import pallas as pl
from jax.experimental.pallas import tpu as pltpu
from jax.sharding import PartitionSpec as P

NNUT = 4
plankton_mortality = 0.05
grazer_mortality = 0.3
assimilation = 0.3
attenuation = 0.4

ROWS = 8
LANES = 128
FIRST = 8
GROUP = 4
PER = LANES // GROUP
BATCH = 20
MESH = pl.DeviceIdType.MESH


def stencil_weights(here, after):
    hp, hm = jnp.maximum(here, 0.0), jnp.minimum(here, 0.0)
    ap, am = jnp.maximum(after, 0.0), jnp.minimum(after, 0.0)
    sixth = 1.0 / 6.0
    return (
        -sixth * hp,
        5.0 * sixth * hp + 2.0 * sixth * hm + sixth * ap,
        1.0 - 4.0 * sixth * hp - sixth * hm + sixth * ap + 4.0 * sixth * am,
        -sixth * hm - 2.0 * sixth * ap - 5.0 * sixth * am,
        sixth * am,
    )


def place_of(field):
    return field // PER, PER - 1 - field % PER


def spread(value, lane, dims):
    return jnp.broadcast_to(value[:, lane:lane + 1], dims)


def packed_spread(value, field, quarter):
    start = GROUP * place_of(field)[1]
    parts = [spread(value, start + j, value.shape) for j in range(GROUP)]
    return jnp.where(quarter < 2, jnp.where(quarter == 0, parts[0], parts[1]),
                     jnp.where(quarter == 2, parts[2], parts[3]))


def exchange_kernel(dims, tracers, velocity, land_mask, sunlight, *refs):
    sources, outs, tables, buffers = refs[:7], refs[7:13], refs[13:20], refs[20:]
    result, own, far, base, along_w, across_w = outs
    growth_max, half_sat, light_half, graze_max, graze_half, palatable, stoichiometry = tables
    (
        pad, mask_buf, sun_buf, swept, tend, pack, left_in, right_in, qpad, halo_term, across_buf,
        strips, corner_out, corner_left, corner_right, halo_w, meta_out, meta_in, prey,
        load_sems, own_sems, send_sems, recv_sems,
    ) = buffers
    count, levels, along, nphy, nzoo, stride = dims
    tiles = along // ROWS
    flow_field, wet_field, cross_field = count, count + 1, count + 2
    groups = pack.shape[1]
    tx_size, ty_size = lax.axis_size("tx"), lax.axis_size("ty")
    tx, ty = lax.axis_index("tx"), lax.axis_index("ty")
    up, down = lax.rem(tx + 1, tx_size), lax.rem(tx + tx_size - 1, tx_size)
    right, left = lax.rem(ty + 1, ty_size), lax.rem(ty + ty_size - 1, ty_size)
    has_left, has_right = ty > 0, ty < ty_size - 1
    early = tx == 0

    barrier = pltpu.get_barrier_semaphore()

    def greet(**target):
        pl.semaphore_signal(barrier, inc=1, device_id=target, device_id_type=MESH)

    greet(tx=up)
    greet(tx=down)

    @pl.when(has_right)
    def _():
        greet(ty=right)
        greet(tx=up, ty=right)
        greet(tx=down, ty=right)

    @pl.when(has_left)
    def _():
        greet(ty=left)
        greet(tx=up, ty=left)
        greet(tx=down, ty=left)

    def gather():
        sides = has_left.astype(jnp.int32) + has_right.astype(jnp.int32)
        pl.semaphore_wait(barrier, 2 + 3 * sides)

    def own_copy(edge, level, k):
        row = k if edge == 0 else along - 4 + k
        return pltpu.make_async_copy(
            tracers.at[:, level, row, :], own.at[edge, level, k], own_sems.at[edge, level, k])

    def load(slot, src, dst):
        copy = pltpu.make_async_copy(src, dst, load_sems.at[slot])
        copy.start()
        return copy

    sent = [own_copy(1, level, k) for level in range(levels) for k in (2, 3)]
    sent_down = [own_copy(0, level, k) for level in range(levels) for k in (0, 1)]
    kept = [own_copy(edge, level, k + 2 * (1 - edge)) for edge in range(2) for level in range(levels) for k in range(2)]
    for copy in sent:
        copy.start()
    loads = [
        load(0, land_mask, mask_buf),
        load(1, velocity.at[0], pad.at[flow_field, :, pl.ds(FIRST, along), :]),
    ]
    for copy in sent_down:
        copy.start()
    loads += [
        load(2, tracers, pad.at[pl.ds(0, count), :, pl.ds(FIRST, along), :]),
        load(3, velocity.at[1], pad.at[cross_field, :, pl.ds(FIRST, along), :]),
        load(4, sunlight, sun_buf),
    ]
    small = [load(5 + i, src, dst) for i, (src, dst) in enumerate(zip(sources, tables))]
    for copy in kept:
        copy.start()

    def remote(slot, src, dst, **target):
        return pltpu.make_async_remote_copy(
            src_ref=src, dst_ref=dst, send_sem=send_sems.at[slot], recv_sem=recv_sems.at[slot],
            device_id=target, device_id_type=MESH)

    up_rows = remote(0, own.at[1, :, pl.ds(2, 2)], far.at[0], tx=up)
    down_rows = remote(1, own.at[0, :, pl.ds(0, 2)], far.at[1], tx=down)
    up_meta = remote(2, meta_out.at[1], meta_in.at[0], tx=up)
    down_meta = remote(3, meta_out.at[0], meta_in.at[1], tx=down)
    to_right = [
        remote(4, corner_out.at[1], corner_left.at[0], tx=up, ty=right),
        remote(5, corner_out.at[0], corner_left.at[1], tx=down, ty=right),
        remote(6, pack, left_in, ty=right),
    ]
    to_left = [
        remote(7, corner_out.at[1], corner_right.at[0], tx=up, ty=left),
        remote(8, corner_out.at[0], corner_right.at[1], tx=down, ty=left),
        remote(9, pack, right_in, ty=left),
    ]

    def first_sends():
        gather()
        up_rows.start()
        up_meta.start()
        down_meta.start()

    def last_sends():
        @pl.when(has_left)
        def _():
            for copy in to_left:
                copy.start()

        @pl.when(has_right)
        def _():
            for copy in to_right:
                copy.start()

        down_rows.start()

    loads[0].wait()
    pad[wet_field, :, FIRST:FIRST + along, :] = mask_buf[...].astype(jnp.float32)
    loads[1].wait()
    for edge, row in enumerate((FIRST, FIRST + along - 2)):
        meta_out[edge, 0] = pad[flow_field, :, row:row + 2, :]
        meta_out[edge, 1] = pad[wet_field, :, row:row + 2, :]
    for copy in sent:
        copy.wait()
    pl.when(jnp.logical_not(early))(first_sends)

    for copy in sent_down:
        copy.wait()
    for slot in (2, 3):
        loads[slot].wait()

    lane = lax.broadcasted_iota(jnp.int32, (ROWS, LANES), 1)
    lane_group = lane // GROUP
    quarter = lane % GROUP

    def pack_level(level, carry):
        for tile in (0, tiles - 1, *range(1, tiles - 1)):
            rows = pl.ds(FIRST + tile * ROWS, ROWS)
            packed = [None] * groups
            for field in range(count + 3):
                group, place = place_of(field)
                turned = pltpu.roll(pad[field, level, rows, :], (GROUP * place + 2) % LANES, 1)
                if packed[group] is None:
                    packed[group] = turned
                else:
                    packed[group] = jnp.where(lane_group == place, turned, packed[group])
            for group, value in enumerate(packed):
                pack[level, group, tile * ROWS:(tile + 1) * ROWS, :] = value
                for edge, edge_tile, row in ((0, 0, 0), (1, tiles - 1, ROWS - 2)):
                    if tile == edge_tile:
                        for r in range(2):
                            corner_out[edge, r, pl.ds(level * groups + group, 1), :] = value[row + r:row + r + 1, :]
        return carry

    lax.fori_loop(0, levels, pack_level, 0)
    pl.when(jnp.logical_not(early))(last_sends)

    def sweep_level(level, carry):
        for tile in range(tiles):
            start = FIRST + tile * ROWS

            def at(field, shift):
                return pad[field, level, pl.ds(start + shift, ROWS), :]

            wet = at(wet_field, 0)
            here = at(flow_field, 0) * at(wet_field, -1) * wet
            after = at(flow_field, 1) * wet * at(wet_field, 1)
            weights = stencil_weights(here, after)
            for begin in range(0, count, 8):
                batch = range(begin, min(begin + 8, count))
                values = []
                for field in batch:
                    value = at(field, -2) * weights[0]
                    for shift in range(-1, 3):
                        value = value + at(field, shift) * weights[shift + 2]
                    values.append(value)
                for field, value in zip(batch, values):
                    swept[field, level, tile * ROWS:(tile + 1) * ROWS, :] = value
        return carry

    lax.fori_loop(0, levels, sweep_level, 0)

    for copy in small:
        copy.wait()
    loads[4].wait()

    def to_float(z, carry):
        for k in range(nphy):
            prey[z, k] = palatable[z, k].astype(jnp.float32)
        return carry

    lax.fori_loop(0, nzoo, to_float, 0)

    def tend_rows(field, level, row=0, size=along):
        return pl.ds(pl.multiple_of(field * stride + level * along + row, ROWS), size)

    def ecology(level, carry):
        @pl.when(jnp.logical_and(early, level == levels - 1))
        def _():
            first_sends()
            last_sends()

        def field(index):
            return pad[index, level, pl.ds(FIRST, along), :]

        wet = field(wet_field)
        depth = jnp.full((along, LANES), -attenuation * (level.astype(jnp.float32) + 0.5), jnp.float32)
        light = sun_buf[...] * jnp.exp(depth)
        inverse = [1.0 / field(j) for j in range(NNUT)]
        recycled = jnp.zeros((along, LANES), jnp.float32)
        for k in range(nphy):
            phyto = field(NNUT + k)
            worst = inverse[0] * half_sat[0, k]
            for j in range(1, NNUT):
                worst = jnp.maximum(worst, inverse[j] * half_sat[j, k])
            growth = growth_max[k] * light * phyto / ((1.0 + worst) * (light + light_half[k]))
            loss = plankton_mortality * phyto
            change = growth - loss
            recycled = recycled - change
            tend[tend_rows(NNUT + k, level), :] = change
        available = [None] * nzoo
        for k in range(nphy):
            phyto = field(NNUT + k)
            for z in range(nzoo):
                term = prey[z, k] * phyto
                available[z] = term if k == 0 else available[z] + term
        rates = []
        for z in range(nzoo):
            zoo = field(NNUT + nphy + z)
            rate = graze_max[z] * zoo / (graze_half[z] + available[z])
            ingested = rate * available[z]
            loss = grazer_mortality * zoo * zoo
            tend[tend_rows(NNUT + nphy + z, level), :] = wet * (assimilation * ingested - loss)
            recycled = recycled + loss + (1.0 - assimilation) * ingested
            rates.append(rate)
        for k in range(nphy):
            eaten = prey[0, k] * rates[0]
            for z in range(1, nzoo):
                eaten = eaten + prey[z, k] * rates[z]
            rows = tend_rows(NNUT + k, level)
            tend[rows, :] = wet * (tend[rows, :] - field(NNUT + k) * eaten)
        recycled = wet * recycled
        for j in range(NNUT):
            tend[tend_rows(j, level), :] = stoichiometry[j] * recycled
        return carry

    lax.fori_loop(0, levels, ecology, 0)

    @pl.when(jnp.logical_not(has_left))
    def _():
        left_in[...] = jnp.zeros_like(left_in)
        corner_left[...] = jnp.zeros_like(corner_left)

    @pl.when(jnp.logical_not(has_right))
    def _():
        right_in[...] = jnp.zeros_like(right_in)
        corner_right[...] = jnp.zeros_like(corner_right)

    def finish(i):
        @pl.when(has_right)
        def _():
            to_right[i].wait_send()
            to_left[i].wait_recv()

        @pl.when(has_left)
        def _():
            to_left[i].wait_send()
            to_right[i].wait_recv()

    finish(2)
    full_lane = lax.broadcasted_iota(jnp.int32, (along, LANES), 1)
    full_quarter = full_lane % GROUP
    full = (along, LANES)
    ends = jnp.logical_or(lane < 2, lane >= LANES - 2)

    def join(from_left, from_right, which):
        return jnp.where(which < 2, pltpu.roll(from_right, LANES - 2, 1), pltpu.roll(from_left, 2, 1))

    def across_level(level, carry):
        middle = pl.ds(FIRST, along)
        joined = []
        for group in range(groups):
            value = join(left_in[level, group], right_in[level, group], full_quarter)
            qpad[group, middle, :] = value
            joined.append(value)
            for k in range(4):
                spot = pl.ds(level * groups + group, 1)
                strips[0, 2 + k, spot, :] = value[k:k + 1, :]
                strips[1, k, spot, :] = value[along - 4 + k:along - 3 + k, :]
        last = joined[groups - 1]
        qpad[groups, middle, :] = packed_spread(last, flow_field, full_quarter)
        qpad[groups + 1, middle, :] = packed_spread(last, wet_field, full_quarter)

        def q(index, shift):
            return qpad[index, pl.ds(FIRST + shift, along), :]

        wet = q(groups + 1, 0)
        here = q(groups, 0) * q(groups + 1, -1) * wet
        after = q(groups, 1) * wet * q(groups + 1, 1)
        weights = stencil_weights(here, after)

        wet_spot = GROUP * place_of(wet_field)[1]
        cross_spot = GROUP * place_of(cross_field)[1]
        cross, wet = pad[cross_field, level, middle, :], pad[wet_field, level, middle, :]
        first, final = full_lane == 0, full_lane == LANES - 1
        wet_below = jnp.where(first, spread(last, wet_spot + 3, full), pltpu.roll(wet, 1, 1))
        wet_above = jnp.where(final, spread(last, wet_spot, full), pltpu.roll(wet, LANES - 1, 1))
        cross_above = jnp.where(final, spread(last, cross_spot, full), pltpu.roll(cross, LANES - 1, 1))
        w = stencil_weights(cross * wet_below * wet, cross_above * wet * wet_above)
        near = jnp.where(full_quarter < 2,
                         jnp.where(full_quarter == 0, spread(w[4], LANES - 2, full), spread(w[4], LANES - 1, full)),
                         jnp.where(full_quarter == 2, spread(w[0], 0, full), spread(w[0], 1, full)))
        next_to = jnp.where(full_quarter == 1, spread(w[3], LANES - 1, full),
                            jnp.where(full_quarter == 2, spread(w[1], 0, full), 0.0))
        masked = (
            jnp.where(full_lane < 2, 0.0, w[0]),
            jnp.where(first, 0.0, w[1]),
            w[2],
            jnp.where(final, 0.0, w[3]),
            jnp.where(full_lane >= LANES - 2, 0.0, w[4]),
        )
        for i, value in enumerate(masked):
            across_buf[i] = value
        for edge, row in ((0, 0), (1, along - 2)):
            for r in range(2):
                for i, value in enumerate(masked):
                    across_w[edge, level, r, i:i + 1, :] = value[row + r:row + r + 1, :]
                for group in range(groups):
                    spot = pl.ds(level * groups + group, 1)
                    halo_w[0, edge, r, spot, :] = near[row + r:row + r + 1, :]
                    halo_w[1, edge, r, spot, :] = next_to[row + r:row + r + 1, :]
        for group in range(groups):
            total = q(group, -2) * weights[0]
            for shift in range(-1, 3):
                total = total + q(group, shift) * weights[shift + 2]
            beside = jnp.where(full_quarter == 1, pltpu.roll(total, 1, 1), pltpu.roll(total, LANES - 1, 1))
            halo_term[group] = near * total + next_to * beside

        for tile in range(tiles):
            rows = slice(tile * ROWS, (tile + 1) * ROWS)
            w = [across_buf[i, rows, :] for i in range(5)]
            terms = [halo_term[group, rows, :] for group in range(groups)]
            for begin in range(0, count, BATCH):
                batch = range(begin, min(begin + BATCH, count))
                totals = []
                for field in batch:
                    group, place = place_of(field)
                    value = swept[field, level, rows, :]
                    total = tend[tend_rows(field, level, tile * ROWS, ROWS), :] + value * w[2]
                    total = total + pltpu.roll(value, 2, 1) * w[0] + pltpu.roll(value, 1, 1) * w[1]
                    total = total + pltpu.roll(value, LANES - 1, 1) * w[3] + pltpu.roll(value, LANES - 2, 1) * w[4]
                    term = pltpu.roll(terms[group], (LANES - 2 - GROUP * place) % LANES, 1)
                    totals.append(total + jnp.where(ends, term, 0.0))
                for field, total in zip(batch, totals):
                    result[field, level, rows, :] = total
        return carry

    lax.fori_loop(0, levels, across_level, 0)

    for copy in kept:
        copy.wait()
    up_meta.wait()
    down_meta.wait()
    pad[wet_field, :, FIRST - 2:FIRST, :] = meta_in[0, 1]
    for i, index in enumerate((flow_field, wet_field)):
        pad[index, :, FIRST + along:FIRST + along + 2, :] = meta_in[1, i]
    for level in range(levels):
        for edge, tile, row in ((0, 0, 0), (1, tiles - 1, ROWS - 2)):
            start = FIRST + tile * ROWS

            def at(index, shift):
                return pad[index, level, start + shift:start + shift + ROWS, :]

            wet = at(wet_field, 0)
            weights = stencil_weights(at(flow_field, 0) * at(wet_field, -1) * wet,
                                      at(flow_field, 1) * wet * at(wet_field, 1))
            for r in range(2):
                for i, value in enumerate(weights):
                    along_w[edge, level, r, i:i + 1, :] = value[row + r:row + r + 1, :]

    finish(0)
    finish(1)
    odd = lax.broadcasted_iota(jnp.int32, (ROWS, LANES), 0) % groups == groups - 1
    for edge in range(2):
        for r in range(2):
            strips[edge, r + 4 * edge] = join(corner_left[edge, r], corner_right[edge, r], quarter)

        def both(value):
            return jnp.where(odd, value, pltpu.roll(value, ROWS - 1, 0))

        strip = [strips[edge, k] for k in range(6)]
        wets = {k: both(packed_spread(strip[k], wet_field, quarter)) for k in range(1, 5)}
        flows = {k: both(packed_spread(strip[k], flow_field, quarter)) for k in range(2, 5)}
        faces = {k: flows[k] * wets[k - 1] * wets[k] for k in range(2, 5)}
        for r in range(2):
            weights = stencil_weights(faces[r + 2], faces[r + 3])
            total = strip[r] * weights[0]
            for shift in range(1, 5):
                total = total + strip[r + shift] * weights[shift]
            beside = jnp.where(quarter == 1, pltpu.roll(total, 1, 1), pltpu.roll(total, LANES - 1, 1))
            term = halo_w[0, edge, r] * total + halo_w[1, edge, r] * beside
            row = r if edge == 0 else along - 2 + r
            for level in range(levels):
                for begin in range(0, count, ROWS):
                    group, inside = divmod(begin, PER)
                    line = jnp.broadcast_to(term[level * groups + group:level * groups + group + 1, :], (ROWS, LANES))
                    line = pltpu.roll(line, 2 + GROUP * inside, 1, stride=GROUP, stride_axis=0)
                    rows = pl.ds(begin * stride + level * along + row, ROWS, stride=stride)
                    base[edge, level, r, begin:begin + ROWS, :] = tend[rows, :] + jnp.where(ends, line, 0.0)

    up_rows.wait()
    down_rows.wait()


def across_kernel(dims, result, own, far, base, along_w, across_w, updated, rows_out, sems):
    count, levels, along = dims
    inner = pl.ds(2, along - 4)
    copies = [pltpu.make_async_copy(result.at[:, :, inner, :], updated.at[:, :, inner, :], sems.at[0])]
    copies[0].start()
    for edge in range(2):
        for level in range(levels):
            near = [own[edge, level, k] for k in range(4)]
            beyond = [far[edge, level, k] for k in range(2)]
            lines = beyond + near if edge == 0 else near + beyond
            for r in range(2):
                along_lines, across_lines = along_w[edge, level, r], across_w[edge, level, r]
                value = lines[r] * along_lines[0:1, :]
                for shift in range(1, 5):
                    value = value + lines[r + shift] * along_lines[shift:shift + 1, :]
                total = base[edge, level, r] + value * across_lines[2:3, :]
                total = total + pltpu.roll(value, 2, 1) * across_lines[0:1, :]
                total = total + pltpu.roll(value, 1, 1) * across_lines[1:2, :]
                total = total + pltpu.roll(value, LANES - 1, 1) * across_lines[3:4, :]
                total = total + pltpu.roll(value, LANES - 2, 1) * across_lines[4:5, :]
                rows_out[edge, level, r] = total
    for edge in range(2):
        for level in range(levels):
            for r in range(2):
                row = r if edge == 0 else along - 2 + r
                copy = pltpu.make_async_copy(
                    rows_out.at[edge, level, r], updated.at[:, level, row, :],
                    sems.at[1 + (edge * levels + level) * 2 + r])
                copy.start()
                copies.append(copy)
    for copy in copies:
        copy.wait()


def shards(
    tracers,
    velocity,
    land_mask,
    sunlight,
    growth_max,
    half_sat,
    light_half,
    graze_max,
    graze_half,
    palatable,
    stoichiometry,
):
    count, levels, along, across = tracers.shape
    nphy, nzoo = growth_max.shape[0], graze_max.shape[0]
    groups = -(-(count + 3) // PER)
    assert across == LANES and along % ROWS == 0 and along >= 2 * ROWS
    assert count % ROWS == 0 and groups == 2 and (count + 2) % PER >= 2 and levels * groups <= ROWS
    f32 = jnp.float32
    any_space = pl.BlockSpec(memory_space=pl.ANY)
    hbm = pl.BlockSpec(memory_space=pltpu.HBM)
    vmem = pl.BlockSpec(memory_space=pltpu.VMEM)
    small = (growth_max, half_sat, light_half, graze_max, graze_half, palatable, stoichiometry)
    stride = levels * along + ROWS
    line = (ROWS, LANES)
    columns = (levels, groups, along, LANES)
    outputs = [
        (count, levels, along, LANES),
        (2, levels, 4, count, LANES),
        (2, levels, 2, count, LANES),
        (2, levels, 2, count, LANES),
        (2, levels, 2) + line,
        (2, levels, 2) + line,
    ]
    prepared = pl.pallas_call(
        functools.partial(exchange_kernel, (count, levels, along, nphy, nzoo, stride)),
        out_shape=tuple(jax.ShapeDtypeStruct(shape, f32) for shape in outputs),
        in_specs=[hbm] * 11,
        out_specs=(vmem,) * len(outputs),
        scratch_shapes=[pltpu.SMEM(x.shape, x.dtype) for x in small] + [
            pltpu.VMEM((count + 3, levels, FIRST + along + ROWS, LANES), f32),
            pltpu.VMEM(land_mask.shape, jnp.int32),
            pltpu.VMEM(sunlight.shape, f32),
            pltpu.VMEM((count, levels, along, LANES), f32),
            pltpu.VMEM((count * stride, LANES), f32),
            pltpu.VMEM(columns, f32),
            pltpu.VMEM(columns, f32),
            pltpu.VMEM(columns, f32),
            pltpu.VMEM((groups + 2, FIRST + along + ROWS, LANES), f32),
            pltpu.VMEM((groups, along, LANES), f32),
            pltpu.VMEM((5, along, LANES), f32),
            pltpu.VMEM((2, 6) + line, f32),
            pltpu.VMEM((2, 2) + line, f32),
            pltpu.VMEM((2, 2) + line, f32),
            pltpu.VMEM((2, 2) + line, f32),
            pltpu.VMEM((2, 2, 2) + line, f32),
            pltpu.VMEM((2, 2, levels, 2, LANES), f32),
            pltpu.VMEM((2, 2, levels, 2, LANES), f32),
            pltpu.SMEM(palatable.shape, f32),
            pltpu.SemaphoreType.DMA((12,)),
            pltpu.SemaphoreType.DMA((2, levels, 4)),
            pltpu.SemaphoreType.DMA((10,)),
            pltpu.SemaphoreType.DMA((10,)),
        ],
        compiler_params=pltpu.CompilerParams(
            collective_id=0, has_side_effects=True, vmem_limit_bytes=32 * 2**20
        ),
        name="exchange",
    )(*[
        pltpu.with_memory_space_constraint(x, pltpu.HBM)
        for x in (tracers, velocity, land_mask, sunlight) + small
    ])
    return pl.pallas_call(
        functools.partial(across_kernel, (count, levels, along)),
        out_shape=jax.ShapeDtypeStruct(tracers.shape, f32),
        in_specs=[vmem] * len(outputs),
        out_specs=any_space,
        scratch_shapes=[
            pltpu.VMEM((2, levels, 2, count, LANES), f32),
            pltpu.SemaphoreType.DMA((1 + 4 * levels,)),
        ],
        compiler_params=pltpu.CompilerParams(vmem_limit_bytes=24 * 2**20),
        name="across",
    )(*prepared)


def solution(mesh):
    return jax.shard_map(
        shards,
        mesh=mesh,
        in_specs=(
            P("member", None, "tx", "ty"),
            P(None, None, "tx", "ty"),
            P(None, "tx", "ty"),
            P("tx", "ty"),
            P("member"),
            P("member", None),
            P("member"),
            P("member"),
            P("member"),
            P("member", None),
            P(),
        ),
        out_specs=P("member", None, "tx", "ty"),
        check_vma=False,
    )
```

```python
import functools

import jax
import jax.numpy as jnp
from jax import lax
from jax.experimental import pallas as pl
from jax.experimental.pallas import tpu as pltpu
from jax.sharding import PartitionSpec as P

NNUT = 4
plankton_mortality = 0.05
grazer_mortality = 0.3
assimilation = 0.3
attenuation = 0.4

ROWS = 8
LANES = 128
FIRST = 8
GROUP = 4
PER = LANES // GROUP
BATCH = 20
MESH = pl.DeviceIdType.MESH


def stencil_weights(here, after):
    hp, hm = jnp.maximum(here, 0.0), jnp.minimum(here, 0.0)
    ap, am = jnp.maximum(after, 0.0), jnp.minimum(after, 0.0)
    sixth = 1.0 / 6.0
    return (
        -sixth * hp,
        5.0 * sixth * hp + 2.0 * sixth * hm + sixth * ap,
        1.0 - 4.0 * sixth * hp - sixth * hm + sixth * ap + 4.0 * sixth * am,
        -sixth * hm - 2.0 * sixth * ap - 5.0 * sixth * am,
        sixth * am,
    )


def place_of(field):
    return field // PER, PER - 1 - field % PER


def spread(value, lane, dims):
    return jnp.broadcast_to(value[:, lane:lane + 1], dims)


def packed_spread(value, field, quarter):
    start = GROUP * place_of(field)[1]
    parts = [spread(value, start + j, value.shape) for j in range(GROUP)]
    return jnp.where(quarter < 2, jnp.where(quarter == 0, parts[0], parts[1]),
                     jnp.where(quarter == 2, parts[2], parts[3]))


def exchange_kernel(dims, tracers, velocity, land_mask, sunlight, *refs):
    sources, outs, tables, buffers = refs[:7], refs[7:13], refs[13:20], refs[20:]
    result, own, far, base, along_w, across_w = outs
    growth_max, half_sat, light_half, graze_max, graze_half, palatable, stoichiometry = tables
    (
        pad, mask_buf, sun_buf, swept, tend, pack, left_in, right_in, qpad, halo_term, across_buf,
        strips, corner_out, corner_left, corner_right, halo_w, meta_out, meta_in, prey,
        load_sems, main_sems, own_sems, send_sems, recv_sems, ready_sems,
    ) = buffers
    count, levels, along, nphy, nzoo, stride = dims
    tiles = along // ROWS
    flow_field, wet_field, cross_field = count, count + 1, count + 2
    groups = pack.shape[1]
    tx_size, ty_size = lax.axis_size("tx"), lax.axis_size("ty")
    tx, ty = lax.axis_index("tx"), lax.axis_index("ty")
    up, down = lax.rem(tx + 1, tx_size), lax.rem(tx + tx_size - 1, tx_size)
    right, left = lax.rem(ty + 1, ty_size), lax.rem(ty + ty_size - 1, ty_size)
    has_left, has_right = ty > 0, ty < ty_size - 1
    at_first, at_last = tx == 0, tx == tx_size - 1

    barrier = pltpu.get_barrier_semaphore()
    TO_RIGHT, TO_UP, TO_UP_SIDES, TO_DOWN, TO_DOWN_SIDES = range(5)

    def tell(sem, **target):
        pl.semaphore_signal(sem, inc=1, device_id=target, device_id_type=MESH)

    def tell_row(row, straight, aslant):
        tell(straight, tx=row)

        @pl.when(has_right)
        def _():
            tell(aslant, tx=row, ty=right)

        @pl.when(has_left)
        def _():
            tell(aslant, tx=row, ty=left)

    @pl.when(has_right)
    def _():
        tell(barrier, ty=right)

    @pl.when(jnp.logical_not(at_last))
    def _():
        tell_row(up, barrier, barrier)

    @pl.when(at_first)
    def _():
        tell_row(down, barrier, barrier)

    lefts, rights = has_left.astype(jnp.int32), has_right.astype(jnp.int32)
    sides = lefts + rights

    def own_copy(edge, level, k):
        row = k if edge == 0 else along - 4 + k
        return pltpu.make_async_copy(
            tracers.at[:, level, row, :], own.at[edge, level, k], own_sems.at[edge, level, k])

    def load(slot, src, dst):
        copy = pltpu.make_async_copy(src, dst, load_sems.at[slot])
        copy.start()
        return copy

    sent = [own_copy(1, level, k) for level in range(levels) for k in (2, 3)]
    sent_down = [own_copy(0, level, k) for level in range(levels) for k in (0, 1)]
    kept = [own_copy(edge, level, k + 2 * (1 - edge)) for edge in range(2) for level in range(levels) for k in range(2)]
    for copy in sent:
        copy.start()
    loads = [
        load(0, land_mask, mask_buf),
        load(1, velocity.at[0], pad.at[flow_field, :, pl.ds(FIRST, along), :]),
    ]
    for copy in sent_down:
        copy.start()
    loads += [
        load(2, velocity.at[1], pad.at[cross_field, :, pl.ds(FIRST, along), :]),
    ]

    def main(level):
        return pltpu.make_async_copy(
            tracers.at[:, level], pad.at[pl.ds(0, count), level, pl.ds(FIRST, along), :], main_sems.at[level])

    for level in range(levels):
        main(level).start()
    loads.append(load(3, sunlight, sun_buf))
    small = [load(4 + i, src, dst) for i, (src, dst) in enumerate(zip(sources, tables))]
    for copy in kept:
        copy.start()

    earlier = lefts + jnp.where(at_first, 0, 1 + sides) + jnp.where(at_last, 1 + sides, 0)

    @pl.when(earlier > 0)
    def _():
        pl.semaphore_wait(barrier, earlier)

    @pl.when(has_left)
    def _():
        tell(ready_sems.at[TO_RIGHT], ty=left)

    @pl.when(jnp.logical_not(at_first))
    def _():
        tell_row(down, ready_sems.at[TO_UP], ready_sems.at[TO_UP_SIDES])

    @pl.when(at_last)
    def _():
        tell_row(up, ready_sems.at[TO_DOWN], ready_sems.at[TO_DOWN_SIDES])

    def remote(slot, src, dst, **target):
        return pltpu.make_async_remote_copy(
            src_ref=src, dst_ref=dst, send_sem=send_sems.at[slot], recv_sem=recv_sems.at[slot],
            device_id=target, device_id_type=MESH)

    up_rows = remote(0, own.at[1, :, pl.ds(2, 2)], far.at[0], tx=up)
    down_rows = remote(1, own.at[0, :, pl.ds(0, 2)], far.at[1], tx=down)
    up_meta = remote(2, meta_out.at[1], meta_in.at[0], tx=up)
    down_meta = remote(3, meta_out.at[0], meta_in.at[1], tx=down)
    to_right = [
        remote(4, corner_out.at[1], corner_left.at[0], tx=up, ty=right),
        remote(5, corner_out.at[0], corner_left.at[1], tx=down, ty=right),
        remote(6, pack, left_in, ty=right),
    ]
    to_left = [
        remote(7, corner_out.at[1], corner_right.at[0], tx=up, ty=left),
        remote(8, corner_out.at[0], corner_right.at[1], tx=down, ty=left),
        remote(9, pack, right_in, ty=left),
    ]

    def start(condition, copies):
        @pl.when(condition)
        def _():
            for copy in copies:
                copy.start()

    def start_sides(edge):
        start(has_right, [to_right[1 - edge]])
        start(has_left, [to_left[1 - edge]])

    for copy in sent:
        copy.wait()
    start(at_last, [up_rows])
    for copy in sent_down:
        copy.wait()
    start(jnp.logical_not(at_first), [down_rows])
    for slot in range(3):
        loads[slot].wait()
    pad[wet_field, :, FIRST:FIRST + along, :] = mask_buf[...].astype(jnp.float32)
    for edge, row in enumerate((FIRST, FIRST + along - 2)):
        meta_out[edge, 0] = pad[flow_field, :, row:row + 2, :]
        meta_out[edge, 1] = pad[wet_field, :, row:row + 2, :]

    lane = lax.broadcasted_iota(jnp.int32, (ROWS, LANES), 1)
    lane_group = lane // GROUP
    quarter = lane % GROUP

    def sweep_level(level, carry):
        main(level).wait()

        @pl.when(jnp.logical_and(jnp.logical_not(at_last), level == min(1, levels - 1)))
        def _():
            pl.semaphore_wait(ready_sems.at[TO_UP], 1)
            up_meta.start()
            up_rows.start()

        for tile in (0, tiles - 1, *range(1, tiles - 1)):
            start_row = FIRST + tile * ROWS

            def at(field, shift):
                return pad[field, level, pl.ds(start_row + shift, ROWS), :]

            wet = at(wet_field, 0)
            here = at(flow_field, 0) * at(wet_field, -1) * wet
            after = at(flow_field, 1) * wet * at(wet_field, 1)
            weights = stencil_weights(here, after)
            packed = [None] * groups
            for begin in range(0, count + 3, 8):
                batch = range(begin, min(begin + 8, count + 3))
                values = []
                for field in batch:
                    if field < count:
                        value = at(field, -2) * weights[0]
                        for shift in range(-1, 3):
                            value = value + at(field, shift) * weights[shift + 2]
                        values.append(value)
                    group, place = place_of(field)
                    turned = pltpu.roll(at(field, 0), (GROUP * place + 2) % LANES, 1)
                    if packed[group] is None:
                        packed[group] = turned
                    else:
                        packed[group] = jnp.where(lane_group == place, turned, packed[group])
                for field, value in zip(batch, values):
                    swept[field, level, tile * ROWS:(tile + 1) * ROWS, :] = value
            for group, value in enumerate(packed):
                pack[level, group, tile * ROWS:(tile + 1) * ROWS, :] = value
                for edge, edge_tile, row in ((0, 0, 0), (1, tiles - 1, ROWS - 2)):
                    if tile == edge_tile:
                        for r in range(2):
                            corner_out[edge, r, pl.ds(level * groups + group, 1), :] = value[row + r:row + r + 1, :]
        return carry

    lax.fori_loop(0, levels, sweep_level, 0)

    @pl.when(at_last)
    def _():
        start_sides(1)
        up_meta.start()

    @pl.when(jnp.logical_not(at_first))
    def _():
        start_sides(0)
        down_meta.start()

    start(has_left, [to_left[2]])

    @pl.when(has_right)
    def _():
        pl.semaphore_wait(ready_sems.at[TO_RIGHT], 1)
        to_right[2].start()


    for copy in small:
        copy.wait()
    loads[3].wait()
    for z in range(nzoo):
        for k in range(nphy):
            prey[z, k] = palatable[z, k].astype(jnp.float32)

    def tend_rows(field, level, row=0, size=along):
        return pl.ds(pl.multiple_of(field * stride + level * along + row, ROWS), size)

    def ecology(level, carry):
        @pl.when(jnp.logical_and(jnp.logical_not(at_last), level == min(1, levels - 1)))
        def _():
            @pl.when(sides > 0)
            def _():
                pl.semaphore_wait(ready_sems.at[TO_UP_SIDES], sides)

            start_sides(1)

        def field(index):
            return pad[index, level, pl.ds(FIRST, along), :]

        wet = field(wet_field)
        depth = jnp.full((along, LANES), -attenuation * (level.astype(jnp.float32) + 0.5), jnp.float32)
        light = sun_buf[...] * jnp.exp(depth)
        inverse = [1.0 / field(j) for j in range(NNUT)]
        recycled = jnp.zeros((along, LANES), jnp.float32)
        for k in range(nphy):
            phyto = field(NNUT + k)
            worst = inverse[0] * half_sat[0, k]
            for j in range(1, NNUT):
                worst = jnp.maximum(worst, inverse[j] * half_sat[j, k])
            growth = growth_max[k] * light * phyto / ((1.0 + worst) * (light + light_half[k]))
            loss = plankton_mortality * phyto
            change = growth - loss
            recycled = recycled - change
            tend[tend_rows(NNUT + k, level), :] = change
        available = [None] * nzoo
        for k in range(nphy):
            phyto = field(NNUT + k)
            for z in range(nzoo):
                term = prey[z, k] * phyto
                available[z] = term if k == 0 else available[z] + term
        rates = []
        for z in range(nzoo):
            zoo = field(NNUT + nphy + z)
            rate = graze_max[z] * zoo / (graze_half[z] + available[z])
            ingested = rate * available[z]
            loss = grazer_mortality * zoo * zoo
            tend[tend_rows(NNUT + nphy + z, level), :] = wet * (assimilation * ingested - loss)
            recycled = recycled + loss + (1.0 - assimilation) * ingested
            rates.append(rate)
        for k in range(nphy):
            eaten = prey[0, k] * rates[0]
            for z in range(1, nzoo):
                eaten = eaten + prey[z, k] * rates[z]
            rows = tend_rows(NNUT + k, level)
            tend[rows, :] = wet * (tend[rows, :] - field(NNUT + k) * eaten)
        recycled = wet * recycled
        for j in range(NNUT):
            tend[tend_rows(j, level), :] = stoichiometry[j] * recycled
        return carry

    lax.fori_loop(0, levels, ecology, 0)

    @pl.when(at_first)
    def _():
        pl.semaphore_wait(ready_sems.at[TO_DOWN], 1)
        down_meta.start()
        down_rows.start()


    @pl.when(jnp.logical_not(has_left))
    def _():
        left_in[...] = jnp.zeros_like(left_in)
        corner_left[...] = jnp.zeros_like(corner_left)

    @pl.when(jnp.logical_not(has_right))
    def _():
        right_in[...] = jnp.zeros_like(right_in)
        corner_right[...] = jnp.zeros_like(corner_right)

    def finish(i):
        @pl.when(has_right)
        def _():
            to_right[i].wait_send()
            to_left[i].wait_recv()

        @pl.when(has_left)
        def _():
            to_left[i].wait_send()
            to_right[i].wait_recv()

    finish(2)
    full_lane = lax.broadcasted_iota(jnp.int32, (along, LANES), 1)
    full_quarter = full_lane % GROUP
    full = (along, LANES)
    ends = jnp.logical_or(lane < 2, lane >= LANES - 2)

    def join(from_left, from_right, which):
        return jnp.where(which < 2, pltpu.roll(from_right, LANES - 2, 1), pltpu.roll(from_left, 2, 1))

    def halo_level(level):
        middle = pl.ds(FIRST, along)
        joined = []
        for group in range(groups):
            value = join(left_in[level, group], right_in[level, group], full_quarter)
            qpad[level, group, middle, :] = value
            joined.append(value)
            for k in range(4):
                spot = slice(level * groups + group, level * groups + group + 1)
                strips[0, 2 + k, spot, :] = value[k:k + 1, :]
                strips[1, k, spot, :] = value[along - 4 + k:along - 3 + k, :]
        last = joined[groups - 1]
        qpad[level, groups, middle, :] = packed_spread(last, flow_field, full_quarter)
        qpad[level, groups + 1, middle, :] = packed_spread(last, wet_field, full_quarter)

        def q(index, shift):
            return qpad[level, index, pl.ds(FIRST + shift, along), :]

        wet = q(groups + 1, 0)
        here = q(groups, 0) * q(groups + 1, -1) * wet
        after = q(groups, 1) * wet * q(groups + 1, 1)
        weights = stencil_weights(here, after)

        wet_spot = GROUP * place_of(wet_field)[1]
        cross_spot = GROUP * place_of(cross_field)[1]
        cross, wet = pad[cross_field, level, middle, :], pad[wet_field, level, middle, :]
        first, final = full_lane == 0, full_lane == LANES - 1
        wet_below = jnp.where(first, spread(last, wet_spot + 3, full), pltpu.roll(wet, 1, 1))
        wet_above = jnp.where(final, spread(last, wet_spot, full), pltpu.roll(wet, LANES - 1, 1))
        cross_above = jnp.where(final, spread(last, cross_spot, full), pltpu.roll(cross, LANES - 1, 1))
        w = stencil_weights(cross * wet_below * wet, cross_above * wet * wet_above)
        near = jnp.where(full_quarter < 2,
                         jnp.where(full_quarter == 0, spread(w[4], LANES - 2, full), spread(w[4], LANES - 1, full)),
                         jnp.where(full_quarter == 2, spread(w[0], 0, full), spread(w[0], 1, full)))
        next_to = jnp.where(full_quarter == 1, spread(w[3], LANES - 1, full),
                            jnp.where(full_quarter == 2, spread(w[1], 0, full), 0.0))
        masked = (
            jnp.where(full_lane < 2, 0.0, w[0]),
            jnp.where(first, 0.0, w[1]),
            w[2],
            jnp.where(final, 0.0, w[3]),
            jnp.where(full_lane >= LANES - 2, 0.0, w[4]),
        )
        for i, value in enumerate(masked):
            across_buf[level, i] = value
        for edge, row in ((0, 0), (1, along - 2)):
            for r in range(2):
                for i, value in enumerate(masked):
                    across_w[edge, level, r, i:i + 1, :] = value[row + r:row + r + 1, :]
                for group in range(groups):
                    spot = slice(level * groups + group, level * groups + group + 1)
                    halo_w[0, edge, r, spot, :] = near[row + r:row + r + 1, :]
                    halo_w[1, edge, r, spot, :] = next_to[row + r:row + r + 1, :]
        for group in range(groups):
            total = q(group, -2) * weights[0]
            for shift in range(-1, 3):
                total = total + q(group, shift) * weights[shift + 2]
            beside = jnp.where(full_quarter == 1, pltpu.roll(total, 1, 1), pltpu.roll(total, LANES - 1, 1))
            halo_term[level, group] = near * total + next_to * beside

    for level in range(levels):
        halo_level(level)

    def across_level(level, carry):
        @pl.when(jnp.logical_and(at_first, level == min(1, levels - 1)))
        def _():
            @pl.when(sides > 0)
            def _():
                pl.semaphore_wait(ready_sems.at[TO_DOWN_SIDES], sides)

            start_sides(0)

        for tile in range(tiles):
            rows = slice(tile * ROWS, (tile + 1) * ROWS)
            w = [across_buf[level, i, rows, :] for i in range(5)]
            terms = [halo_term[level, group, rows, :] for group in range(groups)]
            for begin in range(0, count, BATCH):
                batch = range(begin, min(begin + BATCH, count))
                totals = []
                for field in batch:
                    group, place = place_of(field)
                    value = swept[field, level, rows, :]
                    total = tend[tend_rows(field, level, tile * ROWS, ROWS), :] + value * w[2]
                    total = total + pltpu.roll(value, 2, 1) * w[0] + pltpu.roll(value, 1, 1) * w[1]
                    total = total + pltpu.roll(value, LANES - 1, 1) * w[3] + pltpu.roll(value, LANES - 2, 1) * w[4]
                    term = pltpu.roll(terms[group], (LANES - 2 - GROUP * place) % LANES, 1)
                    totals.append(total + jnp.where(ends, term, 0.0))
                for field, total in zip(batch, totals):
                    result[field, level, rows, :] = total
        return carry

    lax.fori_loop(0, levels, across_level, 0)

    for copy in kept:
        copy.wait()
    up_meta.wait()
    down_meta.wait()
    pad[wet_field, :, FIRST - 2:FIRST, :] = meta_in[0, 1]
    for i, index in enumerate((flow_field, wet_field)):
        pad[index, :, FIRST + along:FIRST + along + 2, :] = meta_in[1, i]
    for level in range(levels):
        for edge, tile, row in ((0, 0, 0), (1, tiles - 1, ROWS - 2)):
            start = FIRST + tile * ROWS

            def at(index, shift):
                return pad[index, level, start + shift:start + shift + ROWS, :]

            wet = at(wet_field, 0)
            weights = stencil_weights(at(flow_field, 0) * at(wet_field, -1) * wet,
                                      at(flow_field, 1) * wet * at(wet_field, 1))
            for r in range(2):
                for i, value in enumerate(weights):
                    along_w[edge, level, r, i:i + 1, :] = value[row + r:row + r + 1, :]

    finish(0)
    finish(1)
    odd = lax.broadcasted_iota(jnp.int32, (ROWS, LANES), 0) % groups == groups - 1
    for edge in range(2):
        for r in range(2):
            strips[edge, r + 4 * edge] = join(corner_left[edge, r], corner_right[edge, r], quarter)

        def both(value):
            return jnp.where(odd, value, pltpu.roll(value, ROWS - 1, 0))

        strip = [strips[edge, k] for k in range(6)]
        wets = {k: both(packed_spread(strip[k], wet_field, quarter)) for k in range(1, 5)}
        flows = {k: both(packed_spread(strip[k], flow_field, quarter)) for k in range(2, 5)}
        faces = {k: flows[k] * wets[k - 1] * wets[k] for k in range(2, 5)}
        for r in range(2):
            weights = stencil_weights(faces[r + 2], faces[r + 3])
            total = strip[r] * weights[0]
            for shift in range(1, 5):
                total = total + strip[r + shift] * weights[shift]
            beside = jnp.where(quarter == 1, pltpu.roll(total, 1, 1), pltpu.roll(total, LANES - 1, 1))
            term = halo_w[0, edge, r] * total + halo_w[1, edge, r] * beside
            row = r if edge == 0 else along - 2 + r
            for level in range(levels):
                for begin in range(0, count, ROWS):
                    group, inside = divmod(begin, PER)
                    line = jnp.broadcast_to(term[level * groups + group:level * groups + group + 1, :], (ROWS, LANES))
                    line = pltpu.roll(line, 2 + GROUP * inside, 1, stride=GROUP, stride_axis=0)
                    rows = pl.ds(begin * stride + level * along + row, ROWS, stride=stride)
                    base[edge, level, r, begin:begin + ROWS, :] = tend[rows, :] + jnp.where(ends, line, 0.0)

    up_rows.wait()
    down_rows.wait()


def across_kernel(dims, result, own, far, base, along_w, across_w, updated, rows_out, sems):
    count, levels, along = dims
    inner = pl.ds(2, along - 4)
    copies = [pltpu.make_async_copy(result.at[:, :, inner, :], updated.at[:, :, inner, :], sems.at[0])]
    copies[0].start()
    for edge in range(2):
        for level in range(levels):
            near = [own[edge, level, k] for k in range(4)]
            beyond = [far[edge, level, k] for k in range(2)]
            lines = beyond + near if edge == 0 else near + beyond
            for r in range(2):
                along_lines, across_lines = along_w[edge, level, r], across_w[edge, level, r]
                value = lines[r] * along_lines[0:1, :]
                for shift in range(1, 5):
                    value = value + lines[r + shift] * along_lines[shift:shift + 1, :]
                total = base[edge, level, r] + value * across_lines[2:3, :]
                total = total + pltpu.roll(value, 2, 1) * across_lines[0:1, :]
                total = total + pltpu.roll(value, 1, 1) * across_lines[1:2, :]
                total = total + pltpu.roll(value, LANES - 1, 1) * across_lines[3:4, :]
                total = total + pltpu.roll(value, LANES - 2, 1) * across_lines[4:5, :]
                rows_out[edge, level, r] = total
    for edge in range(2):
        for level in range(levels):
            for r in range(2):
                row = r if edge == 0 else along - 2 + r
                copy = pltpu.make_async_copy(
                    rows_out.at[edge, level, r], updated.at[:, level, row, :],
                    sems.at[1 + (edge * levels + level) * 2 + r])
                copy.start()
                copies.append(copy)
    for copy in copies:
        copy.wait()


def shards(
    tracers,
    velocity,
    land_mask,
    sunlight,
    growth_max,
    half_sat,
    light_half,
    graze_max,
    graze_half,
    palatable,
    stoichiometry,
):
    count, levels, along, across = tracers.shape
    nphy, nzoo = growth_max.shape[0], graze_max.shape[0]
    groups = -(-(count + 3) // PER)
    assert across == LANES and along % ROWS == 0 and along >= 2 * ROWS
    assert count % ROWS == 0 and groups == 2 and (count + 2) % PER >= 2 and levels * groups <= ROWS
    f32 = jnp.float32
    any_space = pl.BlockSpec(memory_space=pl.ANY)
    hbm = pl.BlockSpec(memory_space=pltpu.HBM)
    vmem = pl.BlockSpec(memory_space=pltpu.VMEM)
    small = (growth_max, half_sat, light_half, graze_max, graze_half, palatable, stoichiometry)
    stride = levels * along + ROWS
    line = (ROWS, LANES)
    columns = (levels, groups, along, LANES)
    outputs = [
        (count, levels, along, LANES),
        (2, levels, 4, count, LANES),
        (2, levels, 2, count, LANES),
        (2, levels, 2, count, LANES),
        (2, levels, 2) + line,
        (2, levels, 2) + line,
    ]
    prepared = pl.pallas_call(
        functools.partial(exchange_kernel, (count, levels, along, nphy, nzoo, stride)),
        out_shape=tuple(jax.ShapeDtypeStruct(shape, f32) for shape in outputs),
        in_specs=[hbm] * 11,
        out_specs=(vmem,) * len(outputs),
        scratch_shapes=[pltpu.SMEM(x.shape, x.dtype) for x in small] + [
            pltpu.VMEM((count + 3, levels, FIRST + along + ROWS, LANES), f32),
            pltpu.VMEM(land_mask.shape, jnp.int32),
            pltpu.VMEM(sunlight.shape, f32),
            pltpu.VMEM((count, levels, along, LANES), f32),
            pltpu.VMEM((count * stride, LANES), f32),
            pltpu.VMEM(columns, f32),
            pltpu.VMEM(columns, f32),
            pltpu.VMEM(columns, f32),
            pltpu.VMEM((levels, groups + 2, FIRST + along + ROWS, LANES), f32),
            pltpu.VMEM((levels, groups, along, LANES), f32),
            pltpu.VMEM((levels, 5, along, LANES), f32),
            pltpu.VMEM((2, 6) + line, f32),
            pltpu.VMEM((2, 2) + line, f32),
            pltpu.VMEM((2, 2) + line, f32),
            pltpu.VMEM((2, 2) + line, f32),
            pltpu.VMEM((2, 2, 2) + line, f32),
            pltpu.VMEM((2, 2, levels, 2, LANES), f32),
            pltpu.VMEM((2, 2, levels, 2, LANES), f32),
            pltpu.SMEM(palatable.shape, f32),
            pltpu.SemaphoreType.DMA((11,)),
            pltpu.SemaphoreType.DMA((levels,)),
            pltpu.SemaphoreType.DMA((2, levels, 4)),
            pltpu.SemaphoreType.DMA((10,)),
            pltpu.SemaphoreType.DMA((10,)),
            pltpu.SemaphoreType.REGULAR((5,)),
        ],
        compiler_params=pltpu.CompilerParams(
            collective_id=0, has_side_effects=True, vmem_limit_bytes=32 * 2**20
        ),
        name="exchange",
    )(*[
        pltpu.with_memory_space_constraint(x, pltpu.HBM)
        for x in (tracers, velocity, land_mask, sunlight) + small
    ])
    return pl.pallas_call(
        functools.partial(across_kernel, (count, levels, along)),
        out_shape=jax.ShapeDtypeStruct(tracers.shape, f32),
        in_specs=[vmem] * len(outputs),
        out_specs=any_space,
        scratch_shapes=[
            pltpu.VMEM((2, levels, 2, count, LANES), f32),
            pltpu.SemaphoreType.DMA((1 + 4 * levels,)),
        ],
        compiler_params=pltpu.CompilerParams(vmem_limit_bytes=24 * 2**20),
        name="across",
    )(*prepared)


def solution(mesh):
    return jax.shard_map(
        shards,
        mesh=mesh,
        in_specs=(
            P("member", None, "tx", "ty"),
            P(None, None, "tx", "ty"),
            P(None, "tx", "ty"),
            P("tx", "ty"),
            P("member"),
            P("member", None),
            P("member"),
            P("member"),
            P("member"),
            P("member", None),
            P(),
        ),
        out_specs=P("member", None, "tx", "ty"),
        check_vma=False,
    )
```

```python
import functools

import jax
import jax.numpy as jnp
from jax import lax
from jax.experimental import pallas as pl
from jax.experimental.pallas import tpu as pltpu
from jax.sharding import PartitionSpec as P

NNUT = 4
plankton_mortality = 0.05
grazer_mortality = 0.3
assimilation = 0.3
attenuation = 0.4

ROWS = 8
LANES = 128
FIRST = 8
GROUP = 4
PER = LANES // GROUP
BATCH = 20
MESH = pl.DeviceIdType.MESH


def stencil_weights(here, after):
    hp, hm = jnp.maximum(here, 0.0), jnp.minimum(here, 0.0)
    ap, am = jnp.maximum(after, 0.0), jnp.minimum(after, 0.0)
    sixth = 1.0 / 6.0
    return (
        -sixth * hp,
        5.0 * sixth * hp + 2.0 * sixth * hm + sixth * ap,
        1.0 - 4.0 * sixth * hp - sixth * hm + sixth * ap + 4.0 * sixth * am,
        -sixth * hm - 2.0 * sixth * ap - 5.0 * sixth * am,
        sixth * am,
    )


def place_of(field):
    return field // PER, PER - 1 - field % PER


def spread(value, lane, dims):
    return jnp.broadcast_to(value[:, lane:lane + 1], dims)


def packed_spread(value, field, quarter):
    start = GROUP * place_of(field)[1]
    parts = [spread(value, start + j, value.shape) for j in range(GROUP)]
    return jnp.where(quarter < 2, jnp.where(quarter == 0, parts[0], parts[1]),
                     jnp.where(quarter == 2, parts[2], parts[3]))


def join(from_left, from_right, which):
    return jnp.where(which < 2, pltpu.roll(from_right, LANES - 2, 1), pltpu.roll(from_left, 2, 1))


def exchange_kernel(dims, tracers, velocity, land_mask, sunlight, *refs):
    sources, outs, tables, buffers = refs[:7], refs[7:17], refs[17:24], refs[24:]
    result, own, far, tend, along_w, across_w, strips, corner_left, corner_right, halo_w = outs
    growth_max, half_sat, light_half, graze_max, graze_half, palatable, stoichiometry = tables
    (
        pad, mask_buf, sun_buf, swept, pack, left_in, right_in, qpad, halo_term, across_buf,
        corner_out, meta_out, meta_in, prey, load_sems, main_sems, send_sems, recv_sems, ready_sems,
    ) = buffers
    count, levels, along, nphy, nzoo, stride = dims
    tiles = along // ROWS
    flow_field, wet_field, cross_field = count, count + 1, count + 2
    groups = pack.shape[1]
    tx_size, ty_size = lax.axis_size("tx"), lax.axis_size("ty")
    tx, ty = lax.axis_index("tx"), lax.axis_index("ty")
    up, down = lax.rem(tx + 1, tx_size), lax.rem(tx + tx_size - 1, tx_size)
    right, left = lax.rem(ty + 1, ty_size), lax.rem(ty + ty_size - 1, ty_size)
    has_left, has_right = ty > 0, ty < ty_size - 1
    at_first, at_last = tx == 0, tx == tx_size - 1
    root = jnp.logical_and(at_first, jnp.logical_and(lax.axis_index("member") == 0, ty < 2))
    others = jnp.logical_not(root)

    barrier = pltpu.get_barrier_semaphore()
    TO_RIGHT, TO_UP, TO_UP_SIDES, TO_DOWN, TO_DOWN_SIDES = range(5)

    def tell(sem, **target):
        pl.semaphore_signal(sem, inc=1, device_id=target, device_id_type=MESH)

    def tell_row(row, straight, aslant):
        tell(straight, tx=row)

        @pl.when(has_right)
        def _():
            tell(aslant, tx=row, ty=right)

        @pl.when(has_left)
        def _():
            tell(aslant, tx=row, ty=left)

    @pl.when(has_right)
    def _():
        tell(barrier, ty=right)

    @pl.when(jnp.logical_not(at_last))
    def _():
        tell_row(up, barrier, barrier)

    @pl.when(at_first)
    def _():
        tell_row(down, barrier, barrier)

    lefts, rights = has_left.astype(jnp.int32), has_right.astype(jnp.int32)
    sides = lefts + rights

    OWN_UP, OWN_DOWN, OWN_KEPT, PLANES, SUN, TABLE = range(6)

    def own_copy(slot, edge, level, k):
        row = k if edge == 0 else along - 4 + k
        return pltpu.make_async_copy(tracers.at[:, level, row, :], own.at[edge, level, k], load_sems.at[slot])

    def load(sem, src, dst):
        copy = pltpu.make_async_copy(src, dst, sem)
        copy.start()
        return copy

    def await_load(slot, ref):
        pltpu.make_async_copy(ref, ref, load_sems.at[slot]).wait()

    for level in range(levels):
        for k in (2, 3):
            own_copy(OWN_UP, 1, level, k).start()
    load(load_sems.at[PLANES], land_mask, mask_buf)
    load(load_sems.at[PLANES], velocity.at[0], pad.at[flow_field, :, pl.ds(FIRST, along), :])
    for level in range(levels):
        for k in (0, 1):
            own_copy(OWN_DOWN, 0, level, k).start()
    load(load_sems.at[PLANES], velocity.at[1], pad.at[cross_field, :, pl.ds(FIRST, along), :])

    def main(level):
        return pltpu.make_async_copy(
            tracers.at[:, level], pad.at[pl.ds(0, count), level, pl.ds(FIRST, along), :], main_sems.at[level])

    for level in range(levels):
        main(level).start()
    sun = load(load_sems.at[SUN], sunlight, sun_buf)
    table_sems = [load_sems.at[TABLE + i] for i in range(3)] + [send_sems.at[2 + i] for i in range(4)]
    small = [load(sem, src, dst) for sem, src, dst in zip(table_sems, sources, tables)]
    for level in range(levels):
        for k in range(2):
            own_copy(OWN_KEPT, 0, level, 2 + k).start()
            own_copy(OWN_KEPT, 1, level, k).start()

    earlier = lefts + jnp.where(at_first, 0, 1 + sides) + jnp.where(at_last, 1 + sides, 0)

    @pl.when(earlier > 0)
    def _():
        pl.semaphore_wait(barrier, earlier)

    @pl.when(has_left)
    def _():
        tell(ready_sems.at[TO_RIGHT], ty=left)

    @pl.when(jnp.logical_not(at_first))
    def _():
        tell_row(down, ready_sems.at[TO_UP], ready_sems.at[TO_UP_SIDES])

    @pl.when(at_last)
    def _():
        tell_row(up, ready_sems.at[TO_DOWN], ready_sems.at[TO_DOWN_SIDES])

    def remote(slot, src, dst, **target):
        return pltpu.make_async_remote_copy(
            src_ref=src, dst_ref=dst, send_sem=send_sems.at[slot], recv_sem=recv_sems.at[slot],
            device_id=target, device_id_type=MESH)

    ROW, META, RIGHT_CORNERS, RIGHT_COLUMNS, LEFT_CORNERS, LEFT_COLUMNS = range(6)
    up_rows = remote(ROW, own.at[1, :, pl.ds(2, 2)], far.at[0], tx=up)
    down_rows = remote(ROW, own.at[0, :, pl.ds(0, 2)], far.at[1], tx=down)
    up_meta = remote(META, meta_out.at[1], meta_in.at[0], tx=up)
    down_meta = remote(META, meta_out.at[0], meta_in.at[1], tx=down)
    to_right = [
        remote(RIGHT_CORNERS, corner_out.at[1], corner_left.at[0], tx=up, ty=right),
        remote(RIGHT_CORNERS, corner_out.at[0], corner_left.at[1], tx=down, ty=right),
        remote(RIGHT_COLUMNS, pack, left_in, ty=right),
    ]
    to_left = [
        remote(LEFT_CORNERS, corner_out.at[1], corner_right.at[0], tx=up, ty=left),
        remote(LEFT_CORNERS, corner_out.at[0], corner_right.at[1], tx=down, ty=left),
        remote(LEFT_COLUMNS, pack, right_in, ty=left),
    ]
    both_rows = remote(ROW, far, far, tx=up)
    both_metas = remote(META, meta_in, meta_in, tx=up)
    right_corners = remote(RIGHT_CORNERS, corner_left, corner_left, tx=up)
    left_corners = remote(LEFT_CORNERS, corner_right, corner_right, tx=up)

    def start(condition, copies):
        @pl.when(condition)
        def _():
            for copy in copies:
                copy.start()

    def start_sides(edge):
        start(has_right, [to_right[1 - edge]])
        start(has_left, [to_left[1 - edge]])

    await_load(OWN_UP, own.at[1, :, pl.ds(2, 2)])
    odd_core = lax.rem(ty, 2) == 1
    start(jnp.logical_and(at_last, jnp.logical_not(odd_core)), [up_rows])
    await_load(OWN_DOWN, own.at[0, :, pl.ds(0, 2)])
    await_load(PLANES, pad.at[pl.ds(count, 3), :, pl.ds(FIRST, along), :])
    pad[wet_field, :, FIRST:FIRST + along, :] = mask_buf[...].astype(jnp.float32)
    for edge, row in enumerate((FIRST, FIRST + along - 2)):
        meta_out[edge, 0] = pad[flow_field, :, row:row + 2, :]
        meta_out[edge, 1] = pad[wet_field, :, row:row + 2, :]
    start(at_last, [up_meta, down_meta])
    middle = jnp.logical_not(jnp.logical_or(at_first, at_last))
    start(middle, [down_meta, down_rows])

    lane = lax.broadcasted_iota(jnp.int32, (ROWS, LANES), 1)
    lane_group = lane // GROUP
    quarter = lane % GROUP

    def sweep_level(level, carry):
        main(level).wait()

        for tile in (0, tiles - 1, *range(1, tiles - 1)):
            start_row = FIRST + tile * ROWS

            def at(field, shift):
                return pad[field, level, pl.ds(start_row + shift, ROWS), :]

            wet = at(wet_field, 0)
            here = at(flow_field, 0) * at(wet_field, -1) * wet
            after = at(flow_field, 1) * wet * at(wet_field, 1)
            weights = stencil_weights(here, after)
            packed = [None] * groups
            for begin in range(0, count + 3, 8):
                batch = range(begin, min(begin + 8, count + 3))
                values = []
                for field in batch:
                    if field < count:
                        value = at(field, -2) * weights[0]
                        for shift in range(-1, 3):
                            value = value + at(field, shift) * weights[shift + 2]
                        values.append(value)
                    group, place = place_of(field)
                    turned = pltpu.roll(at(field, 0), (GROUP * place + 2) % LANES, 1)
                    if packed[group] is None:
                        packed[group] = turned
                    else:
                        packed[group] = jnp.where(lane_group == place, turned, packed[group])
                for field, value in zip(batch, values):
                    swept[field, level, tile * ROWS:(tile + 1) * ROWS, :] = value
            for group, value in enumerate(packed):
                pack[level, group, tile * ROWS:(tile + 1) * ROWS, :] = value
                for edge, edge_tile, row in ((0, 0, 0), (1, tiles - 1, ROWS - 2)):
                    if tile == edge_tile:
                        for r in range(2):
                            corner_out[edge, r, pl.ds(level * groups + group, 1), :] = value[row + r:row + r + 1, :]
        return carry

    lax.fori_loop(0, levels, sweep_level, 0)
    for copy in small:
        copy.wait()
    sun.wait()

    def send_up():
        pl.semaphore_wait(ready_sems.at[TO_UP], 1)
        up_meta.start()
        up_rows.start()

    def send_down():
        pl.semaphore_wait(ready_sems.at[TO_DOWN], 1)
        down_meta.start()
        down_rows.start()

    pl.when(at_last)(lambda: start_sides(1))
    pl.when(jnp.logical_not(at_first))(lambda: start_sides(0))
    start(has_left, [to_left[2]])
    start(jnp.logical_and(at_last, odd_core), [up_rows])
    start(at_last, [down_rows])
    pl.when(jnp.logical_and(others, jnp.logical_not(at_last)))(send_up)

    @pl.when(has_right)
    def _():
        pl.semaphore_wait(ready_sems.at[TO_RIGHT], 1)
        to_right[2].start()


    for z in range(nzoo):
        for k in range(nphy):
            prey[z, k] = palatable[z, k].astype(jnp.float32)

    def tend_rows(field, level, row=0, size=along):
        return pl.ds(pl.multiple_of(field * stride + level * along + row, ROWS), size)

    def ecology(level, carry):
        second = level == min(1, levels - 1)
        pl.when(jnp.logical_and(root, second))(send_up)
        pl.when(jnp.logical_and(jnp.logical_and(at_first, others), second))(send_down)

        @pl.when(jnp.logical_and(jnp.logical_not(at_last), second))
        def _():
            @pl.when(sides > 0)
            def _():
                pl.semaphore_wait(ready_sems.at[TO_UP_SIDES], sides)

            start_sides(1)

        def field(index):
            return pad[index, level, pl.ds(FIRST, along), :]

        wet = field(wet_field)
        depth = jnp.full((along, LANES), -attenuation * (level.astype(jnp.float32) + 0.5), jnp.float32)
        light = sun_buf[...] * jnp.exp(depth)
        inverse = [1.0 / field(j) for j in range(NNUT)]
        recycled = jnp.zeros((along, LANES), jnp.float32)
        for k in range(nphy):
            phyto = field(NNUT + k)
            worst = inverse[0] * half_sat[0, k]
            for j in range(1, NNUT):
                worst = jnp.maximum(worst, inverse[j] * half_sat[j, k])
            growth = growth_max[k] * light * phyto / ((1.0 + worst) * (light + light_half[k]))
            loss = plankton_mortality * phyto
            change = growth - loss
            recycled = recycled - change
            tend[tend_rows(NNUT + k, level), :] = change
        available = [None] * nzoo
        for k in range(nphy):
            phyto = field(NNUT + k)
            for z in range(nzoo):
                term = prey[z, k] * phyto
                available[z] = term if k == 0 else available[z] + term
        rates = []
        for z in range(nzoo):
            zoo = field(NNUT + nphy + z)
            rate = graze_max[z] * zoo / (graze_half[z] + available[z])
            ingested = rate * available[z]
            loss = grazer_mortality * zoo * zoo
            tend[tend_rows(NNUT + nphy + z, level), :] = wet * (assimilation * ingested - loss)
            recycled = recycled + loss + (1.0 - assimilation) * ingested
            rates.append(rate)
        for k in range(nphy):
            eaten = prey[0, k] * rates[0]
            for z in range(1, nzoo):
                eaten = eaten + prey[z, k] * rates[z]
            rows = tend_rows(NNUT + k, level)
            tend[rows, :] = wet * (tend[rows, :] - field(NNUT + k) * eaten)
        recycled = wet * recycled
        for j in range(NNUT):
            tend[tend_rows(j, level), :] = stoichiometry[j] * recycled
        return carry

    lax.fori_loop(0, levels, ecology, 0)
    pl.when(root)(send_down)


    @pl.when(jnp.logical_not(has_left))
    def _():
        left_in[...] = jnp.zeros_like(left_in)
        corner_left[...] = jnp.zeros_like(corner_left)

    @pl.when(jnp.logical_not(has_right))
    def _():
        right_in[...] = jnp.zeros_like(right_in)
        corner_right[...] = jnp.zeros_like(corner_right)

    def finish(to_right, to_left):
        @pl.when(has_right)
        def _():
            to_right.wait_send()
            to_left.wait_recv()

        @pl.when(has_left)
        def _():
            to_left.wait_send()
            to_right.wait_recv()

    finish(to_right[2], to_left[2])
    full_lane = lax.broadcasted_iota(jnp.int32, (along, LANES), 1)
    full_quarter = full_lane % GROUP
    full = (along, LANES)
    ends = jnp.logical_or(lane < 2, lane >= LANES - 2)

    def halo_level(level):
        middle = pl.ds(FIRST, along)
        joined = []
        for group in range(groups):
            value = join(left_in[level, group], right_in[level, group], full_quarter)
            qpad[level, group, middle, :] = value
            joined.append(value)
            for k in range(4):
                spot = slice(level * groups + group, level * groups + group + 1)
                strips[0, 2 + k, spot, :] = value[k:k + 1, :]
                strips[1, k, spot, :] = value[along - 4 + k:along - 3 + k, :]
        last = joined[groups - 1]
        qpad[level, groups, middle, :] = packed_spread(last, flow_field, full_quarter)
        qpad[level, groups + 1, middle, :] = packed_spread(last, wet_field, full_quarter)

        def q(index, shift):
            return qpad[level, index, pl.ds(FIRST + shift, along), :]

        wet = q(groups + 1, 0)
        here = q(groups, 0) * q(groups + 1, -1) * wet
        after = q(groups, 1) * wet * q(groups + 1, 1)
        weights = stencil_weights(here, after)

        wet_spot = GROUP * place_of(wet_field)[1]
        cross_spot = GROUP * place_of(cross_field)[1]
        cross, wet = pad[cross_field, level, middle, :], pad[wet_field, level, middle, :]
        first, final = full_lane == 0, full_lane == LANES - 1
        wet_below = jnp.where(first, spread(last, wet_spot + 3, full), pltpu.roll(wet, 1, 1))
        wet_above = jnp.where(final, spread(last, wet_spot, full), pltpu.roll(wet, LANES - 1, 1))
        cross_above = jnp.where(final, spread(last, cross_spot, full), pltpu.roll(cross, LANES - 1, 1))
        w = stencil_weights(cross * wet_below * wet, cross_above * wet * wet_above)
        near = jnp.where(full_quarter < 2,
                         jnp.where(full_quarter == 0, spread(w[4], LANES - 2, full), spread(w[4], LANES - 1, full)),
                         jnp.where(full_quarter == 2, spread(w[0], 0, full), spread(w[0], 1, full)))
        next_to = jnp.where(full_quarter == 1, spread(w[3], LANES - 1, full),
                            jnp.where(full_quarter == 2, spread(w[1], 0, full), 0.0))
        masked = (
            jnp.where(full_lane < 2, 0.0, w[0]),
            jnp.where(first, 0.0, w[1]),
            w[2],
            jnp.where(final, 0.0, w[3]),
            jnp.where(full_lane >= LANES - 2, 0.0, w[4]),
        )
        for i, value in enumerate(masked):
            across_buf[level, i] = value
        for edge, row in ((0, 0), (1, along - 2)):
            for r in range(2):
                for i, value in enumerate(masked):
                    across_w[edge, level, r, i:i + 1, :] = value[row + r:row + r + 1, :]
                for group in range(groups):
                    spot = slice(level * groups + group, level * groups + group + 1)
                    halo_w[0, edge, r, spot, :] = near[row + r:row + r + 1, :]
                    halo_w[1, edge, r, spot, :] = next_to[row + r:row + r + 1, :]
        for group in range(groups):
            total = q(group, -2) * weights[0]
            for shift in range(-1, 3):
                total = total + q(group, shift) * weights[shift + 2]
            beside = jnp.where(full_quarter == 1, pltpu.roll(total, 1, 1), pltpu.roll(total, LANES - 1, 1))
            halo_term[level, group] = near * total + next_to * beside

    for level in range(levels):
        halo_level(level)

    def across_level(level, carry):
        @pl.when(jnp.logical_and(at_first, level == min(1, levels - 1)))
        def _():
            @pl.when(sides > 0)
            def _():
                pl.semaphore_wait(ready_sems.at[TO_DOWN_SIDES], sides)

            start_sides(0)

        for tile in range(tiles):
            rows = slice(tile * ROWS, (tile + 1) * ROWS)
            w = [across_buf[level, i, rows, :] for i in range(5)]
            terms = [halo_term[level, group, rows, :] for group in range(groups)]
            for begin in range(0, count, BATCH):
                batch = range(begin, min(begin + BATCH, count))
                totals = []
                for field in batch:
                    group, place = place_of(field)
                    value = swept[field, level, rows, :]
                    total = tend[tend_rows(field, level, tile * ROWS, ROWS), :] + value * w[2]
                    total = total + pltpu.roll(value, 2, 1) * w[0] + pltpu.roll(value, 1, 1) * w[1]
                    total = total + pltpu.roll(value, LANES - 1, 1) * w[3] + pltpu.roll(value, LANES - 2, 1) * w[4]
                    term = pltpu.roll(terms[group], (LANES - 2 - GROUP * place) % LANES, 1)
                    totals.append(total + jnp.where(ends, term, 0.0))
                for field, total in zip(batch, totals):
                    result[field, level, rows, :] = total
        return carry

    lax.fori_loop(0, levels, across_level, 0)

    await_load(OWN_KEPT, far)
    both_metas.wait()
    pad[wet_field, :, FIRST - 2:FIRST, :] = meta_in[0, 1]
    for i, index in enumerate((flow_field, wet_field)):
        pad[index, :, FIRST + along:FIRST + along + 2, :] = meta_in[1, i]
    for level in range(levels):
        for edge, tile, row in ((0, 0, 0), (1, tiles - 1, ROWS - 2)):
            start = FIRST + tile * ROWS

            def at(index, shift):
                return pad[index, level, start + shift:start + shift + ROWS, :]

            wet = at(wet_field, 0)
            weights = stencil_weights(at(flow_field, 0) * at(wet_field, -1) * wet,
                                      at(flow_field, 1) * wet * at(wet_field, 1))
            for r in range(2):
                for i, value in enumerate(weights):
                    along_w[edge, level, r, i:i + 1, :] = value[row + r:row + r + 1, :]

    finish(right_corners, left_corners)
    both_rows.wait()


def across_kernel(dims, result, own, far, tend, along_w, across_w, strips, corner_left, corner_right, halo_w,
                  updated, rows_out, sems):
    count, levels, along, stride = dims
    groups = -(-(count + 3) // PER)
    flow_field, wet_field = count, count + 1
    inner = pl.ds(2, along - 4)
    whole = pltpu.make_async_copy(result.at[:, :, inner, :], updated.at[:, :, inner, :], sems.at[0])
    whole.start()

    lane = lax.broadcasted_iota(jnp.int32, (ROWS, LANES), 1)
    quarter = lane % GROUP
    ends = jnp.logical_or(lane < 2, lane >= LANES - 2)
    odd = lax.broadcasted_iota(jnp.int32, (ROWS, LANES), 0) % groups == groups - 1

    def both(value):
        return jnp.where(odd, value, pltpu.roll(value, ROWS - 1, 0))

    terms = {}
    for edge in range(2):
        strip = [
            join(corner_left[edge, k - 4 * edge], corner_right[edge, k - 4 * edge], quarter)
            if k - 4 * edge in (0, 1) else strips[edge, k]
            for k in range(6)
        ]
        wets = {k: both(packed_spread(strip[k], wet_field, quarter)) for k in range(1, 5)}
        flows = {k: both(packed_spread(strip[k], flow_field, quarter)) for k in range(2, 5)}
        faces = {k: flows[k] * wets[k - 1] * wets[k] for k in range(2, 5)}
        for r in range(2):
            weights = stencil_weights(faces[r + 2], faces[r + 3])
            total = strip[r] * weights[0]
            for shift in range(1, 5):
                total = total + strip[r + shift] * weights[shift]
            beside = jnp.where(quarter == 1, pltpu.roll(total, 1, 1), pltpu.roll(total, LANES - 1, 1))
            terms[edge, r] = halo_w[0, edge, r] * total + halo_w[1, edge, r] * beside

    for edge in range(2):
        for level in range(levels):
            near = [own[edge, level, k] for k in range(4)]
            beyond = [far[edge, level, k] for k in range(2)]
            lines = beyond + near if edge == 0 else near + beyond
            for r in range(2):
                row = r if edge == 0 else along - 2 + r
                along_lines, across_lines = along_w[edge, level, r], across_w[edge, level, r]
                value = lines[r] * along_lines[0:1, :]
                for shift in range(1, 5):
                    value = value + lines[r + shift] * along_lines[shift:shift + 1, :]
                total = value * across_lines[2:3, :]
                total = total + pltpu.roll(value, 2, 1) * across_lines[0:1, :]
                total = total + pltpu.roll(value, 1, 1) * across_lines[1:2, :]
                total = total + pltpu.roll(value, LANES - 1, 1) * across_lines[3:4, :]
                total = total + pltpu.roll(value, LANES - 2, 1) * across_lines[4:5, :]
                for begin in range(0, count, ROWS):
                    group, inside = divmod(begin, PER)
                    spot = level * groups + group
                    line = jnp.broadcast_to(terms[edge, r][spot:spot + 1, :], (ROWS, LANES))
                    line = pltpu.roll(line, 2 + GROUP * inside, 1, stride=GROUP, stride_axis=0)
                    rows = pl.ds(begin * stride + level * along + row, ROWS, stride=stride)
                    rows_out[edge, level, r, begin:begin + ROWS, :] = (
                        total[begin:begin + ROWS, :] + tend[rows, :] + jnp.where(ends, line, 0.0))
                pltpu.make_async_copy(
                    rows_out.at[edge, level, r], updated.at[:, level, row, :], sems.at[1]).start()
    whole.wait()
    pltpu.make_async_copy(rows_out, rows_out, sems.at[1]).wait()


def shards(
    tracers,
    velocity,
    land_mask,
    sunlight,
    growth_max,
    half_sat,
    light_half,
    graze_max,
    graze_half,
    palatable,
    stoichiometry,
):
    count, levels, along, across = tracers.shape
    nphy, nzoo = growth_max.shape[0], graze_max.shape[0]
    groups = -(-(count + 3) // PER)
    assert across == LANES and along % ROWS == 0 and along >= 2 * ROWS
    assert count % ROWS == 0 and groups == 2 and (count + 2) % PER >= 2 and levels * groups <= ROWS
    f32 = jnp.float32
    any_space = pl.BlockSpec(memory_space=pl.ANY)
    hbm = pl.BlockSpec(memory_space=pltpu.HBM)
    vmem = pl.BlockSpec(memory_space=pltpu.VMEM)
    small = (growth_max, half_sat, light_half, graze_max, graze_half, palatable, stoichiometry)
    stride = levels * along + ROWS
    line = (ROWS, LANES)
    columns = (levels, groups, along, LANES)
    outputs = [
        (count, levels, along, LANES),
        (2, levels, 4, count, LANES),
        (2, levels, 2, count, LANES),
        (count * stride, LANES),
        (2, levels, 2) + line,
        (2, levels, 2) + line,
        (2, 6) + line,
        (2, 2) + line,
        (2, 2) + line,
        (2, 2, 2) + line,
    ]
    prepared = pl.pallas_call(
        functools.partial(exchange_kernel, (count, levels, along, nphy, nzoo, stride)),
        out_shape=tuple(jax.ShapeDtypeStruct(shape, f32) for shape in outputs),
        in_specs=[hbm] * 11,
        out_specs=(vmem,) * len(outputs),
        scratch_shapes=[pltpu.SMEM(x.shape, x.dtype) for x in small] + [
            pltpu.VMEM((count + 3, levels, FIRST + along + ROWS, LANES), f32),
            pltpu.VMEM(land_mask.shape, jnp.int32),
            pltpu.VMEM(sunlight.shape, f32),
            pltpu.VMEM((count, levels, along, LANES), f32),
            pltpu.VMEM(columns, f32),
            pltpu.VMEM(columns, f32),
            pltpu.VMEM(columns, f32),
            pltpu.VMEM((levels, groups + 2, FIRST + along + ROWS, LANES), f32),
            pltpu.VMEM((levels, groups, along, LANES), f32),
            pltpu.VMEM((levels, 5, along, LANES), f32),
            pltpu.VMEM((2, 2) + line, f32),
            pltpu.VMEM((2, 2, levels, 2, LANES), f32),
            pltpu.VMEM((2, 2, levels, 2, LANES), f32),
            pltpu.SMEM(palatable.shape, f32),
            pltpu.SemaphoreType.DMA((8,)),
            pltpu.SemaphoreType.DMA((levels,)),
            pltpu.SemaphoreType.DMA((6,)),
            pltpu.SemaphoreType.DMA((6,)),
            pltpu.SemaphoreType.REGULAR((5,)),
        ],
        compiler_params=pltpu.CompilerParams(
            collective_id=0, has_side_effects=True, vmem_limit_bytes=32 * 2**20
        ),
        name="exchange",
    )(*[
        pltpu.with_memory_space_constraint(x, pltpu.HBM)
        for x in (tracers, velocity, land_mask, sunlight) + small
    ])
    return pl.pallas_call(
        functools.partial(across_kernel, (count, levels, along, stride)),
        out_shape=jax.ShapeDtypeStruct(tracers.shape, f32),
        in_specs=[vmem] * len(outputs),
        out_specs=any_space,
        scratch_shapes=[
            pltpu.VMEM((2, levels, 2, count, LANES), f32),
            pltpu.SemaphoreType.DMA((2,)),
        ],
        compiler_params=pltpu.CompilerParams(vmem_limit_bytes=24 * 2**20),
        name="across",
    )(*prepared)


def solution(mesh):
    return jax.shard_map(
        shards,
        mesh=mesh,
        in_specs=(
            P("member", None, "tx", "ty"),
            P(None, None, "tx", "ty"),
            P(None, "tx", "ty"),
            P("tx", "ty"),
            P("member"),
            P("member", None),
            P("member"),
            P("member"),
            P("member"),
            P("member", None),
            P(),
        ),
        out_specs=P("member", None, "tx", "ty"),
        check_vma=False,
    )
```

```python
import functools

import jax
import jax.numpy as jnp
from jax import lax
from jax.experimental import pallas as pl
from jax.experimental.pallas import tpu as pltpu
from jax.sharding import PartitionSpec as P

NNUT = 4
plankton_mortality = 0.05
grazer_mortality = 0.3
assimilation = 0.3
attenuation = 0.4

ROWS = 8
LANES = 128
FIRST = 8
GROUP = 4
PER = LANES // GROUP
BATCH = 8
HALF = ROWS // 2
MESH = pl.DeviceIdType.MESH


def stencil_weights(here, after):
    hp, hm = jnp.maximum(here, 0.0), jnp.minimum(here, 0.0)
    ap, am = jnp.maximum(after, 0.0), jnp.minimum(after, 0.0)
    sixth = 1.0 / 6.0
    return (
        -sixth * hp,
        5.0 * sixth * hp + 2.0 * sixth * hm + sixth * ap,
        1.0 - 4.0 * sixth * hp - sixth * hm + sixth * ap + 4.0 * sixth * am,
        -sixth * hm - 2.0 * sixth * ap - 5.0 * sixth * am,
        sixth * am,
    )


def place_of(field):
    return field // PER, PER - 1 - field % PER


def spread(value, lane, dims):
    return jnp.broadcast_to(value[:, lane:lane + 1], dims)


def packed_spread(value, field, quarter):
    start = GROUP * place_of(field)[1]
    parts = [spread(value, start + j, value.shape) for j in range(GROUP)]
    return jnp.where(quarter < 2, jnp.where(quarter == 0, parts[0], parts[1]),
                     jnp.where(quarter == 2, parts[2], parts[3]))


def join(from_left, from_right, which):
    return (jnp.where(which < 2, pltpu.roll(from_right, LANES - 2, 1), pltpu.roll(from_left, 2, 1)),
            jnp.where(which < 2, from_right, from_left))


def exchange_kernel(dims, tracers, velocity, land_mask, sunlight, *refs):
    sources, outs, tables, buffers = refs[:7], refs[7:17], refs[17:24], refs[24:]
    result, own, far, tend, along_w, across_w, strips, corner_left, corner_right, halo_w = outs
    growth_max, half_sat, light_half, graze_max, graze_half, palatable, stoichiometry = tables
    (
        pad, mask_buf, sun_buf, swept, pack, left_in, right_in, qpad, halo_term, across_buf,
        corner_out, shifts, meta_out, meta_in, prey, load_sems, main_sems, send_sems, recv_sems, ready_sems,
    ) = buffers
    count, levels, along, nphy, nzoo, stride = dims
    tiles = along // ROWS
    flow_field, wet_field, cross_field = count, count + 1, count + 2
    groups = qpad.shape[1] - 2
    tx_size, ty_size = lax.axis_size("tx"), lax.axis_size("ty")
    tx, ty = lax.axis_index("tx"), lax.axis_index("ty")
    up, down = lax.rem(tx + 1, tx_size), lax.rem(tx + tx_size - 1, tx_size)
    right, left = lax.rem(ty + 1, ty_size), lax.rem(ty + ty_size - 1, ty_size)
    has_left, has_right = ty > 0, ty < ty_size - 1
    at_first, at_last = tx == 0, tx == tx_size - 1
    root = jnp.logical_and(at_first, jnp.logical_and(lax.axis_index("member") == 0, ty < 2))
    others = jnp.logical_not(root)

    barrier = pltpu.get_barrier_semaphore()
    TO_RIGHT, TO_UP, TO_UP_SIDES, TO_DOWN, TO_DOWN_SIDES = range(5)

    def tell(sem, **target):
        pl.semaphore_signal(sem, inc=1, device_id=target, device_id_type=MESH)

    def tell_row(row, straight, aslant):
        tell(straight, tx=row)

        @pl.when(has_right)
        def _():
            tell(aslant, tx=row, ty=right)

        @pl.when(has_left)
        def _():
            tell(aslant, tx=row, ty=left)

    @pl.when(has_right)
    def _():
        tell(barrier, ty=right)

    @pl.when(jnp.logical_not(at_last))
    def _():
        tell_row(up, barrier, barrier)

    @pl.when(at_first)
    def _():
        tell_row(down, barrier, barrier)

    lefts, rights = has_left.astype(jnp.int32), has_right.astype(jnp.int32)
    sides = lefts + rights

    OWN_UP, OWN_DOWN, OWN_KEPT, PLANES, SUN, TABLE = range(6)

    def own_copy(slot, edge, level, k):
        row = k if edge == 0 else along - 4 + k
        return pltpu.make_async_copy(tracers.at[:, level, row, :], own.at[edge, level, k], load_sems.at[slot])

    def load(sem, src, dst):
        copy = pltpu.make_async_copy(src, dst, sem)
        copy.start()
        return copy

    def await_load(slot, ref):
        pltpu.make_async_copy(ref, ref, load_sems.at[slot]).wait()

    for level in range(levels):
        for k in (2, 3):
            own_copy(OWN_UP, 1, level, k).start()
    load(load_sems.at[PLANES], land_mask, mask_buf)
    load(load_sems.at[PLANES], velocity.at[0], pad.at[flow_field, :, pl.ds(FIRST, along), :])
    for level in range(levels):
        for k in (0, 1):
            own_copy(OWN_DOWN, 0, level, k).start()
    load(load_sems.at[PLANES], velocity.at[1], pad.at[cross_field, :, pl.ds(FIRST, along), :])

    def main(level):
        return pltpu.make_async_copy(
            tracers.at[:, level], pad.at[pl.ds(0, count), level, pl.ds(FIRST, along), :], main_sems.at[level])

    for level in range(levels):
        main(level).start()
    sun = load(load_sems.at[SUN], sunlight, sun_buf)
    table_sems = [load_sems.at[TABLE + i] for i in range(3)] + [send_sems.at[2 + i] for i in range(4)]
    small = [load(sem, src, dst) for sem, src, dst in zip(table_sems, sources, tables)]
    for level in range(levels):
        for k in range(2):
            own_copy(OWN_KEPT, 0, level, 2 + k).start()
            own_copy(OWN_KEPT, 1, level, k).start()

    earlier = lefts + jnp.where(at_first, 0, 1 + sides) + jnp.where(at_last, 1 + sides, 0)

    @pl.when(earlier > 0)
    def _():
        pl.semaphore_wait(barrier, earlier)

    @pl.when(has_left)
    def _():
        tell(ready_sems.at[TO_RIGHT], ty=left)

    @pl.when(jnp.logical_not(at_first))
    def _():
        tell_row(down, ready_sems.at[TO_UP], ready_sems.at[TO_UP_SIDES])

    @pl.when(at_last)
    def _():
        tell_row(up, ready_sems.at[TO_DOWN], ready_sems.at[TO_DOWN_SIDES])

    def remote(slot, src, dst, **target):
        return pltpu.make_async_remote_copy(
            src_ref=src, dst_ref=dst, send_sem=send_sems.at[slot], recv_sem=recv_sems.at[slot],
            device_id=target, device_id_type=MESH)

    ROW, META, RIGHT_CORNERS, RIGHT_COLUMNS, LEFT_CORNERS, LEFT_COLUMNS = range(6)
    up_rows = remote(ROW, own.at[1, :, pl.ds(2, 2)], far.at[0], tx=up)
    down_rows = remote(ROW, own.at[0, :, pl.ds(0, 2)], far.at[1], tx=down)
    up_meta = remote(META, meta_out.at[1], meta_in.at[0], tx=up)
    down_meta = remote(META, meta_out.at[0], meta_in.at[1], tx=down)
    to_right = [
        remote(RIGHT_CORNERS, corner_out.at[1, 1], corner_left.at[0], tx=up, ty=right),
        remote(RIGHT_CORNERS, corner_out.at[1, 0], corner_left.at[1], tx=down, ty=right),
        remote(RIGHT_COLUMNS, pack.at[1], left_in, ty=right),
    ]
    to_left = [
        remote(LEFT_CORNERS, corner_out.at[0, 1], corner_right.at[0], tx=up, ty=left),
        remote(LEFT_CORNERS, corner_out.at[0, 0], corner_right.at[1], tx=down, ty=left),
        remote(LEFT_COLUMNS, pack.at[0], right_in, ty=left),
    ]
    both_rows = remote(ROW, far, far, tx=up)
    both_metas = remote(META, meta_in, meta_in, tx=up)
    right_corners = remote(RIGHT_CORNERS, corner_left, corner_left, tx=up)
    left_corners = remote(LEFT_CORNERS, corner_right, corner_right, tx=up)

    def start(condition, copies):
        @pl.when(condition)
        def _():
            for copy in copies:
                copy.start()

    def start_sides(edge):
        start(has_right, [to_right[1 - edge]])
        start(has_left, [to_left[1 - edge]])

    source = lax.broadcasted_iota(jnp.int32, (2 * LANES, LANES), 0) % LANES
    target = lax.broadcasted_iota(jnp.int32, (2 * LANES, LANES), 1)
    for i, offset in enumerate((-2, -1, 1, 2)):
        shifts[:, i * LANES:(i + 1) * LANES] = jnp.where(source == target + offset, 1.0, 0.0).astype(jnp.bfloat16)

    await_load(OWN_UP, own.at[1, :, pl.ds(2, 2)])
    odd_core = lax.rem(ty, 2) == 1
    start(jnp.logical_and(at_last, jnp.logical_not(odd_core)), [up_rows])
    await_load(OWN_DOWN, own.at[0, :, pl.ds(0, 2)])
    await_load(PLANES, pad.at[pl.ds(count, 3), :, pl.ds(FIRST, along), :])
    pad[wet_field, :, FIRST:FIRST + along, :] = mask_buf[...].astype(jnp.float32)
    for edge, row in enumerate((FIRST, FIRST + along - 2)):
        meta_out[edge, 0] = pad[flow_field, :, row:row + 2, :]
        meta_out[edge, 1] = pad[wet_field, :, row:row + 2, :]
    start(at_last, [up_meta, down_meta])
    middle = jnp.logical_not(jnp.logical_or(at_first, at_last))
    start(middle, [down_meta, down_rows])

    lane = lax.broadcasted_iota(jnp.int32, (ROWS, LANES), 1)
    lane_group = lane // GROUP
    quarter = lane % GROUP

    def sweep_level(level, carry):
        main(level).wait()

        for tile in (0, tiles - 1, *range(1, tiles - 1)):
            start_row = FIRST + tile * ROWS

            def at(field, shift):
                return pad[field, level, pl.ds(start_row + shift, ROWS), :]

            wet = at(wet_field, 0)
            here = at(flow_field, 0) * at(wet_field, -1) * wet
            after = at(flow_field, 1) * wet * at(wet_field, 1)
            weights = stencil_weights(here, after)
            packed = [None] * groups
            for begin in range(0, count + 3, 8):
                batch = range(begin, min(begin + 8, count + 3))
                values = []
                for field in batch:
                    if field < count:
                        value = at(field, -2) * weights[0]
                        for shift in range(-1, 3):
                            value = value + at(field, shift) * weights[shift + 2]
                        values.append(value)
                    group, place = place_of(field)
                    turned = pltpu.roll(at(field, 0), (GROUP * place + 2) % LANES, 1)
                    if packed[group] is None:
                        packed[group] = turned
                    else:
                        packed[group] = jnp.where(lane_group == place, turned, packed[group])
                for field, value in zip(batch, values):
                    swept[field, level, tile * ROWS:(tile + 1) * ROWS, :] = value
            for_left = jnp.where(quarter >= 2, packed[0], pltpu.roll(packed[1], LANES - 2, 1))
            for_right = jnp.where(quarter < 2, packed[0], pltpu.roll(packed[1], 2, 1))
            for side, value in enumerate((for_left, for_right)):
                pack[side, level, tile * ROWS:(tile + 1) * ROWS, :] = value
                for edge, edge_tile, row in ((0, 0, 0), (1, tiles - 1, ROWS - 2)):
                    if tile == edge_tile:
                        for r in range(2):
                            corner_out[side, edge, r, pl.ds(level, 1), :] = value[row + r:row + r + 1, :]
        return carry

    lax.fori_loop(0, levels, sweep_level, 0)
    for copy in small:
        copy.wait()
    sun.wait()

    def send_up():
        pl.semaphore_wait(ready_sems.at[TO_UP], 1)
        up_meta.start()
        up_rows.start()

    def send_down():
        pl.semaphore_wait(ready_sems.at[TO_DOWN], 1)
        down_meta.start()
        down_rows.start()

    pl.when(at_last)(lambda: start_sides(1))
    pl.when(jnp.logical_not(at_first))(lambda: start_sides(0))
    start(has_left, [to_left[2]])
    start(jnp.logical_and(at_last, odd_core), [up_rows])
    start(at_last, [down_rows])
    pl.when(jnp.logical_and(others, jnp.logical_not(at_last)))(send_up)

    @pl.when(has_right)
    def _():
        pl.semaphore_wait(ready_sems.at[TO_RIGHT], 1)
        to_right[2].start()


    for z in range(nzoo):
        for k in range(nphy):
            prey[z, k] = palatable[z, k].astype(jnp.float32)

    def tend_rows(field, level, row=0, size=along):
        return pl.ds(pl.multiple_of(field * stride + level * along + row, ROWS), size)

    def ecology(level, carry):
        second = level == min(1, levels - 1)
        pl.when(jnp.logical_and(root, second))(send_up)
        pl.when(jnp.logical_and(jnp.logical_and(at_first, others), second))(send_down)

        @pl.when(jnp.logical_and(jnp.logical_not(at_last), second))
        def _():
            @pl.when(sides > 0)
            def _():
                pl.semaphore_wait(ready_sems.at[TO_UP_SIDES], sides)

            start_sides(1)

        def field(index):
            return pad[index, level, pl.ds(FIRST, along), :]

        wet = field(wet_field)
        depth = jnp.full((along, LANES), -attenuation * (level.astype(jnp.float32) + 0.5), jnp.float32)
        light = sun_buf[...] * jnp.exp(depth)
        inverse = [1.0 / field(j) for j in range(NNUT)]
        recycled = jnp.zeros((along, LANES), jnp.float32)
        for k in range(nphy):
            phyto = field(NNUT + k)
            worst = inverse[0] * half_sat[0, k]
            for j in range(1, NNUT):
                worst = jnp.maximum(worst, inverse[j] * half_sat[j, k])
            growth = growth_max[k] * light * phyto / ((1.0 + worst) * (light + light_half[k]))
            loss = plankton_mortality * phyto
            change = growth - loss
            recycled = recycled - change
            tend[tend_rows(NNUT + k, level), :] = change
        available = [None] * nzoo
        for k in range(nphy):
            phyto = field(NNUT + k)
            for z in range(nzoo):
                term = prey[z, k] * phyto
                available[z] = term if k == 0 else available[z] + term
        rates = []
        for z in range(nzoo):
            zoo = field(NNUT + nphy + z)
            rate = graze_max[z] * zoo / (graze_half[z] + available[z])
            ingested = rate * available[z]
            loss = grazer_mortality * zoo * zoo
            tend[tend_rows(NNUT + nphy + z, level), :] = wet * (assimilation * ingested - loss)
            recycled = recycled + loss + (1.0 - assimilation) * ingested
            rates.append(rate)
        for k in range(nphy):
            eaten = prey[0, k] * rates[0]
            for z in range(1, nzoo):
                eaten = eaten + prey[z, k] * rates[z]
            rows = tend_rows(NNUT + k, level)
            tend[rows, :] = wet * (tend[rows, :] - field(NNUT + k) * eaten)
        recycled = wet * recycled
        for j in range(NNUT):
            tend[tend_rows(j, level), :] = stoichiometry[j] * recycled
        return carry

    lax.fori_loop(0, levels, ecology, 0)
    pl.when(root)(send_down)


    @pl.when(jnp.logical_not(has_left))
    def _():
        left_in[...] = jnp.zeros_like(left_in)
        corner_left[...] = jnp.zeros_like(corner_left)

    @pl.when(jnp.logical_not(has_right))
    def _():
        right_in[...] = jnp.zeros_like(right_in)
        corner_right[...] = jnp.zeros_like(corner_right)

    def finish(to_right, to_left):
        @pl.when(has_right)
        def _():
            to_right.wait_send()
            to_left.wait_recv()

        @pl.when(has_left)
        def _():
            to_left.wait_send()
            to_right.wait_recv()

    @pl.when(at_first)
    def _():
        @pl.when(sides > 0)
        def _():
            pl.semaphore_wait(ready_sems.at[TO_DOWN_SIDES], sides)

        start_sides(0)

    finish(to_right[2], to_left[2])
    full_lane = lax.broadcasted_iota(jnp.int32, (along, LANES), 1)
    full_quarter = full_lane % GROUP
    full = (along, LANES)
    full_ends = jnp.logical_or(full_lane < 2, full_lane >= LANES - 2)

    def halo_level(level):
        middle = pl.ds(FIRST, along)
        joined = []
        for group, value in enumerate(join(left_in[level], right_in[level], full_quarter)):
            qpad[level, group, middle, :] = value
            joined.append(value)
            for k in range(4):
                spot = slice(group * HALF + level, group * HALF + level + 1)
                strips[0, 2 + k, spot, :] = value[k:k + 1, :]
                strips[1, k, spot, :] = value[along - 4 + k:along - 3 + k, :]
        last = joined[groups - 1]
        qpad[level, groups, middle, :] = packed_spread(last, flow_field, full_quarter)
        qpad[level, groups + 1, middle, :] = packed_spread(last, wet_field, full_quarter)

        def q(index, shift):
            return qpad[level, index, pl.ds(FIRST + shift, along), :]

        wet = q(groups + 1, 0)
        here = q(groups, 0) * q(groups + 1, -1) * wet
        after = q(groups, 1) * wet * q(groups + 1, 1)
        weights = stencil_weights(here, after)

        wet_spot = GROUP * place_of(wet_field)[1]
        cross_spot = GROUP * place_of(cross_field)[1]
        cross, wet = pad[cross_field, level, middle, :], pad[wet_field, level, middle, :]
        first, final = full_lane == 0, full_lane == LANES - 1
        wet_below = jnp.where(first, spread(last, wet_spot + 3, full), pltpu.roll(wet, 1, 1))
        wet_above = jnp.where(final, spread(last, wet_spot, full), pltpu.roll(wet, LANES - 1, 1))
        cross_above = jnp.where(final, spread(last, cross_spot, full), pltpu.roll(cross, LANES - 1, 1))
        w = stencil_weights(cross * wet_below * wet, cross_above * wet * wet_above)
        near = jnp.where(full_quarter < 2,
                         jnp.where(full_quarter == 0, spread(w[4], LANES - 2, full), spread(w[4], LANES - 1, full)),
                         jnp.where(full_quarter == 2, spread(w[0], 0, full), spread(w[0], 1, full)))
        next_to = jnp.where(full_quarter == 1, spread(w[3], LANES - 1, full),
                            jnp.where(full_quarter == 2, spread(w[1], 0, full), 0.0))
        masked = (
            jnp.where(full_lane < 2, 0.0, w[0]),
            jnp.where(first, 0.0, w[1]),
            w[2],
            jnp.where(final, 0.0, w[3]),
            jnp.where(full_lane >= LANES - 2, 0.0, w[4]),
        )
        for i, value in enumerate(masked):
            across_buf[level, i] = value
        for edge, row in ((0, 0), (1, along - 2)):
            for r in range(2):
                for i, value in enumerate(masked):
                    across_w[edge, level, r, i:i + 1, :] = value[row + r:row + r + 1, :]
                for group in range(groups):
                    spot = slice(group * HALF + level, group * HALF + level + 1)
                    halo_w[0, edge, r, spot, :] = near[row + r:row + r + 1, :]
                    halo_w[1, edge, r, spot, :] = next_to[row + r:row + r + 1, :]
        for group in range(groups):
            total = q(group, -2) * weights[0]
            for shift in range(-1, 3):
                total = total + q(group, shift) * weights[shift + 2]
            beside = jnp.where(full_quarter == 1, pltpu.roll(total, 1, 1), pltpu.roll(total, LANES - 1, 1))
            halo_term[level, group] = near * total + next_to * beside

    for level in range(levels):
        halo_level(level)

    def across_level(level, carry):
        w = [across_buf[level, i] for i in range(5)]
        terms = [halo_term[level, group] for group in range(groups)]
        for begin in range(0, count, BATCH):
            batch = range(begin, min(begin + BATCH, count))
            block = jnp.concatenate([swept[field, level] for field in batch], axis=0)
            coarse = block.astype(jnp.bfloat16)
            rest = (block - coarse.astype(jnp.float32)).astype(jnp.bfloat16)
            near = jnp.dot(jnp.concatenate([coarse, rest], axis=1), shifts[...], preferred_element_type=jnp.float32)
            for i, field in enumerate(batch):
                group, place = place_of(field)
                part = near[i * along:(i + 1) * along]
                total = tend[tend_rows(field, level), :] + block[i * along:(i + 1) * along] * w[2]
                for k, weight in enumerate((w[0], w[1], w[3], w[4])):
                    total = total + part[:, k * LANES:(k + 1) * LANES] * weight
                term = pltpu.roll(terms[group], (LANES - 2 - GROUP * place) % LANES, 1)
                result[field, level] = total + jnp.where(full_ends, term, 0.0)
        return carry

    lax.fori_loop(0, levels, across_level, 0)

    await_load(OWN_KEPT, far)
    both_metas.wait()
    pad[wet_field, :, FIRST - 2:FIRST, :] = meta_in[0, 1]
    for i, index in enumerate((flow_field, wet_field)):
        pad[index, :, FIRST + along:FIRST + along + 2, :] = meta_in[1, i]
    for level in range(levels):
        for edge, tile, row in ((0, 0, 0), (1, tiles - 1, ROWS - 2)):
            start = FIRST + tile * ROWS

            def at(index, shift):
                return pad[index, level, start + shift:start + shift + ROWS, :]

            wet = at(wet_field, 0)
            weights = stencil_weights(at(flow_field, 0) * at(wet_field, -1) * wet,
                                      at(flow_field, 1) * wet * at(wet_field, 1))
            for r in range(2):
                for i, value in enumerate(weights):
                    along_w[edge, level, r, i:i + 1, :] = value[row + r:row + r + 1, :]

    finish(right_corners, left_corners)
    both_rows.wait()


def across_kernel(dims, result, own, far, tend, along_w, across_w, strips, corner_left, corner_right, halo_w,
                  updated, rows_out, sems):
    count, levels, along, stride = dims
    groups = -(-(count + 3) // PER)
    flow_field, wet_field = count, count + 1
    inner = pl.ds(2, along - 4)
    whole = pltpu.make_async_copy(result.at[:, :, inner, :], updated.at[:, :, inner, :], sems.at[0])
    whole.start()

    lane = lax.broadcasted_iota(jnp.int32, (ROWS, LANES), 1)
    quarter = lane % GROUP
    ends = jnp.logical_or(lane < 2, lane >= LANES - 2)
    upper = lax.broadcasted_iota(jnp.int32, (ROWS, LANES), 0) >= HALF

    def both(value):
        return jnp.where(upper, value, pltpu.roll(value, HALF, 0))

    terms = {}
    for edge in range(2):
        strip = [strips[edge, k] for k in range(6)]
        for r in range(2):
            first, second = join(corner_left[edge, r], corner_right[edge, r], quarter)
            strip[r + 4 * edge] = jnp.where(upper, pltpu.roll(second, HALF, 0), first)
        wets = {k: both(packed_spread(strip[k], wet_field, quarter)) for k in range(1, 5)}
        flows = {k: both(packed_spread(strip[k], flow_field, quarter)) for k in range(2, 5)}
        faces = {k: flows[k] * wets[k - 1] * wets[k] for k in range(2, 5)}
        for r in range(2):
            weights = stencil_weights(faces[r + 2], faces[r + 3])
            total = strip[r] * weights[0]
            for shift in range(1, 5):
                total = total + strip[r + shift] * weights[shift]
            beside = jnp.where(quarter == 1, pltpu.roll(total, 1, 1), pltpu.roll(total, LANES - 1, 1))
            terms[edge, r] = halo_w[0, edge, r] * total + halo_w[1, edge, r] * beside

    for edge in range(2):
        for level in range(levels):
            near = [own[edge, level, k] for k in range(4)]
            beyond = [far[edge, level, k] for k in range(2)]
            lines = beyond + near if edge == 0 else near + beyond
            for r in range(2):
                row = r if edge == 0 else along - 2 + r
                along_lines, across_lines = along_w[edge, level, r], across_w[edge, level, r]
                value = lines[r] * along_lines[0:1, :]
                for shift in range(1, 5):
                    value = value + lines[r + shift] * along_lines[shift:shift + 1, :]
                total = value * across_lines[2:3, :]
                total = total + pltpu.roll(value, 2, 1) * across_lines[0:1, :]
                total = total + pltpu.roll(value, 1, 1) * across_lines[1:2, :]
                total = total + pltpu.roll(value, LANES - 1, 1) * across_lines[3:4, :]
                total = total + pltpu.roll(value, LANES - 2, 1) * across_lines[4:5, :]
                for begin in range(0, count, ROWS):
                    group, inside = divmod(begin, PER)
                    spot = group * HALF + level
                    line = jnp.broadcast_to(terms[edge, r][spot:spot + 1, :], (ROWS, LANES))
                    line = pltpu.roll(line, 2 + GROUP * inside, 1, stride=GROUP, stride_axis=0)
                    rows = pl.ds(begin * stride + level * along + row, ROWS, stride=stride)
                    rows_out[edge, level, r, begin:begin + ROWS, :] = (
                        total[begin:begin + ROWS, :] + tend[rows, :] + jnp.where(ends, line, 0.0))
                pltpu.make_async_copy(
                    rows_out.at[edge, level, r], updated.at[:, level, row, :], sems.at[1]).start()
    whole.wait()
    pltpu.make_async_copy(rows_out, rows_out, sems.at[1]).wait()


def shards(
    tracers,
    velocity,
    land_mask,
    sunlight,
    growth_max,
    half_sat,
    light_half,
    graze_max,
    graze_half,
    palatable,
    stoichiometry,
):
    count, levels, along, across = tracers.shape
    nphy, nzoo = growth_max.shape[0], graze_max.shape[0]
    groups = -(-(count + 3) // PER)
    assert across == LANES and along % ROWS == 0 and along >= 2 * ROWS
    assert count % ROWS == 0 and groups == 2 and (count + 2) % PER >= 2 and levels <= HALF
    f32 = jnp.float32
    any_space = pl.BlockSpec(memory_space=pl.ANY)
    hbm = pl.BlockSpec(memory_space=pltpu.HBM)
    vmem = pl.BlockSpec(memory_space=pltpu.VMEM)
    small = (growth_max, half_sat, light_half, graze_max, graze_half, palatable, stoichiometry)
    stride = levels * along + ROWS
    line = (ROWS, LANES)
    columns = (levels, along, LANES)
    outputs = [
        (count, levels, along, LANES),
        (2, levels, 4, count, LANES),
        (2, levels, 2, count, LANES),
        (count * stride, LANES),
        (2, levels, 2) + line,
        (2, levels, 2) + line,
        (2, 6) + line,
        (2, 2) + line,
        (2, 2) + line,
        (2, 2, 2) + line,
    ]
    prepared = pl.pallas_call(
        functools.partial(exchange_kernel, (count, levels, along, nphy, nzoo, stride)),
        out_shape=tuple(jax.ShapeDtypeStruct(shape, f32) for shape in outputs),
        in_specs=[hbm] * 11,
        out_specs=(vmem,) * len(outputs),
        scratch_shapes=[pltpu.SMEM(x.shape, x.dtype) for x in small] + [
            pltpu.VMEM((count + 3, levels, FIRST + along + ROWS, LANES), f32),
            pltpu.VMEM(land_mask.shape, jnp.int32),
            pltpu.VMEM(sunlight.shape, f32),
            pltpu.VMEM((count, levels, along, LANES), f32),
            pltpu.VMEM((2,) + columns, f32),
            pltpu.VMEM(columns, f32),
            pltpu.VMEM(columns, f32),
            pltpu.VMEM((levels, groups + 2, FIRST + along + ROWS, LANES), f32),
            pltpu.VMEM((levels, groups, along, LANES), f32),
            pltpu.VMEM((levels, 5, along, LANES), f32),
            pltpu.VMEM((2, 2, 2) + line, f32),
            pltpu.VMEM((2 * LANES, 4 * LANES), jnp.bfloat16),
            pltpu.VMEM((2, 2, levels, 2, LANES), f32),
            pltpu.VMEM((2, 2, levels, 2, LANES), f32),
            pltpu.SMEM(palatable.shape, f32),
            pltpu.SemaphoreType.DMA((8,)),
            pltpu.SemaphoreType.DMA((levels,)),
            pltpu.SemaphoreType.DMA((6,)),
            pltpu.SemaphoreType.DMA((6,)),
            pltpu.SemaphoreType.REGULAR((5,)),
        ],
        compiler_params=pltpu.CompilerParams(
            collective_id=0, has_side_effects=True, vmem_limit_bytes=32 * 2**20
        ),
        name="exchange",
    )(*[
        pltpu.with_memory_space_constraint(x, pltpu.HBM)
        for x in (tracers, velocity, land_mask, sunlight) + small
    ])
    return pl.pallas_call(
        functools.partial(across_kernel, (count, levels, along, stride)),
        out_shape=jax.ShapeDtypeStruct(tracers.shape, f32),
        in_specs=[vmem] * len(outputs),
        out_specs=any_space,
        scratch_shapes=[
            pltpu.VMEM((2, levels, 2, count, LANES), f32),
            pltpu.SemaphoreType.DMA((2,)),
        ],
        compiler_params=pltpu.CompilerParams(vmem_limit_bytes=24 * 2**20),
        name="across",
    )(*prepared)


def solution(mesh):
    return jax.shard_map(
        shards,
        mesh=mesh,
        in_specs=(
            P("member", None, "tx", "ty"),
            P(None, None, "tx", "ty"),
            P(None, "tx", "ty"),
            P("tx", "ty"),
            P("member"),
            P("member", None),
            P("member"),
            P("member"),
            P("member"),
            P("member", None),
            P(),
        ),
        out_specs=P("member", None, "tx", "ty"),
        check_vma=False,
    )
```

```python
import functools

import jax
import jax.numpy as jnp
from jax import lax
from jax.experimental import pallas as pl
from jax.experimental.pallas import tpu as pltpu
from jax.sharding import PartitionSpec as P

NNUT = 4
plankton_mortality = 0.05
grazer_mortality = 0.3
assimilation = 0.3
attenuation = 0.4

ROWS = 8
LANES = 128
FIRST = 8
GROUP = 4
PER = LANES // GROUP
BATCH = 8
HALF = ROWS // 2
MESH = pl.DeviceIdType.MESH


def stencil_weights(here, after):
    hp, hm = jnp.maximum(here, 0.0), jnp.minimum(here, 0.0)
    ap, am = jnp.maximum(after, 0.0), jnp.minimum(after, 0.0)
    sixth = 1.0 / 6.0
    return (
        -sixth * hp,
        5.0 * sixth * hp + 2.0 * sixth * hm + sixth * ap,
        1.0 - 4.0 * sixth * hp - sixth * hm + sixth * ap + 4.0 * sixth * am,
        -sixth * hm - 2.0 * sixth * ap - 5.0 * sixth * am,
        sixth * am,
    )


def place_of(field):
    return field // PER, PER - 1 - field % PER


def spread(value, lane, dims):
    return jnp.broadcast_to(value[:, lane:lane + 1], dims)


def packed_spread(value, field, quarter):
    start = GROUP * place_of(field)[1]
    parts = [spread(value, start + j, value.shape) for j in range(GROUP)]
    return jnp.where(quarter < 2, jnp.where(quarter == 0, parts[0], parts[1]),
                     jnp.where(quarter == 2, parts[2], parts[3]))


def join(from_left, from_right, which):
    return (jnp.where(which < 2, pltpu.roll(from_right, LANES - 2, 1), pltpu.roll(from_left, 2, 1)),
            jnp.where(which < 2, from_right, from_left))


def exchange_kernel(dims, tracers, velocity, land_mask, sunlight, *refs):
    sources, outs, tables, buffers = refs[:7], refs[7:17], refs[17:24], refs[24:]
    result, own, far, tend, along_w, across_w, strips, corner_left, corner_right, halo_w = outs
    growth_max, half_sat, light_half, graze_max, graze_half, palatable, stoichiometry = tables
    (
        pad, mask_buf, sun_buf, swept, pack, left_in, right_in, qpad, halo_term, across_buf,
        corner_out, shifts, meta_out, meta_in, prey, load_sems, main_sems, send_sems, recv_sems, ready_sems,
    ) = buffers
    count, levels, along, nphy, nzoo, stride = dims
    tiles = along // ROWS
    flow_field, wet_field, cross_field = count, count + 1, count + 2
    groups = qpad.shape[1] - 2
    tx_size, ty_size = lax.axis_size("tx"), lax.axis_size("ty")
    tx, ty = lax.axis_index("tx"), lax.axis_index("ty")
    up, down = lax.rem(tx + 1, tx_size), lax.rem(tx + tx_size - 1, tx_size)
    right, left = lax.rem(ty + 1, ty_size), lax.rem(ty + ty_size - 1, ty_size)
    has_left, has_right = ty > 0, ty < ty_size - 1
    at_first, at_last = tx == 0, tx == tx_size - 1
    root = jnp.logical_and(at_first, jnp.logical_and(lax.axis_index("member") == 0, ty < 2))
    others = jnp.logical_not(root)

    barrier = pltpu.get_barrier_semaphore()
    TO_RIGHT, TO_UP, TO_UP_SIDES, TO_DOWN, TO_DOWN_SIDES = range(5)

    def tell(sem, **target):
        pl.semaphore_signal(sem, inc=1, device_id=target, device_id_type=MESH)

    def tell_row(row, straight, aslant):
        tell(straight, tx=row)

        @pl.when(has_right)
        def _():
            tell(aslant, tx=row, ty=right)

        @pl.when(has_left)
        def _():
            tell(aslant, tx=row, ty=left)

    @pl.when(has_right)
    def _():
        tell(barrier, ty=right)

    @pl.when(jnp.logical_not(at_last))
    def _():
        tell_row(up, barrier, barrier)

    @pl.when(at_first)
    def _():
        tell_row(down, barrier, barrier)

    lefts, rights = has_left.astype(jnp.int32), has_right.astype(jnp.int32)
    sides = lefts + rights

    OWN_UP, OWN_DOWN, OWN_KEPT, PLANES, SUN, TABLE = range(6)

    def own_copy(slot, edge, level, k):
        row = k if edge == 0 else along - 4 + k
        return pltpu.make_async_copy(tracers.at[:, level, row, :], own.at[edge, level, k], load_sems.at[slot])

    def load(sem, src, dst):
        copy = pltpu.make_async_copy(src, dst, sem)
        copy.start()
        return copy

    def await_load(slot, ref):
        pltpu.make_async_copy(ref, ref, load_sems.at[slot]).wait()

    for level in range(levels):
        for k in (2, 3):
            own_copy(OWN_UP, 1, level, k).start()
    load(load_sems.at[PLANES], land_mask, mask_buf)
    load(load_sems.at[PLANES], velocity.at[0], pad.at[flow_field, :, pl.ds(FIRST, along), :])
    for level in range(levels):
        for k in (0, 1):
            own_copy(OWN_DOWN, 0, level, k).start()
    load(load_sems.at[PLANES], velocity.at[1], pad.at[cross_field, :, pl.ds(FIRST, along), :])

    def main(level):
        return pltpu.make_async_copy(
            tracers.at[:, level], pad.at[pl.ds(0, count), level, pl.ds(FIRST, along), :], main_sems.at[level])

    for level in range(levels):
        main(level).start()
    sun = load(load_sems.at[SUN], sunlight, sun_buf)
    table_sems = [load_sems.at[TABLE + i] for i in range(3)] + [send_sems.at[2 + i] for i in range(4)]
    small = [load(sem, src, dst) for sem, src, dst in zip(table_sems, sources, tables)]
    for level in range(levels):
        for k in range(2):
            own_copy(OWN_KEPT, 0, level, 2 + k).start()
            own_copy(OWN_KEPT, 1, level, k).start()

    earlier = lefts + jnp.where(at_first, 0, 1 + sides) + jnp.where(at_last, 1 + sides, 0)

    @pl.when(earlier > 0)
    def _():
        pl.semaphore_wait(barrier, earlier)

    @pl.when(has_left)
    def _():
        tell(ready_sems.at[TO_RIGHT], ty=left)

    @pl.when(jnp.logical_not(at_first))
    def _():
        tell_row(down, ready_sems.at[TO_UP], ready_sems.at[TO_UP_SIDES])

    @pl.when(at_last)
    def _():
        tell_row(up, ready_sems.at[TO_DOWN], ready_sems.at[TO_DOWN_SIDES])

    def remote(slot, src, dst, **target):
        return pltpu.make_async_remote_copy(
            src_ref=src, dst_ref=dst, send_sem=send_sems.at[slot], recv_sem=recv_sems.at[slot],
            device_id=target, device_id_type=MESH)

    ROW, META, RIGHT_CORNERS, RIGHT_COLUMNS, LEFT_CORNERS, LEFT_COLUMNS = range(6)
    up_pieces = [
        remote(ROW, own.at[1, level, pl.ds(2, 2)], far.at[0, level], tx=up) for level in range(levels)
    ]
    down_pieces = [
        remote(ROW, own.at[0, level, pl.ds(0, 2)], far.at[1, level], tx=down) for level in range(levels)
    ]
    up_meta = remote(META, meta_out.at[1], meta_in.at[0], tx=up)
    down_meta = remote(META, meta_out.at[0], meta_in.at[1], tx=down)
    to_right = [
        remote(RIGHT_CORNERS, corner_out.at[1, 1], corner_left.at[0], tx=up, ty=right),
        remote(RIGHT_CORNERS, corner_out.at[1, 0], corner_left.at[1], tx=down, ty=right),
        remote(RIGHT_COLUMNS, pack.at[1], left_in, ty=right),
    ]
    to_left = [
        remote(LEFT_CORNERS, corner_out.at[0, 1], corner_right.at[0], tx=up, ty=left),
        remote(LEFT_CORNERS, corner_out.at[0, 0], corner_right.at[1], tx=down, ty=left),
        remote(LEFT_COLUMNS, pack.at[0], right_in, ty=left),
    ]
    both_rows = remote(ROW, far, far, tx=up)
    both_metas = remote(META, meta_in, meta_in, tx=up)
    right_corners = remote(RIGHT_CORNERS, corner_left, corner_left, tx=up)
    left_corners = remote(LEFT_CORNERS, corner_right, corner_right, tx=up)

    def start(condition, copies):
        @pl.when(condition)
        def _():
            for copy in copies:
                copy.start()

    def start_sides(edge):
        start(has_right, [to_right[1 - edge]])
        start(has_left, [to_left[1 - edge]])

    source = lax.broadcasted_iota(jnp.int32, (2 * LANES, LANES), 0) % LANES
    target = lax.broadcasted_iota(jnp.int32, (2 * LANES, LANES), 1)
    for i, offset in enumerate((-2, -1, 1, 2)):
        shifts[:, i * LANES:(i + 1) * LANES] = jnp.where(source == target + offset, 1.0, 0.0).astype(jnp.bfloat16)

    await_load(OWN_UP, own.at[1, :, pl.ds(2, 2)])
    odd_core = lax.rem(ty, 2) == 1
    even_core = jnp.logical_not(odd_core)
    start(jnp.logical_and(at_last, even_core), up_pieces)
    await_load(OWN_DOWN, own.at[0, :, pl.ds(0, 2)])
    middle = jnp.logical_not(jnp.logical_or(at_first, at_last))
    start(jnp.logical_and(middle, even_core), down_pieces)
    await_load(PLANES, pad.at[pl.ds(count, 3), :, pl.ds(FIRST, along), :])
    pad[wet_field, :, FIRST:FIRST + along, :] = mask_buf[...].astype(jnp.float32)
    for edge, row in enumerate((FIRST, FIRST + along - 1)):
        for i, field in enumerate((flow_field, wet_field)):
            for level in range(levels):
                meta_out[edge, i * HALF + level:i * HALF + level + 1, :] = pad[field, level, row:row + 1, :]
    start(at_last, [up_meta, down_meta])
    start(middle, [down_meta])
    start(jnp.logical_and(middle, odd_core), down_pieces[:2])

    lane = lax.broadcasted_iota(jnp.int32, (ROWS, LANES), 1)
    lane_group = lane // GROUP
    quarter = lane % GROUP

    upward = jnp.logical_and(others, jnp.logical_not(at_last))

    beside_root = jnp.logical_and(at_first, jnp.logical_and(lax.axis_index("member") == 0, ty == 2))
    eager = jnp.logical_and(jnp.logical_and(upward, even_core), jnp.logical_not(beside_root))

    def send_up(pieces):
        pl.semaphore_wait(ready_sems.at[TO_UP], 1)
        up_meta.start()
        for piece in pieces:
            piece.start()

    def sweep_level(level, carry):
        main(level).wait()

        @pl.when(jnp.logical_and(eager, level == min(1, levels - 1)))
        def _():
            send_up(up_pieces[:1])


        for tile in (0, tiles - 1, *range(1, tiles - 1)):
            start_row = FIRST + tile * ROWS

            def at(field, shift):
                return pad[field, level, pl.ds(start_row + shift, ROWS), :]

            wet = at(wet_field, 0)
            here = at(flow_field, 0) * at(wet_field, -1) * wet
            after = at(flow_field, 1) * wet * at(wet_field, 1)
            weights = stencil_weights(here, after)
            packed = [None] * groups
            for begin in range(0, count + 3, 8):
                batch = range(begin, min(begin + 8, count + 3))
                values = []
                for field in batch:
                    if field < count:
                        value = at(field, -2) * weights[0]
                        for shift in range(-1, 3):
                            value = value + at(field, shift) * weights[shift + 2]
                        values.append(value)
                    group, place = place_of(field)
                    turned = pltpu.roll(at(field, 0), (GROUP * place + 2) % LANES, 1)
                    if packed[group] is None:
                        packed[group] = turned
                    else:
                        packed[group] = jnp.where(lane_group == place, turned, packed[group])
                for field, value in zip(batch, values):
                    swept[field, level, tile * ROWS:(tile + 1) * ROWS, :] = value
            for group, value in enumerate(packed):
                qpad[level, group, tile * ROWS:(tile + 1) * ROWS, :] = value
        return carry

    lax.fori_loop(0, levels, sweep_level, 0)
    full_lane = lax.broadcasted_iota(jnp.int32, (along, LANES), 1)
    full_quarter = full_lane % GROUP
    for level in range(levels):
        one, two = (qpad[level, group, 0:along, :] for group in range(groups))
        for_left = jnp.where(full_quarter >= 2, one, pltpu.roll(two, LANES - 2, 1))
        for_right = jnp.where(full_quarter < 2, one, pltpu.roll(two, 2, 1))
        for side, value in enumerate((for_left, for_right)):
            pack[side, level] = value
            for edge, row in ((0, 0), (1, along - 2)):
                for r in range(2):
                    corner_out[side, edge, r * HALF + level:r * HALF + level + 1, :] = value[row + r:row + r + 1, :]
    for copy in small:
        copy.wait()
    sun.wait()

    pl.when(jnp.logical_not(at_first))(lambda: start_sides(0))
    pl.when(at_last)(lambda: start_sides(1))
    start(has_left, [to_left[2]])

    def send_up_sides():
        @pl.when(sides > 0)
        def _():
            pl.semaphore_wait(ready_sems.at[TO_UP_SIDES], sides)

        start_sides(1)

    def send_down_sides():
        @pl.when(sides > 0)
        def _():
            pl.semaphore_wait(ready_sems.at[TO_DOWN_SIDES], sides)

        start_sides(0)

    pl.when(upward)(send_up_sides)

    @pl.when(has_right)
    def _():
        pl.semaphore_wait(ready_sems.at[TO_RIGHT], 1)
        to_right[2].start()

    start(jnp.logical_and(at_last, odd_core), up_pieces)
    start(jnp.logical_and(middle, odd_core), down_pieces[2:])
    start(eager, up_pieces[1:])
    pl.when(jnp.logical_and(upward, jnp.logical_not(eager)))(lambda: send_up(up_pieces))

    for z in range(nzoo):
        for k in range(nphy):
            prey[z, k] = palatable[z, k].astype(jnp.float32)

    def tend_rows(field, level, row=0, size=along):
        return pl.ds(pl.multiple_of(field * stride + level * along + row, ROWS), size)

    def ecology(level, carry):
        second, third = level == min(1, levels - 1), level == levels - 1

        @pl.when(jnp.logical_and(jnp.logical_and(root, even_core), level == 0))
        def _():
            send_up(up_pieces)

        pl.when(jnp.logical_and(root, second))(send_up_sides)

        @pl.when(jnp.logical_and(jnp.logical_and(root, odd_core), second))
        def _():
            send_up(up_pieces)

        @pl.when(jnp.logical_and(root, third))
        def _():
            pl.semaphore_wait(ready_sems.at[TO_DOWN], 1)
            down_meta.start()
            for piece in down_pieces:
                piece.start()

        start(jnp.logical_and(at_last, second), down_pieces)

        @pl.when(jnp.logical_and(jnp.logical_and(at_first, others), second))
        def _():
            pl.semaphore_wait(ready_sems.at[TO_DOWN], 1)
            down_meta.start()
            down_pieces[0].start()

        @pl.when(jnp.logical_and(jnp.logical_and(at_first, others), third))
        def _():
            send_down_sides()
            for piece in down_pieces[1:]:
                piece.start()

        def field(index):
            return pad[index, level, pl.ds(FIRST, along), :]

        wet = field(wet_field)
        depth = jnp.full((along, LANES), -attenuation * (level.astype(jnp.float32) + 0.5), jnp.float32)
        light = sun_buf[...] * jnp.exp(depth)
        inverse = [1.0 / field(j) for j in range(NNUT)]
        recycled = jnp.zeros((along, LANES), jnp.float32)
        for k in range(nphy):
            phyto = field(NNUT + k)
            worst = inverse[0] * half_sat[0, k]
            for j in range(1, NNUT):
                worst = jnp.maximum(worst, inverse[j] * half_sat[j, k])
            growth = growth_max[k] * light * phyto / ((1.0 + worst) * (light + light_half[k]))
            loss = plankton_mortality * phyto
            change = growth - loss
            recycled = recycled - change
            tend[tend_rows(NNUT + k, level), :] = change
        available = [None] * nzoo
        for k in range(nphy):
            phyto = field(NNUT + k)
            for z in range(nzoo):
                term = prey[z, k] * phyto
                available[z] = term if k == 0 else available[z] + term
        rates = []
        for z in range(nzoo):
            zoo = field(NNUT + nphy + z)
            rate = graze_max[z] * zoo / (graze_half[z] + available[z])
            ingested = rate * available[z]
            loss = grazer_mortality * zoo * zoo
            tend[tend_rows(NNUT + nphy + z, level), :] = wet * (assimilation * ingested - loss)
            recycled = recycled + loss + (1.0 - assimilation) * ingested
            rates.append(rate)
        for k in range(nphy):
            eaten = prey[0, k] * rates[0]
            for z in range(1, nzoo):
                eaten = eaten + prey[z, k] * rates[z]
            rows = tend_rows(NNUT + k, level)
            tend[rows, :] = wet * (tend[rows, :] - field(NNUT + k) * eaten)
        recycled = wet * recycled
        for j in range(NNUT):
            tend[tend_rows(j, level), :] = stoichiometry[j] * recycled
        return carry

    lax.fori_loop(0, levels, ecology, 0)

    pl.when(root)(send_down_sides)

    @pl.when(jnp.logical_not(has_left))
    def _():
        left_in[...] = jnp.zeros_like(left_in)
        corner_left[...] = jnp.zeros_like(corner_left)

    @pl.when(jnp.logical_not(has_right))
    def _():
        right_in[...] = jnp.zeros_like(right_in)
        corner_right[...] = jnp.zeros_like(corner_right)

    def finish(to_right, to_left):
        @pl.when(has_right)
        def _():
            to_right.wait_send()
            to_left.wait_recv()

        @pl.when(has_left)
        def _():
            to_left.wait_send()
            to_right.wait_recv()

    finish(to_right[2], to_left[2])
    full = (along, LANES)
    full_ends = jnp.logical_or(full_lane < 2, full_lane >= LANES - 2)

    def halo_level(level):
        middle = pl.ds(FIRST, along)
        joined = []
        for group, value in enumerate(join(left_in[level], right_in[level], full_quarter)):
            qpad[level, group, middle, :] = value
            joined.append(value)
            for k in range(4):
                spot = slice(group * HALF + level, group * HALF + level + 1)
                strips[0, 2 + k, spot, :] = value[k:k + 1, :]
                strips[1, k, spot, :] = value[along - 4 + k:along - 3 + k, :]
        last = joined[groups - 1]
        qpad[level, groups, middle, :] = packed_spread(last, flow_field, full_quarter)
        qpad[level, groups + 1, middle, :] = packed_spread(last, wet_field, full_quarter)

        def q(index, shift):
            return qpad[level, index, pl.ds(FIRST + shift, along), :]

        wet = q(groups + 1, 0)
        here = q(groups, 0) * q(groups + 1, -1) * wet
        after = q(groups, 1) * wet * q(groups + 1, 1)
        weights = stencil_weights(here, after)

        wet_spot = GROUP * place_of(wet_field)[1]
        cross_spot = GROUP * place_of(cross_field)[1]
        cross, wet = pad[cross_field, level, middle, :], pad[wet_field, level, middle, :]
        first, final = full_lane == 0, full_lane == LANES - 1
        wet_below = jnp.where(first, spread(last, wet_spot + 3, full), pltpu.roll(wet, 1, 1))
        wet_above = jnp.where(final, spread(last, wet_spot, full), pltpu.roll(wet, LANES - 1, 1))
        cross_above = jnp.where(final, spread(last, cross_spot, full), pltpu.roll(cross, LANES - 1, 1))
        w = stencil_weights(cross * wet_below * wet, cross_above * wet * wet_above)
        near = jnp.where(full_quarter < 2,
                         jnp.where(full_quarter == 0, spread(w[4], LANES - 2, full), spread(w[4], LANES - 1, full)),
                         jnp.where(full_quarter == 2, spread(w[0], 0, full), spread(w[0], 1, full)))
        next_to = jnp.where(full_quarter == 1, spread(w[3], LANES - 1, full),
                            jnp.where(full_quarter == 2, spread(w[1], 0, full), 0.0))
        masked = (
            jnp.where(full_lane < 2, 0.0, w[0]),
            jnp.where(first, 0.0, w[1]),
            w[2],
            jnp.where(final, 0.0, w[3]),
            jnp.where(full_lane >= LANES - 2, 0.0, w[4]),
        )
        for i, value in enumerate(masked):
            across_buf[level, i] = value
        for edge, row in ((0, 0), (1, along - 2)):
            for r in range(2):
                for i, value in enumerate(masked):
                    across_w[edge, level, r, i:i + 1, :] = value[row + r:row + r + 1, :]
                for group in range(groups):
                    spot = slice(group * HALF + level, group * HALF + level + 1)
                    halo_w[0, edge, r, spot, :] = near[row + r:row + r + 1, :]
                    halo_w[1, edge, r, spot, :] = next_to[row + r:row + r + 1, :]
        for group in range(groups):
            total = q(group, -2) * weights[0]
            for shift in range(-1, 3):
                total = total + q(group, shift) * weights[shift + 2]
            beside = jnp.where(full_quarter == 1, pltpu.roll(total, 1, 1), pltpu.roll(total, LANES - 1, 1))
            halo_term[level, group] = near * total + next_to * beside

    for level in range(levels):
        halo_level(level)

    def across_level(level, carry):
        w = [across_buf[level, i] for i in range(5)]
        terms = [halo_term[level, group] for group in range(groups)]
        for begin in range(0, count, BATCH):
            batch = range(begin, min(begin + BATCH, count))
            block = jnp.concatenate([swept[field, level] for field in batch], axis=0)
            coarse = block.astype(jnp.bfloat16)
            rest = (block - coarse.astype(jnp.float32)).astype(jnp.bfloat16)
            near = jnp.dot(jnp.concatenate([coarse, rest], axis=1), shifts[...], preferred_element_type=jnp.float32)
            for i, field in enumerate(batch):
                group, place = place_of(field)
                part = near[i * along:(i + 1) * along]
                total = tend[tend_rows(field, level), :] + block[i * along:(i + 1) * along] * w[2]
                for k, weight in enumerate((w[0], w[1], w[3], w[4])):
                    total = total + part[:, k * LANES:(k + 1) * LANES] * weight
                term = pltpu.roll(terms[group], (LANES - 2 - GROUP * place) % LANES, 1)
                result[field, level] = total + jnp.where(full_ends, term, 0.0)
        return carry

    lax.fori_loop(0, levels, across_level, 0)

    await_load(OWN_KEPT, far)
    both_metas.wait()
    for level in range(levels):
        pad[wet_field, level, FIRST - 1:FIRST, :] = meta_in[0, HALF + level:HALF + level + 1, :]
        for i, index in enumerate((flow_field, wet_field)):
            pad[index, level, FIRST + along:FIRST + along + 1, :] = meta_in[1, i * HALF + level:i * HALF + level + 1, :]
    for level in range(levels):
        for edge, tile, row in ((0, 0, 0), (1, tiles - 1, ROWS - 2)):
            start = FIRST + tile * ROWS

            def at(index, shift):
                return pad[index, level, start + shift:start + shift + ROWS, :]

            wet = at(wet_field, 0)
            weights = stencil_weights(at(flow_field, 0) * at(wet_field, -1) * wet,
                                      at(flow_field, 1) * wet * at(wet_field, 1))
            for r in range(2):
                for i, value in enumerate(weights):
                    along_w[edge, level, r, i:i + 1, :] = value[row + r:row + r + 1, :]

    finish(right_corners, left_corners)
    both_rows.wait()


def across_kernel(dims, result, own, far, tend, along_w, across_w, strips, corner_left, corner_right, halo_w,
                  updated, rows_out, sems):
    count, levels, along, stride = dims
    groups = -(-(count + 3) // PER)
    flow_field, wet_field = count, count + 1
    inner = pl.ds(2, along - 4)
    whole = pltpu.make_async_copy(result.at[:, :, inner, :], updated.at[:, :, inner, :], sems.at[0])
    whole.start()

    lane = lax.broadcasted_iota(jnp.int32, (ROWS, LANES), 1)
    quarter = lane % GROUP
    ends = jnp.logical_or(lane < 2, lane >= LANES - 2)
    upper = lax.broadcasted_iota(jnp.int32, (ROWS, LANES), 0) >= HALF

    def both(value):
        return jnp.where(upper, value, pltpu.roll(value, HALF, 0))

    terms = {}
    for edge in range(2):
        strip = [strips[edge, k] for k in range(6)]
        first, second = join(corner_left[edge], corner_right[edge], quarter)
        strip[4 * edge] = jnp.where(upper, pltpu.roll(second, HALF, 0), first)
        strip[4 * edge + 1] = jnp.where(upper, second, pltpu.roll(first, HALF, 0))
        wets = {k: both(packed_spread(strip[k], wet_field, quarter)) for k in range(1, 5)}
        flows = {k: both(packed_spread(strip[k], flow_field, quarter)) for k in range(2, 5)}
        faces = {k: flows[k] * wets[k - 1] * wets[k] for k in range(2, 5)}
        for r in range(2):
            weights = stencil_weights(faces[r + 2], faces[r + 3])
            total = strip[r] * weights[0]
            for shift in range(1, 5):
                total = total + strip[r + shift] * weights[shift]
            beside = jnp.where(quarter == 1, pltpu.roll(total, 1, 1), pltpu.roll(total, LANES - 1, 1))
            terms[edge, r] = halo_w[0, edge, r] * total + halo_w[1, edge, r] * beside

    for edge in range(2):
        for level in range(levels):
            near = [own[edge, level, k] for k in range(4)]
            beyond = [far[edge, level, k] for k in range(2)]
            lines = beyond + near if edge == 0 else near + beyond
            for r in range(2):
                row = r if edge == 0 else along - 2 + r
                along_lines, across_lines = along_w[edge, level, r], across_w[edge, level, r]
                value = lines[r] * along_lines[0:1, :]
                for shift in range(1, 5):
                    value = value + lines[r + shift] * along_lines[shift:shift + 1, :]
                total = value * across_lines[2:3, :]
                total = total + pltpu.roll(value, 2, 1) * across_lines[0:1, :]
                total = total + pltpu.roll(value, 1, 1) * across_lines[1:2, :]
                total = total + pltpu.roll(value, LANES - 1, 1) * across_lines[3:4, :]
                total = total + pltpu.roll(value, LANES - 2, 1) * across_lines[4:5, :]
                for begin in range(0, count, ROWS):
                    group, inside = divmod(begin, PER)
                    spot = group * HALF + level
                    line = jnp.broadcast_to(terms[edge, r][spot:spot + 1, :], (ROWS, LANES))
                    line = pltpu.roll(line, 2 + GROUP * inside, 1, stride=GROUP, stride_axis=0)
                    rows = pl.ds(begin * stride + level * along + row, ROWS, stride=stride)
                    rows_out[edge, level, r, begin:begin + ROWS, :] = (
                        total[begin:begin + ROWS, :] + tend[rows, :] + jnp.where(ends, line, 0.0))
                pltpu.make_async_copy(
                    rows_out.at[edge, level, r], updated.at[:, level, row, :], sems.at[1]).start()
    whole.wait()
    pltpu.make_async_copy(rows_out, rows_out, sems.at[1]).wait()


def shards(
    tracers,
    velocity,
    land_mask,
    sunlight,
    growth_max,
    half_sat,
    light_half,
    graze_max,
    graze_half,
    palatable,
    stoichiometry,
):
    count, levels, along, across = tracers.shape
    nphy, nzoo = growth_max.shape[0], graze_max.shape[0]
    groups = -(-(count + 3) // PER)
    assert across == LANES and along % ROWS == 0 and along >= 2 * ROWS
    assert count % ROWS == 0 and groups == 2 and (count + 2) % PER >= 2 and levels <= HALF
    f32 = jnp.float32
    any_space = pl.BlockSpec(memory_space=pl.ANY)
    hbm = pl.BlockSpec(memory_space=pltpu.HBM)
    vmem = pl.BlockSpec(memory_space=pltpu.VMEM)
    small = (growth_max, half_sat, light_half, graze_max, graze_half, palatable, stoichiometry)
    stride = levels * along + ROWS
    line = (ROWS, LANES)
    columns = (levels, along, LANES)
    outputs = [
        (count, levels, along, LANES),
        (2, levels, 4, count, LANES),
        (2, levels, 2, count, LANES),
        (count * stride, LANES),
        (2, levels, 2) + line,
        (2, levels, 2) + line,
        (2, 6) + line,
        (2,) + line,
        (2,) + line,
        (2, 2, 2) + line,
    ]
    prepared = pl.pallas_call(
        functools.partial(exchange_kernel, (count, levels, along, nphy, nzoo, stride)),
        out_shape=tuple(jax.ShapeDtypeStruct(shape, f32) for shape in outputs),
        in_specs=[hbm] * 11,
        out_specs=(vmem,) * len(outputs),
        scratch_shapes=[pltpu.SMEM(x.shape, x.dtype) for x in small] + [
            pltpu.VMEM((count + 3, levels, FIRST + along + ROWS, LANES), f32),
            pltpu.VMEM(land_mask.shape, jnp.int32),
            pltpu.VMEM(sunlight.shape, f32),
            pltpu.VMEM((count, levels, along, LANES), f32),
            pltpu.VMEM((2,) + columns, f32),
            pltpu.VMEM(columns, f32),
            pltpu.VMEM(columns, f32),
            pltpu.VMEM((levels, groups + 2, FIRST + along + ROWS, LANES), f32),
            pltpu.VMEM((levels, groups, along, LANES), f32),
            pltpu.VMEM((levels, 5, along, LANES), f32),
            pltpu.VMEM((2, 2) + line, f32),
            pltpu.VMEM((2 * LANES, 4 * LANES), jnp.bfloat16),
            pltpu.VMEM((2,) + line, f32),
            pltpu.VMEM((2,) + line, f32),
            pltpu.SMEM(palatable.shape, f32),
            pltpu.SemaphoreType.DMA((8,)),
            pltpu.SemaphoreType.DMA((levels,)),
            pltpu.SemaphoreType.DMA((6,)),
            pltpu.SemaphoreType.DMA((6,)),
            pltpu.SemaphoreType.REGULAR((5,)),
        ],
        compiler_params=pltpu.CompilerParams(
            collective_id=0, has_side_effects=True, vmem_limit_bytes=32 * 2**20
        ),
        name="exchange",
    )(*[
        pltpu.with_memory_space_constraint(x, pltpu.HBM)
        for x in (tracers, velocity, land_mask, sunlight) + small
    ])
    return pl.pallas_call(
        functools.partial(across_kernel, (count, levels, along, stride)),
        out_shape=jax.ShapeDtypeStruct(tracers.shape, f32),
        in_specs=[vmem] * len(outputs),
        out_specs=any_space,
        scratch_shapes=[
            pltpu.VMEM((2, levels, 2, count, LANES), f32),
            pltpu.SemaphoreType.DMA((2,)),
        ],
        compiler_params=pltpu.CompilerParams(vmem_limit_bytes=24 * 2**20),
        name="across",
    )(*prepared)


def solution(mesh):
    return jax.shard_map(
        shards,
        mesh=mesh,
        in_specs=(
            P("member", None, "tx", "ty"),
            P(None, None, "tx", "ty"),
            P(None, "tx", "ty"),
            P("tx", "ty"),
            P("member"),
            P("member", None),
            P("member"),
            P("member"),
            P("member"),
            P("member", None),
            P(),
        ),
        out_specs=P("member", None, "tx", "ty"),
        check_vma=False,
    )
```

```python
import functools

import jax
import jax.numpy as jnp
from jax import lax
from jax.experimental import pallas as pl
from jax.experimental.pallas import tpu as pltpu
from jax.sharding import PartitionSpec as P

NNUT = 4
plankton_mortality = 0.05
grazer_mortality = 0.3
assimilation = 0.3
attenuation = 0.4

ROWS = 8
LANES = 128
FIRST = 8
GROUP = 4
PER = LANES // GROUP
BATCH = 8
HALF = ROWS // 2
MESH = pl.DeviceIdType.MESH


def stencil_weights(here, after):
    hp, hm = jnp.maximum(here, 0.0), jnp.minimum(here, 0.0)
    ap, am = jnp.maximum(after, 0.0), jnp.minimum(after, 0.0)
    sixth = 1.0 / 6.0
    return (
        -sixth * hp,
        5.0 * sixth * hp + 2.0 * sixth * hm + sixth * ap,
        1.0 - 4.0 * sixth * hp - sixth * hm + sixth * ap + 4.0 * sixth * am,
        -sixth * hm - 2.0 * sixth * ap - 5.0 * sixth * am,
        sixth * am,
    )


def place_of(field):
    return field // PER, PER - 1 - field % PER


def spread(value, lane, dims):
    return jnp.broadcast_to(value[:, lane:lane + 1], dims)


def packed_spread(value, field, quarter):
    start = GROUP * place_of(field)[1]
    parts = [spread(value, start + j, value.shape) for j in range(GROUP)]
    return jnp.where(quarter < 2, jnp.where(quarter == 0, parts[0], parts[1]),
                     jnp.where(quarter == 2, parts[2], parts[3]))


def join(from_left, from_right, which):
    return (jnp.where(which < 2, pltpu.roll(from_right, LANES - 2, 1), pltpu.roll(from_left, 2, 1)),
            jnp.where(which < 2, from_right, from_left))


def exchange_kernel(dims, tracers, velocity, land_mask, sunlight, *refs):
    sources, outs, tables, buffers = refs[:7], refs[7:13], refs[13:20], refs[20:]
    result, own, far, base, along_w, across_w = outs
    growth_max, half_sat, light_half, graze_max, graze_half, palatable, stoichiometry = tables
    (
        pad, mask_buf, sun_buf, swept, tend, strips, corner_left, corner_right, halo_w, pack, left_in, right_in, qpad, halo_term, across_buf,
        corner_out, shifts, meta_out, meta_in, prey, load_sems, main_sems, send_sems, recv_sems, ready_sems,
    ) = buffers
    count, levels, along, nphy, nzoo, stride = dims
    tiles = along // ROWS
    flow_field, wet_field, cross_field = count, count + 1, count + 2
    groups = qpad.shape[1] - 2
    tx_size, ty_size = lax.axis_size("tx"), lax.axis_size("ty")
    tx, ty = lax.axis_index("tx"), lax.axis_index("ty")
    up, down = lax.rem(tx + 1, tx_size), lax.rem(tx + tx_size - 1, tx_size)
    right, left = lax.rem(ty + 1, ty_size), lax.rem(ty + ty_size - 1, ty_size)
    has_left, has_right = ty > 0, ty < ty_size - 1
    at_first, at_last = tx == 0, tx == tx_size - 1
    root = jnp.logical_and(at_first, jnp.logical_and(lax.axis_index("member") == 0, ty < 2))
    others = jnp.logical_not(root)

    barrier = pltpu.get_barrier_semaphore()
    TO_RIGHT, TO_UP, TO_UP_SIDES, TO_DOWN, TO_DOWN_SIDES = range(5)

    def tell(sem, **target):
        pl.semaphore_signal(sem, inc=1, device_id=target, device_id_type=MESH)

    def tell_row(row, straight, aslant):
        tell(straight, tx=row)

        @pl.when(has_right)
        def _():
            tell(aslant, tx=row, ty=right)

        @pl.when(has_left)
        def _():
            tell(aslant, tx=row, ty=left)

    @pl.when(has_right)
    def _():
        tell(barrier, ty=right)

    @pl.when(jnp.logical_not(at_last))
    def _():
        tell_row(up, barrier, barrier)

    @pl.when(at_first)
    def _():
        tell_row(down, barrier, barrier)

    lefts, rights = has_left.astype(jnp.int32), has_right.astype(jnp.int32)
    sides = lefts + rights

    OWN_UP, OWN_DOWN, OWN_KEPT, PLANES, SUN, TABLE = range(6)

    def own_copy(slot, edge, level, k):
        row = k if edge == 0 else along - 4 + k
        return pltpu.make_async_copy(tracers.at[:, level, row, :], own.at[edge, level, k], load_sems.at[slot])

    def load(sem, src, dst):
        copy = pltpu.make_async_copy(src, dst, sem)
        copy.start()
        return copy

    def await_load(slot, ref):
        pltpu.make_async_copy(ref, ref, load_sems.at[slot]).wait()

    for level in range(levels):
        for k in (2, 3):
            own_copy(OWN_UP, 1, level, k).start()
    load(load_sems.at[PLANES], land_mask, mask_buf)
    load(load_sems.at[PLANES], velocity.at[0], pad.at[flow_field, :, pl.ds(FIRST, along), :])
    for level in range(levels):
        for k in (0, 1):
            own_copy(OWN_DOWN, 0, level, k).start()
    load(load_sems.at[PLANES], velocity.at[1], pad.at[cross_field, :, pl.ds(FIRST, along), :])

    def main(level):
        return pltpu.make_async_copy(
            tracers.at[:, level], pad.at[pl.ds(0, count), level, pl.ds(FIRST, along), :], main_sems.at[level])

    for level in range(levels):
        main(level).start()
    sun = load(load_sems.at[SUN], sunlight, sun_buf)
    table_sems = [load_sems.at[TABLE + i] for i in range(3)] + [send_sems.at[2 + i] for i in range(4)]
    small = [load(sem, src, dst) for sem, src, dst in zip(table_sems, sources, tables)]
    for level in range(levels):
        for k in range(2):
            own_copy(OWN_KEPT, 0, level, 2 + k).start()
            own_copy(OWN_KEPT, 1, level, k).start()

    earlier = lefts + jnp.where(at_first, 0, 1 + sides) + jnp.where(at_last, 1 + sides, 0)

    @pl.when(earlier > 0)
    def _():
        pl.semaphore_wait(barrier, earlier)

    @pl.when(has_left)
    def _():
        tell(ready_sems.at[TO_RIGHT], ty=left)

    @pl.when(jnp.logical_not(at_first))
    def _():
        tell_row(down, ready_sems.at[TO_UP], ready_sems.at[TO_UP_SIDES])

    @pl.when(at_last)
    def _():
        tell_row(up, ready_sems.at[TO_DOWN], ready_sems.at[TO_DOWN_SIDES])

    def remote(slot, src, dst, **target):
        return pltpu.make_async_remote_copy(
            src_ref=src, dst_ref=dst, send_sem=send_sems.at[slot], recv_sem=recv_sems.at[slot],
            device_id=target, device_id_type=MESH)

    ROW, META, RIGHT_CORNERS, RIGHT_COLUMNS, LEFT_CORNERS, LEFT_COLUMNS = range(6)
    up_pieces = [
        remote(ROW, own.at[1, level, pl.ds(2, 2)], far.at[0, level], tx=up) for level in range(levels)
    ]
    down_pieces = [
        remote(ROW, own.at[0, level, pl.ds(0, 2)], far.at[1, level], tx=down) for level in range(levels)
    ]
    up_meta = remote(META, meta_out.at[1], meta_in.at[0], tx=up)
    down_meta = remote(META, meta_out.at[0], meta_in.at[1], tx=down)
    to_right = [
        remote(RIGHT_CORNERS, corner_out.at[1, 1], corner_left.at[0], tx=up, ty=right),
        remote(RIGHT_CORNERS, corner_out.at[1, 0], corner_left.at[1], tx=down, ty=right),
        remote(RIGHT_COLUMNS, pack.at[1], left_in, ty=right),
    ]
    to_left = [
        remote(LEFT_CORNERS, corner_out.at[0, 1], corner_right.at[0], tx=up, ty=left),
        remote(LEFT_CORNERS, corner_out.at[0, 0], corner_right.at[1], tx=down, ty=left),
        remote(LEFT_COLUMNS, pack.at[0], right_in, ty=left),
    ]
    both_rows = remote(ROW, far, far, tx=up)
    both_metas = remote(META, meta_in, meta_in, tx=up)
    right_corners = remote(RIGHT_CORNERS, corner_left, corner_left, tx=up)
    left_corners = remote(LEFT_CORNERS, corner_right, corner_right, tx=up)

    def start(condition, copies):
        @pl.when(condition)
        def _():
            for copy in copies:
                copy.start()

    def start_sides(edge):
        start(has_right, [to_right[1 - edge]])
        start(has_left, [to_left[1 - edge]])

    source = lax.broadcasted_iota(jnp.int32, (2 * LANES, LANES), 0) % LANES
    target = lax.broadcasted_iota(jnp.int32, (2 * LANES, LANES), 1)
    for i, offset in enumerate((-2, -1, 1, 2)):
        shifts[:, i * LANES:(i + 1) * LANES] = jnp.where(source == target + offset, 1.0, 0.0).astype(jnp.bfloat16)

    await_load(OWN_UP, own.at[1, :, pl.ds(2, 2)])
    odd_core = lax.rem(ty, 2) == 1
    even_core = jnp.logical_not(odd_core)
    start(jnp.logical_and(at_last, even_core), up_pieces)
    await_load(OWN_DOWN, own.at[0, :, pl.ds(0, 2)])
    middle = jnp.logical_not(jnp.logical_or(at_first, at_last))
    start(jnp.logical_and(middle, even_core), down_pieces[:2])
    await_load(PLANES, pad.at[pl.ds(count, 3), :, pl.ds(FIRST, along), :])
    pad[wet_field, :, FIRST:FIRST + along, :] = mask_buf[...].astype(jnp.float32)
    for edge, row in enumerate((FIRST, FIRST + along - 1)):
        for i, field in enumerate((flow_field, wet_field)):
            for level in range(levels):
                meta_out[edge, i * HALF + level:i * HALF + level + 1, :] = pad[field, level, row:row + 1, :]
    start(at_last, [up_meta, down_meta])
    start(middle, [down_meta])
    start(jnp.logical_and(middle, odd_core), down_pieces[:2])

    lane = lax.broadcasted_iota(jnp.int32, (ROWS, LANES), 1)
    lane_group = lane // GROUP
    quarter = lane % GROUP

    upward = jnp.logical_and(others, jnp.logical_not(at_last))

    beside_root = jnp.logical_and(at_first, jnp.logical_and(lax.axis_index("member") == 0, ty == 2))
    eager = jnp.logical_and(jnp.logical_and(upward, even_core), jnp.logical_not(beside_root))

    def send_up(pieces):
        pl.semaphore_wait(ready_sems.at[TO_UP], 1)
        up_meta.start()
        for piece in pieces:
            piece.start()

    def sweep_level(level, carry):
        main(level).wait()

        @pl.when(jnp.logical_and(eager, level == min(1, levels - 1)))
        def _():
            send_up(up_pieces[:1])


        for tile in (0, tiles - 1, *range(1, tiles - 1)):
            start_row = FIRST + tile * ROWS

            def at(field, shift):
                return pad[field, level, pl.ds(start_row + shift, ROWS), :]

            wet = at(wet_field, 0)
            here = at(flow_field, 0) * at(wet_field, -1) * wet
            after = at(flow_field, 1) * wet * at(wet_field, 1)
            weights = stencil_weights(here, after)
            packed = [None] * groups
            for begin in range(0, count + 3, 8):
                batch = range(begin, min(begin + 8, count + 3))
                values = []
                for field in batch:
                    if field < count:
                        value = at(field, -2) * weights[0]
                        for shift in range(-1, 3):
                            value = value + at(field, shift) * weights[shift + 2]
                        values.append(value)
                    group, place = place_of(field)
                    turned = pltpu.roll(at(field, 0), (GROUP * place + 2) % LANES, 1)
                    if packed[group] is None:
                        packed[group] = turned
                    else:
                        packed[group] = jnp.where(lane_group == place, turned, packed[group])
                for field, value in zip(batch, values):
                    swept[field, level, tile * ROWS:(tile + 1) * ROWS, :] = value
            for group, value in enumerate(packed):
                qpad[level, group, tile * ROWS:(tile + 1) * ROWS, :] = value
        return carry

    lax.fori_loop(0, levels, sweep_level, 0)
    full_lane = lax.broadcasted_iota(jnp.int32, (along, LANES), 1)
    full_quarter = full_lane % GROUP
    for level in range(levels):
        one, two = (qpad[level, group, 0:along, :] for group in range(groups))
        for_left = jnp.where(full_quarter >= 2, one, pltpu.roll(two, LANES - 2, 1))
        for_right = jnp.where(full_quarter < 2, one, pltpu.roll(two, 2, 1))
        for side, value in enumerate((for_left, for_right)):
            pack[side, level] = value
            for edge, row in ((0, 0), (1, along - 2)):
                for r in range(2):
                    corner_out[side, edge, r * HALF + level:r * HALF + level + 1, :] = value[row + r:row + r + 1, :]
    for copy in small:
        copy.wait()
    sun.wait()

    pl.when(jnp.logical_not(at_first))(lambda: start_sides(0))
    pl.when(at_last)(lambda: start_sides(1))
    start(middle, down_pieces[2:])
    start(has_left, [to_left[2]])

    def send_up_sides():
        @pl.when(sides > 0)
        def _():
            pl.semaphore_wait(ready_sems.at[TO_UP_SIDES], sides)

        start_sides(1)

    def send_down_sides():
        @pl.when(sides > 0)
        def _():
            pl.semaphore_wait(ready_sems.at[TO_DOWN_SIDES], sides)

        start_sides(0)

    pl.when(upward)(send_up_sides)

    @pl.when(has_right)
    def _():
        pl.semaphore_wait(ready_sems.at[TO_RIGHT], 1)
        to_right[2].start()

    start(jnp.logical_and(at_last, odd_core), up_pieces)
    start(eager, up_pieces[1:])
    pl.when(jnp.logical_and(upward, jnp.logical_not(eager)))(lambda: send_up(up_pieces))

    for z in range(nzoo):
        for k in range(nphy):
            prey[z, k] = palatable[z, k].astype(jnp.float32)

    def tend_rows(field, level, row=0, size=along):
        return pl.ds(pl.multiple_of(field * stride + level * along + row, ROWS), size)

    def ecology(level, carry):
        second, third = level == min(1, levels - 1), level == levels - 1

        @pl.when(jnp.logical_and(jnp.logical_and(root, even_core), level == 0))
        def _():
            send_up(up_pieces)

        pl.when(jnp.logical_and(root, second))(send_up_sides)

        @pl.when(jnp.logical_and(jnp.logical_and(root, odd_core), second))
        def _():
            send_up(up_pieces)

        @pl.when(jnp.logical_and(root, third))
        def _():
            pl.semaphore_wait(ready_sems.at[TO_DOWN], 1)
            down_meta.start()
            for piece in down_pieces:
                piece.start()

        start(jnp.logical_and(at_last, second), down_pieces)

        @pl.when(jnp.logical_and(jnp.logical_and(at_first, others), second))
        def _():
            pl.semaphore_wait(ready_sems.at[TO_DOWN], 1)
            down_meta.start()
            down_pieces[0].start()

        @pl.when(jnp.logical_and(jnp.logical_and(at_first, others), third))
        def _():
            send_down_sides()
            for piece in down_pieces[1:]:
                piece.start()

        def field(index):
            return pad[index, level, pl.ds(FIRST, along), :]

        wet = field(wet_field)
        depth = jnp.full((along, LANES), -attenuation * (level.astype(jnp.float32) + 0.5), jnp.float32)
        light = sun_buf[...] * jnp.exp(depth)
        inverse = [1.0 / field(j) for j in range(NNUT)]
        recycled = jnp.zeros((along, LANES), jnp.float32)
        for k in range(nphy):
            phyto = field(NNUT + k)
            worst = inverse[0] * half_sat[0, k]
            for j in range(1, NNUT):
                worst = jnp.maximum(worst, inverse[j] * half_sat[j, k])
            growth = growth_max[k] * light * phyto / ((1.0 + worst) * (light + light_half[k]))
            loss = plankton_mortality * phyto
            change = growth - loss
            recycled = recycled - change
            tend[tend_rows(NNUT + k, level), :] = change
        available = [None] * nzoo
        for k in range(nphy):
            phyto = field(NNUT + k)
            for z in range(nzoo):
                term = prey[z, k] * phyto
                available[z] = term if k == 0 else available[z] + term
        rates = []
        for z in range(nzoo):
            zoo = field(NNUT + nphy + z)
            rate = graze_max[z] * zoo / (graze_half[z] + available[z])
            ingested = rate * available[z]
            loss = grazer_mortality * zoo * zoo
            tend[tend_rows(NNUT + nphy + z, level), :] = wet * (assimilation * ingested - loss)
            recycled = recycled + loss + (1.0 - assimilation) * ingested
            rates.append(rate)
        for k in range(nphy):
            eaten = prey[0, k] * rates[0]
            for z in range(1, nzoo):
                eaten = eaten + prey[z, k] * rates[z]
            rows = tend_rows(NNUT + k, level)
            tend[rows, :] = wet * (tend[rows, :] - field(NNUT + k) * eaten)
        recycled = wet * recycled
        for j in range(NNUT):
            tend[tend_rows(j, level), :] = stoichiometry[j] * recycled
        return carry

    lax.fori_loop(0, levels, ecology, 0)

    pl.when(root)(send_down_sides)

    @pl.when(jnp.logical_not(has_left))
    def _():
        left_in[...] = jnp.zeros_like(left_in)
        corner_left[...] = jnp.zeros_like(corner_left)

    @pl.when(jnp.logical_not(has_right))
    def _():
        right_in[...] = jnp.zeros_like(right_in)
        corner_right[...] = jnp.zeros_like(corner_right)

    def finish(to_right, to_left):
        @pl.when(has_right)
        def _():
            to_right.wait_send()
            to_left.wait_recv()

        @pl.when(has_left)
        def _():
            to_left.wait_send()
            to_right.wait_recv()

    finish(to_right[2], to_left[2])
    full = (along, LANES)
    full_ends = jnp.logical_or(full_lane < 2, full_lane >= LANES - 2)

    def halo_level(level):
        middle = pl.ds(FIRST, along)
        joined = []
        for group, value in enumerate(join(left_in[level], right_in[level], full_quarter)):
            qpad[level, group, middle, :] = value
            joined.append(value)
            for k in range(4):
                spot = slice(group * HALF + level, group * HALF + level + 1)
                strips[0, 2 + k, spot, :] = value[k:k + 1, :]
                strips[1, k, spot, :] = value[along - 4 + k:along - 3 + k, :]
        last = joined[groups - 1]
        qpad[level, groups, middle, :] = packed_spread(last, flow_field, full_quarter)
        qpad[level, groups + 1, middle, :] = packed_spread(last, wet_field, full_quarter)

        def q(index, shift):
            return qpad[level, index, pl.ds(FIRST + shift, along), :]

        wet = q(groups + 1, 0)
        here = q(groups, 0) * q(groups + 1, -1) * wet
        after = q(groups, 1) * wet * q(groups + 1, 1)
        weights = stencil_weights(here, after)

        wet_spot = GROUP * place_of(wet_field)[1]
        cross_spot = GROUP * place_of(cross_field)[1]
        cross, wet = pad[cross_field, level, middle, :], pad[wet_field, level, middle, :]
        first, final = full_lane == 0, full_lane == LANES - 1
        wet_below = jnp.where(first, spread(last, wet_spot + 3, full), pltpu.roll(wet, 1, 1))
        wet_above = jnp.where(final, spread(last, wet_spot, full), pltpu.roll(wet, LANES - 1, 1))
        cross_above = jnp.where(final, spread(last, cross_spot, full), pltpu.roll(cross, LANES - 1, 1))
        w = stencil_weights(cross * wet_below * wet, cross_above * wet * wet_above)
        near = jnp.where(full_quarter < 2,
                         jnp.where(full_quarter == 0, spread(w[4], LANES - 2, full), spread(w[4], LANES - 1, full)),
                         jnp.where(full_quarter == 2, spread(w[0], 0, full), spread(w[0], 1, full)))
        next_to = jnp.where(full_quarter == 1, spread(w[3], LANES - 1, full),
                            jnp.where(full_quarter == 2, spread(w[1], 0, full), 0.0))
        masked = (
            jnp.where(full_lane < 2, 0.0, w[0]),
            jnp.where(first, 0.0, w[1]),
            w[2],
            jnp.where(final, 0.0, w[3]),
            jnp.where(full_lane >= LANES - 2, 0.0, w[4]),
        )
        for i, value in enumerate(masked):
            across_buf[level, i] = value
        for edge, row in ((0, 0), (1, along - 2)):
            for r in range(2):
                for i, value in enumerate(masked):
                    across_w[edge, level, r, i:i + 1, :] = value[row + r:row + r + 1, :]
                for group in range(groups):
                    spot = slice(group * HALF + level, group * HALF + level + 1)
                    halo_w[0, edge, r, spot, :] = near[row + r:row + r + 1, :]
                    halo_w[1, edge, r, spot, :] = next_to[row + r:row + r + 1, :]
        for group in range(groups):
            total = q(group, -2) * weights[0]
            for shift in range(-1, 3):
                total = total + q(group, shift) * weights[shift + 2]
            beside = jnp.where(full_quarter == 1, pltpu.roll(total, 1, 1), pltpu.roll(total, LANES - 1, 1))
            halo_term[level, group] = near * total + next_to * beside

    for level in range(levels):
        halo_level(level)

    def across_level(level, carry):
        w = [across_buf[level, i] for i in range(5)]
        terms = [halo_term[level, group] for group in range(groups)]
        for begin in range(0, count, BATCH):
            batch = range(begin, min(begin + BATCH, count))
            block = jnp.concatenate([swept[field, level] for field in batch], axis=0)
            coarse = block.astype(jnp.bfloat16)
            rest = (block - coarse.astype(jnp.float32)).astype(jnp.bfloat16)
            near = jnp.dot(jnp.concatenate([coarse, rest], axis=1), shifts[...], preferred_element_type=jnp.float32)
            for i, field in enumerate(batch):
                group, place = place_of(field)
                part = near[i * along:(i + 1) * along]
                total = tend[tend_rows(field, level), :] + block[i * along:(i + 1) * along] * w[2]
                for k, weight in enumerate((w[0], w[1], w[3], w[4])):
                    total = total + part[:, k * LANES:(k + 1) * LANES] * weight
                term = pltpu.roll(terms[group], (LANES - 2 - GROUP * place) % LANES, 1)
                result[field, level] = total + jnp.where(full_ends, term, 0.0)
        return carry

    lax.fori_loop(0, levels, across_level, 0)

    await_load(OWN_KEPT, far)
    both_metas.wait()
    for level in range(levels):
        pad[wet_field, level, FIRST - 1:FIRST, :] = meta_in[0, HALF + level:HALF + level + 1, :]
        for i, index in enumerate((flow_field, wet_field)):
            pad[index, level, FIRST + along:FIRST + along + 1, :] = meta_in[1, i * HALF + level:i * HALF + level + 1, :]
    for level in range(levels):
        for edge, tile, row in ((0, 0, 0), (1, tiles - 1, ROWS - 2)):
            start = FIRST + tile * ROWS

            def at(index, shift):
                return pad[index, level, start + shift:start + shift + ROWS, :]

            wet = at(wet_field, 0)
            weights = stencil_weights(at(flow_field, 0) * at(wet_field, -1) * wet,
                                      at(flow_field, 1) * wet * at(wet_field, 1))
            for r in range(2):
                for i, value in enumerate(weights):
                    along_w[edge, level, r, i:i + 1, :] = value[row + r:row + r + 1, :]

    finish(right_corners, left_corners)
    ends = jnp.logical_or(lane < 2, lane >= LANES - 2)
    upper = lax.broadcasted_iota(jnp.int32, (ROWS, LANES), 0) >= HALF

    def both(value):
        return jnp.where(upper, value, pltpu.roll(value, HALF, 0))

    terms = {}
    for edge in range(2):
        strip = [strips[edge, k] for k in range(6)]
        first, second = join(corner_left[edge], corner_right[edge], quarter)
        strip[4 * edge] = jnp.where(upper, pltpu.roll(second, HALF, 0), first)
        strip[4 * edge + 1] = jnp.where(upper, second, pltpu.roll(first, HALF, 0))
        wets = {k: both(packed_spread(strip[k], wet_field, quarter)) for k in range(1, 5)}
        flows = {k: both(packed_spread(strip[k], flow_field, quarter)) for k in range(2, 5)}
        faces = {k: flows[k] * wets[k - 1] * wets[k] for k in range(2, 5)}
        for r in range(2):
            weights = stencil_weights(faces[r + 2], faces[r + 3])
            total = strip[r] * weights[0]
            for shift in range(1, 5):
                total = total + strip[r + shift] * weights[shift]
            beside = jnp.where(quarter == 1, pltpu.roll(total, 1, 1), pltpu.roll(total, LANES - 1, 1))
            terms[edge, r] = halo_w[0, edge, r] * total + halo_w[1, edge, r] * beside

    for edge in range(2):
        for level in range(levels):
            for r in range(2):
                row = r if edge == 0 else along - 2 + r
                for begin in range(0, count, ROWS):
                    group, inside = divmod(begin, PER)
                    spot = group * HALF + level
                    line = jnp.broadcast_to(terms[edge, r][spot:spot + 1, :], (ROWS, LANES))
                    line = pltpu.roll(line, 2 + GROUP * inside, 1, stride=GROUP, stride_axis=0)
                    rows = pl.ds(begin * stride + level * along + row, ROWS, stride=stride)
                    base[edge, level, r, begin:begin + ROWS, :] = tend[rows, :] + jnp.where(ends, line, 0.0)

    both_rows.wait()


def across_kernel(dims, result, own, far, base, along_w, across_w, updated, rows_out, sems):
    count, levels, along = dims
    inner = pl.ds(2, along - 4)
    whole = pltpu.make_async_copy(result.at[:, :, inner, :], updated.at[:, :, inner, :], sems.at[0])
    whole.start()

    for edge in range(2):
        for level in range(levels):
            near = [own[edge, level, k] for k in range(4)]
            beyond = [far[edge, level, k] for k in range(2)]
            lines = beyond + near if edge == 0 else near + beyond
            for r in range(2):
                row = r if edge == 0 else along - 2 + r
                along_lines, across_lines = along_w[edge, level, r], across_w[edge, level, r]
                value = lines[r] * along_lines[0:1, :]
                for shift in range(1, 5):
                    value = value + lines[r + shift] * along_lines[shift:shift + 1, :]
                total = base[edge, level, r] + value * across_lines[2:3, :]
                total = total + pltpu.roll(value, 2, 1) * across_lines[0:1, :]
                total = total + pltpu.roll(value, 1, 1) * across_lines[1:2, :]
                total = total + pltpu.roll(value, LANES - 1, 1) * across_lines[3:4, :]
                total = total + pltpu.roll(value, LANES - 2, 1) * across_lines[4:5, :]
                rows_out[edge, level, r] = total
                pltpu.make_async_copy(
                    rows_out.at[edge, level, r], updated.at[:, level, row, :], sems.at[1]).start()
    whole.wait()
    pltpu.make_async_copy(rows_out, rows_out, sems.at[1]).wait()


def shards(
    tracers,
    velocity,
    land_mask,
    sunlight,
    growth_max,
    half_sat,
    light_half,
    graze_max,
    graze_half,
    palatable,
    stoichiometry,
):
    count, levels, along, across = tracers.shape
    nphy, nzoo = growth_max.shape[0], graze_max.shape[0]
    groups = -(-(count + 3) // PER)
    assert across == LANES and along % ROWS == 0 and along >= 2 * ROWS
    assert count % ROWS == 0 and groups == 2 and (count + 2) % PER >= 2 and levels <= HALF
    f32 = jnp.float32
    any_space = pl.BlockSpec(memory_space=pl.ANY)
    hbm = pl.BlockSpec(memory_space=pltpu.HBM)
    vmem = pl.BlockSpec(memory_space=pltpu.VMEM)
    small = (growth_max, half_sat, light_half, graze_max, graze_half, palatable, stoichiometry)
    stride = levels * along + ROWS
    line = (ROWS, LANES)
    columns = (levels, along, LANES)
    outputs = [
        (count, levels, along, LANES),
        (2, levels, 4, count, LANES),
        (2, levels, 2, count, LANES),
        (2, levels, 2, count, LANES),
        (2, levels, 2) + line,
        (2, levels, 2) + line,
    ]
    prepared = pl.pallas_call(
        functools.partial(exchange_kernel, (count, levels, along, nphy, nzoo, stride)),
        out_shape=tuple(jax.ShapeDtypeStruct(shape, f32) for shape in outputs),
        in_specs=[hbm] * 11,
        out_specs=(vmem,) * len(outputs),
        scratch_shapes=[pltpu.SMEM(x.shape, x.dtype) for x in small] + [
            pltpu.VMEM((count + 3, levels, FIRST + along + ROWS, LANES), f32),
            pltpu.VMEM(land_mask.shape, jnp.int32),
            pltpu.VMEM(sunlight.shape, f32),
            pltpu.VMEM((count, levels, along, LANES), f32),
            pltpu.VMEM((count * stride, LANES), f32),
            pltpu.VMEM((2, 6) + line, f32),
            pltpu.VMEM((2,) + line, f32),
            pltpu.VMEM((2,) + line, f32),
            pltpu.VMEM((2, 2, 2) + line, f32),
            pltpu.VMEM((2,) + columns, f32),
            pltpu.VMEM(columns, f32),
            pltpu.VMEM(columns, f32),
            pltpu.VMEM((levels, groups + 2, FIRST + along + ROWS, LANES), f32),
            pltpu.VMEM((levels, groups, along, LANES), f32),
            pltpu.VMEM((levels, 5, along, LANES), f32),
            pltpu.VMEM((2, 2) + line, f32),
            pltpu.VMEM((2 * LANES, 4 * LANES), jnp.bfloat16),
            pltpu.VMEM((2,) + line, f32),
            pltpu.VMEM((2,) + line, f32),
            pltpu.SMEM(palatable.shape, f32),
            pltpu.SemaphoreType.DMA((8,)),
            pltpu.SemaphoreType.DMA((levels,)),
            pltpu.SemaphoreType.DMA((6,)),
            pltpu.SemaphoreType.DMA((6,)),
            pltpu.SemaphoreType.REGULAR((5,)),
        ],
        compiler_params=pltpu.CompilerParams(
            collective_id=0, has_side_effects=True, vmem_limit_bytes=32 * 2**20
        ),
        name="exchange",
    )(*[
        pltpu.with_memory_space_constraint(x, pltpu.HBM)
        for x in (tracers, velocity, land_mask, sunlight) + small
    ])
    return pl.pallas_call(
        functools.partial(across_kernel, (count, levels, along)),
        out_shape=jax.ShapeDtypeStruct(tracers.shape, f32),
        in_specs=[vmem] * len(outputs),
        out_specs=any_space,
        scratch_shapes=[
            pltpu.VMEM((2, levels, 2, count, LANES), f32),
            pltpu.SemaphoreType.DMA((2,)),
        ],
        compiler_params=pltpu.CompilerParams(vmem_limit_bytes=24 * 2**20),
        name="across",
    )(*prepared)


def solution(mesh):
    return jax.shard_map(
        shards,
        mesh=mesh,
        in_specs=(
            P("member", None, "tx", "ty"),
            P(None, None, "tx", "ty"),
            P(None, "tx", "ty"),
            P("tx", "ty"),
            P("member"),
            P("member", None),
            P("member"),
            P("member"),
            P("member"),
            P("member", None),
            P(),
        ),
        out_specs=P("member", None, "tx", "ty"),
        check_vma=False,
    )
```

```python
import functools

import jax
import jax.numpy as jnp
from jax import lax
from jax.experimental import pallas as pl
from jax.experimental.pallas import tpu as pltpu
from jax.sharding import PartitionSpec as P

NNUT = 4
plankton_mortality = 0.05
grazer_mortality = 0.3
assimilation = 0.3
attenuation = 0.4

ROWS = 8
LANES = 128
FIRST = 8
GROUP = 4
PER = LANES // GROUP
BATCH = 8
HALF = ROWS // 2
MESH = pl.DeviceIdType.MESH


def stencil_weights(here, after):
    hp, hm = jnp.maximum(here, 0.0), jnp.minimum(here, 0.0)
    ap, am = jnp.maximum(after, 0.0), jnp.minimum(after, 0.0)
    sixth = 1.0 / 6.0
    return (
        -sixth * hp,
        5.0 * sixth * hp + 2.0 * sixth * hm + sixth * ap,
        1.0 - 4.0 * sixth * hp - sixth * hm + sixth * ap + 4.0 * sixth * am,
        -sixth * hm - 2.0 * sixth * ap - 5.0 * sixth * am,
        sixth * am,
    )


def place_of(field):
    return field // PER, PER - 1 - field % PER


def spread(value, lane, dims):
    return jnp.broadcast_to(value[:, lane:lane + 1], dims)


def packed_spread(value, field, quarter):
    start = GROUP * place_of(field)[1]
    parts = [spread(value, start + j, value.shape) for j in range(GROUP)]
    return jnp.where(quarter < 2, jnp.where(quarter == 0, parts[0], parts[1]),
                     jnp.where(quarter == 2, parts[2], parts[3]))


def join(from_left, from_right, which):
    return (jnp.where(which < 2, pltpu.roll(from_right, LANES - 2, 1), pltpu.roll(from_left, 2, 1)),
            jnp.where(which < 2, from_right, from_left))


def exchange_kernel(dims, tracers, velocity, land_mask, sunlight, *refs):
    sources, outs, tables, buffers = refs[:7], refs[7:13], refs[13:20], refs[20:]
    result, own, far, base, along_w, across_w = outs
    growth_max, half_sat, light_half, graze_max, graze_half, palatable, stoichiometry = tables
    (
        pad, mask_buf, sun_buf, swept, tend, strips, corner_left, corner_right, halo_w, pack, left_in, right_in, qpad, halo_term, across_buf,
        corner_out, shifts, meta_out, meta_in, prey, load_sems, main_sems, send_sems, recv_sems, ready_sems,
    ) = buffers
    count, levels, along, nphy, nzoo, stride = dims
    tiles = along // ROWS
    flow_field, wet_field, cross_field = count, count + 1, count + 2
    groups = qpad.shape[1] - 2
    tx_size, ty_size = lax.axis_size("tx"), lax.axis_size("ty")
    tx, ty = lax.axis_index("tx"), lax.axis_index("ty")
    up, down = lax.rem(tx + 1, tx_size), lax.rem(tx + tx_size - 1, tx_size)
    right, left = lax.rem(ty + 1, ty_size), lax.rem(ty + ty_size - 1, ty_size)
    has_left, has_right = ty > 0, ty < ty_size - 1
    at_first, at_last = tx == 0, tx == tx_size - 1
    root = jnp.logical_and(at_first, jnp.logical_and(lax.axis_index("member") == 0, ty < 2))
    others = jnp.logical_not(root)

    barrier = pltpu.get_barrier_semaphore()
    TO_RIGHT, TO_UP, TO_UP_SIDES, TO_DOWN, TO_DOWN_SIDES = range(5)

    def tell(sem, **target):
        pl.semaphore_signal(sem, inc=1, device_id=target, device_id_type=MESH)

    def tell_row(row, straight, aslant):
        tell(straight, tx=row)

        @pl.when(has_right)
        def _():
            tell(aslant, tx=row, ty=right)

        @pl.when(has_left)
        def _():
            tell(aslant, tx=row, ty=left)

    @pl.when(has_right)
    def _():
        tell(barrier, ty=right)

    @pl.when(jnp.logical_not(at_last))
    def _():
        tell_row(up, barrier, barrier)

    @pl.when(at_first)
    def _():
        tell_row(down, barrier, barrier)

    lefts, rights = has_left.astype(jnp.int32), has_right.astype(jnp.int32)
    sides = lefts + rights

    OWN_UP, OWN_DOWN, OWN_KEPT, PLANES, SUN, TABLE = range(6)

    def own_copy(slot, edge, level, k):
        row = k if edge == 0 else along - 4 + k
        return pltpu.make_async_copy(tracers.at[:, level, row, :], own.at[edge, level, k], load_sems.at[slot])

    def load(sem, src, dst):
        copy = pltpu.make_async_copy(src, dst, sem)
        copy.start()
        return copy

    def await_load(slot, ref):
        pltpu.make_async_copy(ref, ref, load_sems.at[slot]).wait()

    for level in range(levels):
        for k in (2, 3):
            own_copy(OWN_UP, 1, level, k).start()
    load(load_sems.at[PLANES], land_mask, mask_buf)
    load(load_sems.at[PLANES], velocity.at[0], pad.at[flow_field, :, pl.ds(FIRST, along), :])
    for level in range(levels):
        for k in (0, 1):
            own_copy(OWN_DOWN, 0, level, k).start()
    load(load_sems.at[PLANES], velocity.at[1], pad.at[cross_field, :, pl.ds(FIRST, along), :])

    def main(level):
        return pltpu.make_async_copy(
            tracers.at[:, level], pad.at[pl.ds(0, count), level, pl.ds(FIRST, along), :], main_sems.at[level])

    for level in range(levels):
        main(level).start()
    sun = load(load_sems.at[SUN], sunlight, sun_buf)
    table_sems = [load_sems.at[TABLE + i] for i in range(3)] + [send_sems.at[2 + i] for i in range(4)]
    small = [load(sem, src, dst) for sem, src, dst in zip(table_sems, sources, tables)]
    for level in range(levels):
        for k in range(2):
            own_copy(OWN_KEPT, 0, level, 2 + k).start()
            own_copy(OWN_KEPT, 1, level, k).start()

    earlier = lefts + jnp.where(at_first, 0, 1 + sides) + jnp.where(at_last, 1 + sides, 0)

    @pl.when(earlier > 0)
    def _():
        pl.semaphore_wait(barrier, earlier)

    @pl.when(has_left)
    def _():
        tell(ready_sems.at[TO_RIGHT], ty=left)

    @pl.when(jnp.logical_not(at_first))
    def _():
        tell_row(down, ready_sems.at[TO_UP], ready_sems.at[TO_UP_SIDES])

    @pl.when(at_last)
    def _():
        tell_row(up, ready_sems.at[TO_DOWN], ready_sems.at[TO_DOWN_SIDES])

    def remote(slot, src, dst, **target):
        return pltpu.make_async_remote_copy(
            src_ref=src, dst_ref=dst, send_sem=send_sems.at[slot], recv_sem=recv_sems.at[slot],
            device_id=target, device_id_type=MESH)

    ROW, META, RIGHT_CORNERS, RIGHT_COLUMNS, LEFT_CORNERS, LEFT_COLUMNS = range(6)
    up_pieces = [
        remote(ROW, own.at[1, level, pl.ds(2, 2)], far.at[0, level], tx=up) for level in range(levels)
    ]
    down_pieces = [
        remote(ROW, own.at[0, level, pl.ds(0, 2)], far.at[1, level], tx=down) for level in range(levels)
    ]
    up_meta = remote(META, meta_out.at[1], meta_in.at[0], tx=up)
    down_meta = remote(META, meta_out.at[0], meta_in.at[1], tx=down)
    to_right = [
        remote(RIGHT_CORNERS, corner_out.at[1, 1], corner_left.at[0], tx=up, ty=right),
        remote(RIGHT_CORNERS, corner_out.at[1, 0], corner_left.at[1], tx=down, ty=right),
        remote(RIGHT_COLUMNS, pack.at[1], left_in, ty=right),
    ]
    to_left = [
        remote(LEFT_CORNERS, corner_out.at[0, 1], corner_right.at[0], tx=up, ty=left),
        remote(LEFT_CORNERS, corner_out.at[0, 0], corner_right.at[1], tx=down, ty=left),
        remote(LEFT_COLUMNS, pack.at[0], right_in, ty=left),
    ]
    both_rows = remote(ROW, far, far, tx=up)
    both_metas = remote(META, meta_in, meta_in, tx=up)
    right_corners = remote(RIGHT_CORNERS, corner_left, corner_left, tx=up)
    left_corners = remote(LEFT_CORNERS, corner_right, corner_right, tx=up)

    def start(condition, copies):
        @pl.when(condition)
        def _():
            for copy in copies:
                copy.start()

    def start_sides(edge):
        start(has_right, [to_right[1 - edge]])
        start(has_left, [to_left[1 - edge]])

    source = lax.broadcasted_iota(jnp.int32, (2 * LANES, LANES), 0) % LANES
    target = lax.broadcasted_iota(jnp.int32, (2 * LANES, LANES), 1)
    for i, offset in enumerate((-2, -1, 1, 2)):
        shifts[:, i * LANES:(i + 1) * LANES] = jnp.where(source == target + offset, 1.0, 0.0).astype(jnp.bfloat16)

    await_load(OWN_UP, own.at[1, :, pl.ds(2, 2)])
    odd_core = lax.rem(ty, 2) == 1
    even_core = jnp.logical_not(odd_core)
    start(jnp.logical_and(at_last, even_core), up_pieces)
    await_load(OWN_DOWN, own.at[0, :, pl.ds(0, 2)])
    middle = jnp.logical_not(jnp.logical_or(at_first, at_last))
    start(jnp.logical_and(middle, even_core), down_pieces)
    await_load(PLANES, pad.at[pl.ds(count, 3), :, pl.ds(FIRST, along), :])
    pad[wet_field, :, FIRST:FIRST + along, :] = mask_buf[...].astype(jnp.float32)
    for edge, row in enumerate((FIRST, FIRST + along - 1)):
        for i, field in enumerate((flow_field, wet_field)):
            for level in range(levels):
                meta_out[edge, i * HALF + level:i * HALF + level + 1, :] = pad[field, level, row:row + 1, :]
    start(at_last, [up_meta, down_meta])
    start(middle, [down_meta])

    lane = lax.broadcasted_iota(jnp.int32, (ROWS, LANES), 1)
    lane_group = lane // GROUP
    quarter = lane % GROUP

    upward = jnp.logical_and(others, jnp.logical_not(at_last))

    beside_root = jnp.logical_and(at_first, jnp.logical_and(lax.axis_index("member") == 0, ty == 2))
    eager = jnp.logical_and(jnp.logical_and(upward, even_core), jnp.logical_not(beside_root))

    def send_up(pieces):
        pl.semaphore_wait(ready_sems.at[TO_UP], 1)
        up_meta.start()
        for piece in pieces:
            piece.start()

    def sweep_level(level, carry):
        main(level).wait()

        @pl.when(jnp.logical_and(eager, level == min(1, levels - 1)))
        def _():
            send_up(up_pieces[:1])


        for tile in (0, tiles - 1, *range(1, tiles - 1)):
            start_row = FIRST + tile * ROWS

            def at(field, shift):
                return pad[field, level, pl.ds(start_row + shift, ROWS), :]

            wet = at(wet_field, 0)
            here = at(flow_field, 0) * at(wet_field, -1) * wet
            after = at(flow_field, 1) * wet * at(wet_field, 1)
            weights = stencil_weights(here, after)
            packed = [None] * groups
            for begin in range(0, count + 3, 8):
                batch = range(begin, min(begin + 8, count + 3))
                values = []
                for field in batch:
                    if field < count:
                        value = at(field, -2) * weights[0]
                        for shift in range(-1, 3):
                            value = value + at(field, shift) * weights[shift + 2]
                        values.append(value)
                    group, place = place_of(field)
                    turned = pltpu.roll(at(field, 0), (GROUP * place + 2) % LANES, 1)
                    if packed[group] is None:
                        packed[group] = turned
                    else:
                        packed[group] = jnp.where(lane_group == place, turned, packed[group])
                for field, value in zip(batch, values):
                    swept[field, level, tile * ROWS:(tile + 1) * ROWS, :] = value
            for group, value in enumerate(packed):
                qpad[level, group, tile * ROWS:(tile + 1) * ROWS, :] = value
        return carry

    lax.fori_loop(0, levels, sweep_level, 0)
    full_lane = lax.broadcasted_iota(jnp.int32, (along, LANES), 1)
    full_quarter = full_lane % GROUP
    for level in range(levels):
        one, two = (qpad[level, group, 0:along, :] for group in range(groups))
        for_left = jnp.where(full_quarter >= 2, one, pltpu.roll(two, LANES - 2, 1))
        for_right = jnp.where(full_quarter < 2, one, pltpu.roll(two, 2, 1))
        for side, value in enumerate((for_left, for_right)):
            pack[side, level] = value
            for edge, row in ((0, 0), (1, along - 2)):
                for r in range(2):
                    corner_out[side, edge, r * HALF + level:r * HALF + level + 1, :] = value[row + r:row + r + 1, :]
    for copy in small:
        copy.wait()
    sun.wait()

    pl.when(jnp.logical_not(at_first))(lambda: start_sides(0))
    pl.when(at_last)(lambda: start_sides(1))
    start(has_left, [to_left[2]])

    def send_up_sides():
        @pl.when(sides > 0)
        def _():
            pl.semaphore_wait(ready_sems.at[TO_UP_SIDES], sides)

        start_sides(1)

    def send_down_sides():
        @pl.when(sides > 0)
        def _():
            pl.semaphore_wait(ready_sems.at[TO_DOWN_SIDES], sides)

        start_sides(0)

    pl.when(upward)(send_up_sides)

    @pl.when(has_right)
    def _():
        pl.semaphore_wait(ready_sems.at[TO_RIGHT], 1)
        to_right[2].start()

    start(jnp.logical_and(at_last, odd_core), up_pieces)
    start(eager, up_pieces[1:])
    pl.when(jnp.logical_and(upward, jnp.logical_not(eager)))(lambda: send_up(up_pieces))

    for z in range(nzoo):
        for k in range(nphy):
            prey[z, k] = palatable[z, k].astype(jnp.float32)

    def tend_rows(field, level, row=0, size=along):
        return pl.ds(pl.multiple_of(field * stride + level * along + row, ROWS), size)

    def ecology(level, carry):
        second, third = level == min(1, levels - 1), level == levels - 1

        @pl.when(jnp.logical_and(jnp.logical_and(root, even_core), level == 0))
        def _():
            send_up(up_pieces)

        pl.when(jnp.logical_and(root, second))(send_up_sides)

        @pl.when(jnp.logical_and(jnp.logical_and(root, odd_core), second))
        def _():
            send_up(up_pieces)

        @pl.when(jnp.logical_and(root, third))
        def _():
            pl.semaphore_wait(ready_sems.at[TO_DOWN], 1)
            down_meta.start()
            for piece in down_pieces:
                piece.start()

        start(jnp.logical_or(jnp.logical_and(at_last, second), jnp.logical_and(jnp.logical_and(middle, odd_core), level == 0)), down_pieces)

        @pl.when(jnp.logical_and(jnp.logical_and(at_first, others), second))
        def _():
            pl.semaphore_wait(ready_sems.at[TO_DOWN], 1)
            down_meta.start()
            down_pieces[0].start()

        @pl.when(jnp.logical_and(jnp.logical_and(at_first, others), third))
        def _():
            send_down_sides()
            for piece in down_pieces[1:]:
                piece.start()

        def field(index):
            return pad[index, level, pl.ds(FIRST, along), :]

        wet = field(wet_field)
        depth = jnp.full((along, LANES), -attenuation * (level.astype(jnp.float32) + 0.5), jnp.float32)
        light = sun_buf[...] * jnp.exp(depth)
        inverse = [1.0 / field(j) for j in range(NNUT)]
        recycled = jnp.zeros((along, LANES), jnp.float32)
        for k in range(nphy):
            phyto = field(NNUT + k)
            worst = inverse[0] * half_sat[0, k]
            for j in range(1, NNUT):
                worst = jnp.maximum(worst, inverse[j] * half_sat[j, k])
            growth = growth_max[k] * light * phyto / ((1.0 + worst) * (light + light_half[k]))
            loss = plankton_mortality * phyto
            change = growth - loss
            recycled = recycled - change
            tend[tend_rows(NNUT + k, level), :] = change
        available = [None] * nzoo
        for k in range(nphy):
            phyto = field(NNUT + k)
            for z in range(nzoo):
                term = prey[z, k] * phyto
                available[z] = term if k == 0 else available[z] + term
        rates = []
        for z in range(nzoo):
            zoo = field(NNUT + nphy + z)
            rate = graze_max[z] * zoo / (graze_half[z] + available[z])
            ingested = rate * available[z]
            loss = grazer_mortality * zoo * zoo
            tend[tend_rows(NNUT + nphy + z, level), :] = wet * (assimilation * ingested - loss)
            recycled = recycled + loss + (1.0 - assimilation) * ingested
            rates.append(rate)
        for k in range(nphy):
            eaten = prey[0, k] * rates[0]
            for z in range(1, nzoo):
                eaten = eaten + prey[z, k] * rates[z]
            rows = tend_rows(NNUT + k, level)
            tend[rows, :] = wet * (tend[rows, :] - field(NNUT + k) * eaten)
        recycled = wet * recycled
        for j in range(NNUT):
            tend[tend_rows(j, level), :] = stoichiometry[j] * recycled
        return carry

    lax.fori_loop(0, levels, ecology, 0)

    pl.when(root)(send_down_sides)

    @pl.when(jnp.logical_not(has_left))
    def _():
        left_in[...] = jnp.zeros_like(left_in)
        corner_left[...] = jnp.zeros_like(corner_left)

    @pl.when(jnp.logical_not(has_right))
    def _():
        right_in[...] = jnp.zeros_like(right_in)
        corner_right[...] = jnp.zeros_like(corner_right)

    def finish(to_right, to_left):
        @pl.when(has_right)
        def _():
            to_right.wait_send()
            to_left.wait_recv()

        @pl.when(has_left)
        def _():
            to_left.wait_send()
            to_right.wait_recv()

    finish(to_right[2], to_left[2])
    full = (along, LANES)
    full_ends = jnp.logical_or(full_lane < 2, full_lane >= LANES - 2)

    def halo_level(level):
        middle = pl.ds(FIRST, along)
        joined = []
        for group, value in enumerate(join(left_in[level], right_in[level], full_quarter)):
            qpad[level, group, middle, :] = value
            joined.append(value)
            for k in range(4):
                spot = slice(group * HALF + level, group * HALF + level + 1)
                strips[0, 2 + k, spot, :] = value[k:k + 1, :]
                strips[1, k, spot, :] = value[along - 4 + k:along - 3 + k, :]
        last = joined[groups - 1]
        qpad[level, groups, middle, :] = packed_spread(last, flow_field, full_quarter)
        qpad[level, groups + 1, middle, :] = packed_spread(last, wet_field, full_quarter)

        def q(index, shift):
            return qpad[level, index, pl.ds(FIRST + shift, along), :]

        wet = q(groups + 1, 0)
        here = q(groups, 0) * q(groups + 1, -1) * wet
        after = q(groups, 1) * wet * q(groups + 1, 1)
        weights = stencil_weights(here, after)

        wet_spot = GROUP * place_of(wet_field)[1]
        cross_spot = GROUP * place_of(cross_field)[1]
        cross, wet = pad[cross_field, level, middle, :], pad[wet_field, level, middle, :]
        first, final = full_lane == 0, full_lane == LANES - 1
        wet_below = jnp.where(first, spread(last, wet_spot + 3, full), pltpu.roll(wet, 1, 1))
        wet_above = jnp.where(final, spread(last, wet_spot, full), pltpu.roll(wet, LANES - 1, 1))
        cross_above = jnp.where(final, spread(last, cross_spot, full), pltpu.roll(cross, LANES - 1, 1))
        w = stencil_weights(cross * wet_below * wet, cross_above * wet * wet_above)
        near = jnp.where(full_quarter < 2,
                         jnp.where(full_quarter == 0, spread(w[4], LANES - 2, full), spread(w[4], LANES - 1, full)),
                         jnp.where(full_quarter == 2, spread(w[0], 0, full), spread(w[0], 1, full)))
        next_to = jnp.where(full_quarter == 1, spread(w[3], LANES - 1, full),
                            jnp.where(full_quarter == 2, spread(w[1], 0, full), 0.0))
        masked = (
            jnp.where(full_lane < 2, 0.0, w[0]),
            jnp.where(first, 0.0, w[1]),
            w[2],
            jnp.where(final, 0.0, w[3]),
            jnp.where(full_lane >= LANES - 2, 0.0, w[4]),
        )
        for i, value in enumerate(masked):
            across_buf[level, i] = value
        for edge, row in ((0, 0), (1, along - 2)):
            for r in range(2):
                for i, value in enumerate(masked):
                    across_w[edge, level, r, i:i + 1, :] = value[row + r:row + r + 1, :]
                for group in range(groups):
                    spot = slice(group * HALF + level, group * HALF + level + 1)
                    halo_w[0, edge, r, spot, :] = near[row + r:row + r + 1, :]
                    halo_w[1, edge, r, spot, :] = next_to[row + r:row + r + 1, :]
        for group in range(groups):
            total = q(group, -2) * weights[0]
            for shift in range(-1, 3):
                total = total + q(group, shift) * weights[shift + 2]
            beside = jnp.where(full_quarter == 1, pltpu.roll(total, 1, 1), pltpu.roll(total, LANES - 1, 1))
            halo_term[level, group] = near * total + next_to * beside

    for level in range(levels):
        halo_level(level)

    def across_level(level, carry):
        w = [across_buf[level, i] for i in range(5)]
        terms = [halo_term[level, group] for group in range(groups)]
        for begin in range(0, count, BATCH):
            batch = range(begin, min(begin + BATCH, count))
            block = jnp.concatenate([swept[field, level] for field in batch], axis=0)
            coarse = block.astype(jnp.bfloat16)
            rest = (block - coarse.astype(jnp.float32)).astype(jnp.bfloat16)
            near = jnp.dot(jnp.concatenate([coarse, rest], axis=1), shifts[...], preferred_element_type=jnp.float32)
            for i, field in enumerate(batch):
                group, place = place_of(field)
                part = near[i * along:(i + 1) * along]
                total = tend[tend_rows(field, level), :] + block[i * along:(i + 1) * along] * w[2]
                for k, weight in enumerate((w[0], w[1], w[3], w[4])):
                    total = total + part[:, k * LANES:(k + 1) * LANES] * weight
                term = pltpu.roll(terms[group], (LANES - 2 - GROUP * place) % LANES, 1)
                result[field, level] = total + jnp.where(full_ends, term, 0.0)
        return carry

    lax.fori_loop(0, levels, across_level, 0)

    await_load(OWN_KEPT, far)
    both_metas.wait()
    for level in range(levels):
        pad[wet_field, level, FIRST - 1:FIRST, :] = meta_in[0, HALF + level:HALF + level + 1, :]
        for i, index in enumerate((flow_field, wet_field)):
            pad[index, level, FIRST + along:FIRST + along + 1, :] = meta_in[1, i * HALF + level:i * HALF + level + 1, :]
    for level in range(levels):
        for edge, tile, row in ((0, 0, 0), (1, tiles - 1, ROWS - 2)):
            start = FIRST + tile * ROWS

            def at(index, shift):
                return pad[index, level, start + shift:start + shift + ROWS, :]

            wet = at(wet_field, 0)
            weights = stencil_weights(at(flow_field, 0) * at(wet_field, -1) * wet,
                                      at(flow_field, 1) * wet * at(wet_field, 1))
            for r in range(2):
                for i, value in enumerate(weights):
                    along_w[edge, level, r, i:i + 1, :] = value[row + r:row + r + 1, :]

    finish(right_corners, left_corners)
    ends = jnp.logical_or(lane < 2, lane >= LANES - 2)
    upper = lax.broadcasted_iota(jnp.int32, (ROWS, LANES), 0) >= HALF

    def both(value):
        return jnp.where(upper, value, pltpu.roll(value, HALF, 0))

    terms = {}
    for edge in range(2):
        strip = [strips[edge, k] for k in range(6)]
        first, second = join(corner_left[edge], corner_right[edge], quarter)
        strip[4 * edge] = jnp.where(upper, pltpu.roll(second, HALF, 0), first)
        strip[4 * edge + 1] = jnp.where(upper, second, pltpu.roll(first, HALF, 0))
        wets = {k: both(packed_spread(strip[k], wet_field, quarter)) for k in range(1, 5)}
        flows = {k: both(packed_spread(strip[k], flow_field, quarter)) for k in range(2, 5)}
        faces = {k: flows[k] * wets[k - 1] * wets[k] for k in range(2, 5)}
        for r in range(2):
            weights = stencil_weights(faces[r + 2], faces[r + 3])
            total = strip[r] * weights[0]
            for shift in range(1, 5):
                total = total + strip[r + shift] * weights[shift]
            beside = jnp.where(quarter == 1, pltpu.roll(total, 1, 1), pltpu.roll(total, LANES - 1, 1))
            terms[edge, r] = halo_w[0, edge, r] * total + halo_w[1, edge, r] * beside

    for edge in range(2):
        for level in range(levels):
            for r in range(2):
                row = r if edge == 0 else along - 2 + r
                for begin in range(0, count, ROWS):
                    group, inside = divmod(begin, PER)
                    spot = group * HALF + level
                    line = jnp.broadcast_to(terms[edge, r][spot:spot + 1, :], (ROWS, LANES))
                    line = pltpu.roll(line, 2 + GROUP * inside, 1, stride=GROUP, stride_axis=0)
                    rows = pl.ds(begin * stride + level * along + row, ROWS, stride=stride)
                    base[edge, level, r, begin:begin + ROWS, :] = tend[rows, :] + jnp.where(ends, line, 0.0)

    both_rows.wait()


def across_kernel(dims, result, own, far, base, along_w, across_w, updated, rows_out, sems):
    count, levels, along = dims
    inner = pl.ds(2, along - 4)
    whole = pltpu.make_async_copy(result.at[:, :, inner, :], updated.at[:, :, inner, :], sems.at[0])
    whole.start()

    for edge in range(2):
        for level in range(levels):
            near = [own[edge, level, k] for k in range(4)]
            beyond = [far[edge, level, k] for k in range(2)]
            lines = beyond + near if edge == 0 else near + beyond
            for r in range(2):
                row = r if edge == 0 else along - 2 + r
                along_lines, across_lines = along_w[edge, level, r], across_w[edge, level, r]
                value = lines[r] * along_lines[0:1, :]
                for shift in range(1, 5):
                    value = value + lines[r + shift] * along_lines[shift:shift + 1, :]
                total = base[edge, level, r] + value * across_lines[2:3, :]
                total = total + pltpu.roll(value, 2, 1) * across_lines[0:1, :]
                total = total + pltpu.roll(value, 1, 1) * across_lines[1:2, :]
                total = total + pltpu.roll(value, LANES - 1, 1) * across_lines[3:4, :]
                total = total + pltpu.roll(value, LANES - 2, 1) * across_lines[4:5, :]
                rows_out[edge, level, r] = total
                pltpu.make_async_copy(
                    rows_out.at[edge, level, r], updated.at[:, level, row, :], sems.at[1]).start()
    whole.wait()
    pltpu.make_async_copy(rows_out, rows_out, sems.at[1]).wait()


def shards(
    tracers,
    velocity,
    land_mask,
    sunlight,
    growth_max,
    half_sat,
    light_half,
    graze_max,
    graze_half,
    palatable,
    stoichiometry,
):
    count, levels, along, across = tracers.shape
    nphy, nzoo = growth_max.shape[0], graze_max.shape[0]
    groups = -(-(count + 3) // PER)
    assert across == LANES and along % ROWS == 0 and along >= 2 * ROWS
    assert count % ROWS == 0 and groups == 2 and (count + 2) % PER >= 2 and levels <= HALF
    f32 = jnp.float32
    any_space = pl.BlockSpec(memory_space=pl.ANY)
    hbm = pl.BlockSpec(memory_space=pltpu.HBM)
    vmem = pl.BlockSpec(memory_space=pltpu.VMEM)
    small = (growth_max, half_sat, light_half, graze_max, graze_half, palatable, stoichiometry)
    stride = levels * along + ROWS
    line = (ROWS, LANES)
    columns = (levels, along, LANES)
    outputs = [
        (count, levels, along, LANES),
        (2, levels, 4, count, LANES),
        (2, levels, 2, count, LANES),
        (2, levels, 2, count, LANES),
        (2, levels, 2) + line,
        (2, levels, 2) + line,
    ]
    prepared = pl.pallas_call(
        functools.partial(exchange_kernel, (count, levels, along, nphy, nzoo, stride)),
        out_shape=tuple(jax.ShapeDtypeStruct(shape, f32) for shape in outputs),
        in_specs=[hbm] * 11,
        out_specs=(vmem,) * len(outputs),
        scratch_shapes=[pltpu.SMEM(x.shape, x.dtype) for x in small] + [
            pltpu.VMEM((count + 3, levels, FIRST + along + ROWS, LANES), f32),
            pltpu.VMEM(land_mask.shape, jnp.int32),
            pltpu.VMEM(sunlight.shape, f32),
            pltpu.VMEM((count, levels, along, LANES), f32),
            pltpu.VMEM((count * stride, LANES), f32),
            pltpu.VMEM((2, 6) + line, f32),
            pltpu.VMEM((2,) + line, f32),
            pltpu.VMEM((2,) + line, f32),
            pltpu.VMEM((2, 2, 2) + line, f32),
            pltpu.VMEM((2,) + columns, f32),
            pltpu.VMEM(columns, f32),
            pltpu.VMEM(columns, f32),
            pltpu.VMEM((levels, groups + 2, FIRST + along + ROWS, LANES), f32),
            pltpu.VMEM((levels, groups, along, LANES), f32),
            pltpu.VMEM((levels, 5, along, LANES), f32),
            pltpu.VMEM((2, 2) + line, f32),
            pltpu.VMEM((2 * LANES, 4 * LANES), jnp.bfloat16),
            pltpu.VMEM((2,) + line, f32),
            pltpu.VMEM((2,) + line, f32),
            pltpu.SMEM(palatable.shape, f32),
            pltpu.SemaphoreType.DMA((8,)),
            pltpu.SemaphoreType.DMA((levels,)),
            pltpu.SemaphoreType.DMA((6,)),
            pltpu.SemaphoreType.DMA((6,)),
            pltpu.SemaphoreType.REGULAR((5,)),
        ],
        compiler_params=pltpu.CompilerParams(
            collective_id=0, has_side_effects=True, vmem_limit_bytes=32 * 2**20
        ),
        name="exchange",
    )(*[
        pltpu.with_memory_space_constraint(x, pltpu.HBM)
        for x in (tracers, velocity, land_mask, sunlight) + small
    ])
    return pl.pallas_call(
        functools.partial(across_kernel, (count, levels, along)),
        out_shape=jax.ShapeDtypeStruct(tracers.shape, f32),
        in_specs=[vmem] * len(outputs),
        out_specs=any_space,
        scratch_shapes=[
            pltpu.VMEM((2, levels, 2, count, LANES), f32),
            pltpu.SemaphoreType.DMA((2,)),
        ],
        compiler_params=pltpu.CompilerParams(vmem_limit_bytes=24 * 2**20),
        name="across",
    )(*prepared)


def solution(mesh):
    return jax.shard_map(
        shards,
        mesh=mesh,
        in_specs=(
            P("member", None, "tx", "ty"),
            P(None, None, "tx", "ty"),
            P(None, "tx", "ty"),
            P("tx", "ty"),
            P("member"),
            P("member", None),
            P("member"),
            P("member"),
            P("member"),
            P("member", None),
            P(),
        ),
        out_specs=P("member", None, "tx", "ty"),
        check_vma=False,
    )
```

```python
import functools

import jax
import jax.numpy as jnp
from jax import lax
from jax.experimental import pallas as pl
from jax.experimental.pallas import tpu as pltpu
from jax.sharding import PartitionSpec as P

NNUT = 4
plankton_mortality = 0.05
grazer_mortality = 0.3
assimilation = 0.3
attenuation = 0.4

ROWS = 8
LANES = 128
FIRST = 8
GROUP = 4
PER = LANES // GROUP
BATCH = 8
HALF = ROWS // 2
MESH = pl.DeviceIdType.MESH


def stencil_weights(here, after):
    hp, hm = jnp.maximum(here, 0.0), jnp.minimum(here, 0.0)
    ap, am = jnp.maximum(after, 0.0), jnp.minimum(after, 0.0)
    sixth = 1.0 / 6.0
    return (
        -sixth * hp,
        5.0 * sixth * hp + 2.0 * sixth * hm + sixth * ap,
        1.0 - 4.0 * sixth * hp - sixth * hm + sixth * ap + 4.0 * sixth * am,
        -sixth * hm - 2.0 * sixth * ap - 5.0 * sixth * am,
        sixth * am,
    )


def place_of(field):
    return field // PER, PER - 1 - field % PER


def spread(value, lane, dims):
    return jnp.broadcast_to(value[:, lane:lane + 1], dims)


def packed_spread(value, field, quarter):
    start = GROUP * place_of(field)[1]
    parts = [spread(value, start + j, value.shape) for j in range(GROUP)]
    return jnp.where(quarter < 2, jnp.where(quarter == 0, parts[0], parts[1]),
                     jnp.where(quarter == 2, parts[2], parts[3]))


def join(from_left, from_right, which):
    return (jnp.where(which < 2, pltpu.roll(from_right, LANES - 2, 1), pltpu.roll(from_left, 2, 1)),
            jnp.where(which < 2, from_right, from_left))


def exchange_kernel(dims, tracers, velocity, land_mask, sunlight, *refs):
    sources, outs, tables, buffers = refs[:7], refs[7:13], refs[13:20], refs[20:]
    result, own, far, base, along_w, across_w = outs
    growth_max, half_sat, light_half, graze_max, graze_half, palatable, stoichiometry = tables
    (
        pad, mask_buf, sun_buf, swept, tend, strips, corner_left, corner_right, halo_w, pack, left_in, right_in, qpad, halo_term, across_buf,
        corner_out, shifts, meta_out, meta_in, prey, load_sems, main_sems, send_sems, recv_sems, ready_sems,
    ) = buffers
    count, levels, along, nphy, nzoo, stride = dims
    tiles = along // ROWS
    flow_field, wet_field, cross_field = count, count + 1, count + 2
    groups = qpad.shape[1] - 2
    tx_size, ty_size = lax.axis_size("tx"), lax.axis_size("ty")
    tx, ty = lax.axis_index("tx"), lax.axis_index("ty")
    up, down = lax.rem(tx + 1, tx_size), lax.rem(tx + tx_size - 1, tx_size)
    right, left = lax.rem(ty + 1, ty_size), lax.rem(ty + ty_size - 1, ty_size)
    has_left, has_right = ty > 0, ty < ty_size - 1
    at_first, at_last = tx == 0, tx == tx_size - 1
    root = jnp.logical_and(at_first, jnp.logical_and(lax.axis_index("member") == 0, ty < 2))
    others = jnp.logical_not(root)

    barrier = pltpu.get_barrier_semaphore()
    TO_RIGHT, TO_UP, TO_UP_SIDES, TO_DOWN, TO_DOWN_SIDES = range(5)

    def tell(sem, **target):
        pl.semaphore_signal(sem, inc=1, device_id=target, device_id_type=MESH)

    def tell_row(row, straight, aslant):
        tell(straight, tx=row)

        @pl.when(has_right)
        def _():
            tell(aslant, tx=row, ty=right)

        @pl.when(has_left)
        def _():
            tell(aslant, tx=row, ty=left)

    @pl.when(has_right)
    def _():
        tell(barrier, ty=right)

    @pl.when(jnp.logical_not(at_last))
    def _():
        tell_row(up, barrier, barrier)

    @pl.when(at_first)
    def _():
        tell_row(down, barrier, barrier)

    lefts, rights = has_left.astype(jnp.int32), has_right.astype(jnp.int32)
    sides = lefts + rights

    OWN_UP, OWN_DOWN, OWN_KEPT, PLANES, SUN, TABLE = range(6)

    def own_copy(slot, edge, level, k):
        row = k if edge == 0 else along - 4 + k
        return pltpu.make_async_copy(tracers.at[:, level, row, :], own.at[edge, level, k], load_sems.at[slot])

    def load(sem, src, dst):
        copy = pltpu.make_async_copy(src, dst, sem)
        copy.start()
        return copy

    def await_load(slot, ref):
        pltpu.make_async_copy(ref, ref, load_sems.at[slot]).wait()

    for level in range(levels):
        for k in (2, 3):
            own_copy(OWN_UP, 1, level, k).start()
    load(load_sems.at[PLANES], land_mask, mask_buf)
    load(load_sems.at[PLANES], velocity.at[0], pad.at[flow_field, :, pl.ds(FIRST, along), :])
    for level in range(levels):
        for k in (0, 1):
            own_copy(OWN_DOWN, 0, level, k).start()
    load(load_sems.at[PLANES], velocity.at[1], pad.at[cross_field, :, pl.ds(FIRST, along), :])

    def main(level):
        return pltpu.make_async_copy(
            tracers.at[:, level], pad.at[pl.ds(0, count), level, pl.ds(FIRST, along), :], main_sems.at[level])

    for level in range(levels):
        main(level).start()
    sun = load(load_sems.at[SUN], sunlight, sun_buf)
    table_sems = [load_sems.at[TABLE + i] for i in range(3)] + [send_sems.at[2 + i] for i in range(4)]
    small = [load(sem, src, dst) for sem, src, dst in zip(table_sems, sources, tables)]
    for level in range(levels):
        for k in range(2):
            own_copy(OWN_KEPT, 0, level, 2 + k).start()
            own_copy(OWN_KEPT, 1, level, k).start()

    earlier = lefts + jnp.where(at_first, 0, 1 + sides) + jnp.where(at_last, 1 + sides, 0)

    @pl.when(earlier > 0)
    def _():
        pl.semaphore_wait(barrier, earlier)

    @pl.when(has_left)
    def _():
        tell(ready_sems.at[TO_RIGHT], ty=left)

    @pl.when(jnp.logical_not(at_first))
    def _():
        tell_row(down, ready_sems.at[TO_UP], ready_sems.at[TO_UP_SIDES])

    @pl.when(at_last)
    def _():
        tell_row(up, ready_sems.at[TO_DOWN], ready_sems.at[TO_DOWN_SIDES])

    def remote(slot, src, dst, **target):
        return pltpu.make_async_remote_copy(
            src_ref=src, dst_ref=dst, send_sem=send_sems.at[slot], recv_sem=recv_sems.at[slot],
            device_id=target, device_id_type=MESH)

    ROW, META, RIGHT_CORNERS, RIGHT_COLUMNS, LEFT_CORNERS, LEFT_COLUMNS = range(6)
    up_pieces = [
        remote(ROW, own.at[1, level, pl.ds(2, 2)], far.at[0, level], tx=up) for level in range(levels)
    ]
    down_pieces = [
        remote(ROW, own.at[0, level, pl.ds(0, 2)], far.at[1, level], tx=down) for level in range(levels)
    ]
    up_meta = remote(META, meta_out.at[1], meta_in.at[0], tx=up)
    down_meta = remote(META, meta_out.at[0], meta_in.at[1], tx=down)
    to_right = [
        remote(RIGHT_CORNERS, corner_out.at[1, 1], corner_left.at[0], tx=up, ty=right),
        remote(RIGHT_CORNERS, corner_out.at[1, 0], corner_left.at[1], tx=down, ty=right),
        remote(RIGHT_COLUMNS, pack.at[1], left_in, ty=right),
    ]
    to_left = [
        remote(LEFT_CORNERS, corner_out.at[0, 1], corner_right.at[0], tx=up, ty=left),
        remote(LEFT_CORNERS, corner_out.at[0, 0], corner_right.at[1], tx=down, ty=left),
        remote(LEFT_COLUMNS, pack.at[0], right_in, ty=left),
    ]
    both_rows = remote(ROW, far, far, tx=up)
    both_metas = remote(META, meta_in, meta_in, tx=up)
    right_corners = remote(RIGHT_CORNERS, corner_left, corner_left, tx=up)
    left_corners = remote(LEFT_CORNERS, corner_right, corner_right, tx=up)

    def start(condition, copies):
        @pl.when(condition)
        def _():
            for copy in copies:
                copy.start()

    def start_sides(edge):
        start(has_right, [to_right[1 - edge]])
        start(has_left, [to_left[1 - edge]])

    source = lax.broadcasted_iota(jnp.int32, (2 * LANES, LANES), 0) % LANES
    target = lax.broadcasted_iota(jnp.int32, (2 * LANES, LANES), 1)
    for i, offset in enumerate((-2, -1, 1, 2)):
        shifts[:, i * LANES:(i + 1) * LANES] = jnp.where(source == target + offset, 1.0, 0.0).astype(jnp.bfloat16)

    await_load(OWN_UP, own.at[1, :, pl.ds(2, 2)])
    odd_core = lax.rem(ty, 2) == 1
    even_core = jnp.logical_not(odd_core)
    start(jnp.logical_and(at_last, even_core), up_pieces)
    await_load(OWN_DOWN, own.at[0, :, pl.ds(0, 2)])
    middle = jnp.logical_not(jnp.logical_or(at_first, at_last))
    await_load(PLANES, pad.at[pl.ds(count, 3), :, pl.ds(FIRST, along), :])
    pad[wet_field, :, FIRST:FIRST + along, :] = mask_buf[...].astype(jnp.float32)
    for edge, row in enumerate((FIRST, FIRST + along - 1)):
        for i, field in enumerate((flow_field, wet_field)):
            for level in range(levels):
                meta_out[edge, i * HALF + level:i * HALF + level + 1, :] = pad[field, level, row:row + 1, :]
    start(at_last, [up_meta, down_meta])
    start(middle, [down_meta])
    start(jnp.logical_and(middle, even_core), down_pieces)
    start(jnp.logical_and(middle, odd_core), down_pieces[:1])

    lane = lax.broadcasted_iota(jnp.int32, (ROWS, LANES), 1)
    lane_group = lane // GROUP
    quarter = lane % GROUP

    upward = jnp.logical_and(others, jnp.logical_not(at_last))

    beside_root = jnp.logical_and(at_first, jnp.logical_and(lax.axis_index("member") == 0, ty == 2))
    eager = jnp.logical_and(jnp.logical_and(upward, even_core), jnp.logical_not(beside_root))

    def send_up(pieces):
        pl.semaphore_wait(ready_sems.at[TO_UP], 1)
        up_meta.start()
        for piece in pieces:
            piece.start()

    def sweep_level(level, carry):
        main(level).wait()

        @pl.when(jnp.logical_and(eager, level == min(1, levels - 1)))
        def _():
            send_up(up_pieces[:1])


        for tile in (0, tiles - 1, *range(1, tiles - 1)):
            start_row = FIRST + tile * ROWS

            def at(field, shift):
                return pad[field, level, pl.ds(start_row + shift, ROWS), :]

            wet = at(wet_field, 0)
            here = at(flow_field, 0) * at(wet_field, -1) * wet
            after = at(flow_field, 1) * wet * at(wet_field, 1)
            weights = stencil_weights(here, after)
            packed = [None] * groups
            for begin in range(0, count + 3, 8):
                batch = range(begin, min(begin + 8, count + 3))
                values = []
                for field in batch:
                    if field < count:
                        value = at(field, -2) * weights[0]
                        for shift in range(-1, 3):
                            value = value + at(field, shift) * weights[shift + 2]
                        values.append(value)
                    group, place = place_of(field)
                    turned = pltpu.roll(at(field, 0), (GROUP * place + 2) % LANES, 1)
                    if packed[group] is None:
                        packed[group] = turned
                    else:
                        packed[group] = jnp.where(lane_group == place, turned, packed[group])
                for field, value in zip(batch, values):
                    swept[field, level, tile * ROWS:(tile + 1) * ROWS, :] = value
            for group, value in enumerate(packed):
                qpad[level, group, tile * ROWS:(tile + 1) * ROWS, :] = value
        return carry

    lax.fori_loop(0, levels, sweep_level, 0)
    full_lane = lax.broadcasted_iota(jnp.int32, (along, LANES), 1)
    full_quarter = full_lane % GROUP
    for level in range(levels):
        one, two = (qpad[level, group, 0:along, :] for group in range(groups))
        for_left = jnp.where(full_quarter >= 2, one, pltpu.roll(two, LANES - 2, 1))
        for_right = jnp.where(full_quarter < 2, one, pltpu.roll(two, 2, 1))
        for side, value in enumerate((for_left, for_right)):
            pack[side, level] = value
            for edge, row in ((0, 0), (1, along - 2)):
                for r in range(2):
                    corner_out[side, edge, r * HALF + level:r * HALF + level + 1, :] = value[row + r:row + r + 1, :]
    for copy in small:
        copy.wait()
    sun.wait()

    pl.when(jnp.logical_not(at_first))(lambda: start_sides(0))
    pl.when(at_last)(lambda: start_sides(1))
    start(has_left, [to_left[2]])

    def send_up_sides():
        @pl.when(sides > 0)
        def _():
            pl.semaphore_wait(ready_sems.at[TO_UP_SIDES], sides)

        start_sides(1)

    def send_down_sides():
        @pl.when(sides > 0)
        def _():
            pl.semaphore_wait(ready_sems.at[TO_DOWN_SIDES], sides)

        start_sides(0)

    pl.when(upward)(send_up_sides)

    @pl.when(has_right)
    def _():
        pl.semaphore_wait(ready_sems.at[TO_RIGHT], 1)
        to_right[2].start()

    start(jnp.logical_and(at_last, odd_core), up_pieces)
    start(eager, up_pieces[1:])
    pl.when(jnp.logical_and(upward, jnp.logical_not(eager)))(lambda: send_up(up_pieces))

    for z in range(nzoo):
        for k in range(nphy):
            prey[z, k] = palatable[z, k].astype(jnp.float32)

    def tend_rows(field, level, row=0, size=along):
        return pl.ds(pl.multiple_of(field * stride + level * along + row, ROWS), size)

    def ecology(level, carry):
        second, third = level == min(1, levels - 1), level == levels - 1

        @pl.when(jnp.logical_and(jnp.logical_and(root, even_core), level == 0))
        def _():
            send_up(up_pieces)

        pl.when(jnp.logical_and(root, second))(send_up_sides)

        @pl.when(jnp.logical_and(jnp.logical_and(root, odd_core), second))
        def _():
            send_up(up_pieces)

        @pl.when(jnp.logical_and(root, third))
        def _():
            pl.semaphore_wait(ready_sems.at[TO_DOWN], 1)
            down_meta.start()
            for piece in down_pieces:
                piece.start()

        start(jnp.logical_and(at_last, second), down_pieces)
        start(jnp.logical_and(jnp.logical_and(middle, odd_core), level == 0), down_pieces[1:])

        @pl.when(jnp.logical_and(jnp.logical_and(at_first, others), second))
        def _():
            pl.semaphore_wait(ready_sems.at[TO_DOWN], 1)
            down_meta.start()
            down_pieces[0].start()

        @pl.when(jnp.logical_and(jnp.logical_and(at_first, others), third))
        def _():
            send_down_sides()
            for piece in down_pieces[1:]:
                piece.start()

        def field(index):
            return pad[index, level, pl.ds(FIRST, along), :]

        wet = field(wet_field)
        depth = jnp.full((along, LANES), -attenuation * (level.astype(jnp.float32) + 0.5), jnp.float32)
        light = sun_buf[...] * jnp.exp(depth)
        inverse = [1.0 / field(j) for j in range(NNUT)]
        recycled = jnp.zeros((along, LANES), jnp.float32)
        for k in range(nphy):
            phyto = field(NNUT + k)
            worst = inverse[0] * half_sat[0, k]
            for j in range(1, NNUT):
                worst = jnp.maximum(worst, inverse[j] * half_sat[j, k])
            growth = growth_max[k] * light * phyto / ((1.0 + worst) * (light + light_half[k]))
            loss = plankton_mortality * phyto
            change = growth - loss
            recycled = recycled - change
            tend[tend_rows(NNUT + k, level), :] = change
        available = [None] * nzoo
        for k in range(nphy):
            phyto = field(NNUT + k)
            for z in range(nzoo):
                term = prey[z, k] * phyto
                available[z] = term if k == 0 else available[z] + term
        rates = []
        for z in range(nzoo):
            zoo = field(NNUT + nphy + z)
            rate = graze_max[z] * zoo / (graze_half[z] + available[z])
            ingested = rate * available[z]
            loss = grazer_mortality * zoo * zoo
            tend[tend_rows(NNUT + nphy + z, level), :] = wet * (assimilation * ingested - loss)
            recycled = recycled + loss + (1.0 - assimilation) * ingested
            rates.append(rate)
        for k in range(nphy):
            eaten = prey[0, k] * rates[0]
            for z in range(1, nzoo):
                eaten = eaten + prey[z, k] * rates[z]
            rows = tend_rows(NNUT + k, level)
            tend[rows, :] = wet * (tend[rows, :] - field(NNUT + k) * eaten)
        recycled = wet * recycled
        for j in range(NNUT):
            tend[tend_rows(j, level), :] = stoichiometry[j] * recycled
        return carry

    lax.fori_loop(0, levels, ecology, 0)

    pl.when(root)(send_down_sides)

    @pl.when(jnp.logical_not(has_left))
    def _():
        left_in[...] = jnp.zeros_like(left_in)
        corner_left[...] = jnp.zeros_like(corner_left)

    @pl.when(jnp.logical_not(has_right))
    def _():
        right_in[...] = jnp.zeros_like(right_in)
        corner_right[...] = jnp.zeros_like(corner_right)

    def finish(to_right, to_left):
        @pl.when(has_right)
        def _():
            to_right.wait_send()
            to_left.wait_recv()

        @pl.when(has_left)
        def _():
            to_left.wait_send()
            to_right.wait_recv()

    finish(to_right[2], to_left[2])
    full = (along, LANES)
    full_ends = jnp.logical_or(full_lane < 2, full_lane >= LANES - 2)

    def halo_level(level):
        middle = pl.ds(FIRST, along)
        joined = []
        for group, value in enumerate(join(left_in[level], right_in[level], full_quarter)):
            qpad[level, group, middle, :] = value
            joined.append(value)
            for k in range(4):
                spot = slice(group * HALF + level, group * HALF + level + 1)
                strips[0, 2 + k, spot, :] = value[k:k + 1, :]
                strips[1, k, spot, :] = value[along - 4 + k:along - 3 + k, :]
        last = joined[groups - 1]
        qpad[level, groups, middle, :] = packed_spread(last, flow_field, full_quarter)
        qpad[level, groups + 1, middle, :] = packed_spread(last, wet_field, full_quarter)

        def q(index, shift):
            return qpad[level, index, pl.ds(FIRST + shift, along), :]

        wet = q(groups + 1, 0)
        here = q(groups, 0) * q(groups + 1, -1) * wet
        after = q(groups, 1) * wet * q(groups + 1, 1)
        weights = stencil_weights(here, after)

        wet_spot = GROUP * place_of(wet_field)[1]
        cross_spot = GROUP * place_of(cross_field)[1]
        cross, wet = pad[cross_field, level, middle, :], pad[wet_field, level, middle, :]
        first, final = full_lane == 0, full_lane == LANES - 1
        wet_below = jnp.where(first, spread(last, wet_spot + 3, full), pltpu.roll(wet, 1, 1))
        wet_above = jnp.where(final, spread(last, wet_spot, full), pltpu.roll(wet, LANES - 1, 1))
        cross_above = jnp.where(final, spread(last, cross_spot, full), pltpu.roll(cross, LANES - 1, 1))
        w = stencil_weights(cross * wet_below * wet, cross_above * wet * wet_above)
        near = jnp.where(full_quarter < 2,
                         jnp.where(full_quarter == 0, spread(w[4], LANES - 2, full), spread(w[4], LANES - 1, full)),
                         jnp.where(full_quarter == 2, spread(w[0], 0, full), spread(w[0], 1, full)))
        next_to = jnp.where(full_quarter == 1, spread(w[3], LANES - 1, full),
                            jnp.where(full_quarter == 2, spread(w[1], 0, full), 0.0))
        masked = (
            jnp.where(full_lane < 2, 0.0, w[0]),
            jnp.where(first, 0.0, w[1]),
            w[2],
            jnp.where(final, 0.0, w[3]),
            jnp.where(full_lane >= LANES - 2, 0.0, w[4]),
        )
        for i, value in enumerate(masked):
            across_buf[level, i] = value
        for edge, row in ((0, 0), (1, along - 2)):
            for r in range(2):
                for i, value in enumerate(masked):
                    across_w[edge, level, r, i:i + 1, :] = value[row + r:row + r + 1, :]
                for group in range(groups):
                    spot = slice(group * HALF + level, group * HALF + level + 1)
                    halo_w[0, edge, r, spot, :] = near[row + r:row + r + 1, :]
                    halo_w[1, edge, r, spot, :] = next_to[row + r:row + r + 1, :]
        for group in range(groups):
            total = q(group, -2) * weights[0]
            for shift in range(-1, 3):
                total = total + q(group, shift) * weights[shift + 2]
            beside = jnp.where(full_quarter == 1, pltpu.roll(total, 1, 1), pltpu.roll(total, LANES - 1, 1))
            halo_term[level, group] = near * total + next_to * beside

    for level in range(levels):
        halo_level(level)

    def across_level(level, carry):
        w = [across_buf[level, i] for i in range(5)]
        terms = [halo_term[level, group] for group in range(groups)]
        for begin in range(0, count, BATCH):
            batch = range(begin, min(begin + BATCH, count))
            block = jnp.concatenate([swept[field, level] for field in batch], axis=0)
            coarse = block.astype(jnp.bfloat16)
            rest = (block - coarse.astype(jnp.float32)).astype(jnp.bfloat16)
            near = jnp.dot(jnp.concatenate([coarse, rest], axis=1), shifts[...], preferred_element_type=jnp.float32)
            for i, field in enumerate(batch):
                group, place = place_of(field)
                part = near[i * along:(i + 1) * along]
                total = tend[tend_rows(field, level), :] + block[i * along:(i + 1) * along] * w[2]
                for k, weight in enumerate((w[0], w[1], w[3], w[4])):
                    total = total + part[:, k * LANES:(k + 1) * LANES] * weight
                term = pltpu.roll(terms[group], (LANES - 2 - GROUP * place) % LANES, 1)
                result[field, level] = total + jnp.where(full_ends, term, 0.0)
        return carry

    lax.fori_loop(0, levels, across_level, 0)

    await_load(OWN_KEPT, far)
    both_metas.wait()
    for level in range(levels):
        pad[wet_field, level, FIRST - 1:FIRST, :] = meta_in[0, HALF + level:HALF + level + 1, :]
        for i, index in enumerate((flow_field, wet_field)):
            pad[index, level, FIRST + along:FIRST + along + 1, :] = meta_in[1, i * HALF + level:i * HALF + level + 1, :]
    for level in range(levels):
        for edge, tile, row in ((0, 0, 0), (1, tiles - 1, ROWS - 2)):
            start = FIRST + tile * ROWS

            def at(index, shift):
                return pad[index, level, start + shift:start + shift + ROWS, :]

            wet = at(wet_field, 0)
            weights = stencil_weights(at(flow_field, 0) * at(wet_field, -1) * wet,
                                      at(flow_field, 1) * wet * at(wet_field, 1))
            for r in range(2):
                for i, value in enumerate(weights):
                    along_w[edge, level, r, i:i + 1, :] = value[row + r:row + r + 1, :]

    finish(right_corners, left_corners)
    ends = jnp.logical_or(lane < 2, lane >= LANES - 2)
    upper = lax.broadcasted_iota(jnp.int32, (ROWS, LANES), 0) >= HALF

    def both(value):
        return jnp.where(upper, value, pltpu.roll(value, HALF, 0))

    terms = {}
    for edge in range(2):
        strip = [strips[edge, k] for k in range(6)]
        first, second = join(corner_left[edge], corner_right[edge], quarter)
        strip[4 * edge] = jnp.where(upper, pltpu.roll(second, HALF, 0), first)
        strip[4 * edge + 1] = jnp.where(upper, second, pltpu.roll(first, HALF, 0))
        wets = {k: both(packed_spread(strip[k], wet_field, quarter)) for k in range(1, 5)}
        flows = {k: both(packed_spread(strip[k], flow_field, quarter)) for k in range(2, 5)}
        faces = {k: flows[k] * wets[k - 1] * wets[k] for k in range(2, 5)}
        for r in range(2):
            weights = stencil_weights(faces[r + 2], faces[r + 3])
            total = strip[r] * weights[0]
            for shift in range(1, 5):
                total = total + strip[r + shift] * weights[shift]
            beside = jnp.where(quarter == 1, pltpu.roll(total, 1, 1), pltpu.roll(total, LANES - 1, 1))
            terms[edge, r] = halo_w[0, edge, r] * total + halo_w[1, edge, r] * beside

    for edge in range(2):
        for level in range(levels):
            for r in range(2):
                row = r if edge == 0 else along - 2 + r
                for begin in range(0, count, ROWS):
                    group, inside = divmod(begin, PER)
                    spot = group * HALF + level
                    line = jnp.broadcast_to(terms[edge, r][spot:spot + 1, :], (ROWS, LANES))
                    line = pltpu.roll(line, 2 + GROUP * inside, 1, stride=GROUP, stride_axis=0)
                    rows = pl.ds(begin * stride + level * along + row, ROWS, stride=stride)
                    base[edge, level, r, begin:begin + ROWS, :] = tend[rows, :] + jnp.where(ends, line, 0.0)

    both_rows.wait()


def across_kernel(dims, result, own, far, base, along_w, across_w, updated, rows_out, sems):
    count, levels, along = dims
    inner = pl.ds(2, along - 4)
    whole = pltpu.make_async_copy(result.at[:, :, inner, :], updated.at[:, :, inner, :], sems.at[0])
    whole.start()

    for edge in range(2):
        for level in range(levels):
            near = [own[edge, level, k] for k in range(4)]
            beyond = [far[edge, level, k] for k in range(2)]
            lines = beyond + near if edge == 0 else near + beyond
            for r in range(2):
                row = r if edge == 0 else along - 2 + r
                along_lines, across_lines = along_w[edge, level, r], across_w[edge, level, r]
                value = lines[r] * along_lines[0:1, :]
                for shift in range(1, 5):
                    value = value + lines[r + shift] * along_lines[shift:shift + 1, :]
                total = base[edge, level, r] + value * across_lines[2:3, :]
                total = total + pltpu.roll(value, 2, 1) * across_lines[0:1, :]
                total = total + pltpu.roll(value, 1, 1) * across_lines[1:2, :]
                total = total + pltpu.roll(value, LANES - 1, 1) * across_lines[3:4, :]
                total = total + pltpu.roll(value, LANES - 2, 1) * across_lines[4:5, :]
                rows_out[edge, level, r] = total
                pltpu.make_async_copy(
                    rows_out.at[edge, level, r], updated.at[:, level, row, :], sems.at[1]).start()
    whole.wait()
    pltpu.make_async_copy(rows_out, rows_out, sems.at[1]).wait()


def shards(
    tracers,
    velocity,
    land_mask,
    sunlight,
    growth_max,
    half_sat,
    light_half,
    graze_max,
    graze_half,
    palatable,
    stoichiometry,
):
    count, levels, along, across = tracers.shape
    nphy, nzoo = growth_max.shape[0], graze_max.shape[0]
    groups = -(-(count + 3) // PER)
    assert across == LANES and along % ROWS == 0 and along >= 2 * ROWS
    assert count % ROWS == 0 and groups == 2 and (count + 2) % PER >= 2 and levels <= HALF
    f32 = jnp.float32
    any_space = pl.BlockSpec(memory_space=pl.ANY)
    hbm = pl.BlockSpec(memory_space=pltpu.HBM)
    vmem = pl.BlockSpec(memory_space=pltpu.VMEM)
    small = (growth_max, half_sat, light_half, graze_max, graze_half, palatable, stoichiometry)
    stride = levels * along + ROWS
    line = (ROWS, LANES)
    columns = (levels, along, LANES)
    outputs = [
        (count, levels, along, LANES),
        (2, levels, 4, count, LANES),
        (2, levels, 2, count, LANES),
        (2, levels, 2, count, LANES),
        (2, levels, 2) + line,
        (2, levels, 2) + line,
    ]
    prepared = pl.pallas_call(
        functools.partial(exchange_kernel, (count, levels, along, nphy, nzoo, stride)),
        out_shape=tuple(jax.ShapeDtypeStruct(shape, f32) for shape in outputs),
        in_specs=[hbm] * 11,
        out_specs=(vmem,) * len(outputs),
        scratch_shapes=[pltpu.SMEM(x.shape, x.dtype) for x in small] + [
            pltpu.VMEM((count + 3, levels, FIRST + along + ROWS, LANES), f32),
            pltpu.VMEM(land_mask.shape, jnp.int32),
            pltpu.VMEM(sunlight.shape, f32),
            pltpu.VMEM((count, levels, along, LANES), f32),
            pltpu.VMEM((count * stride, LANES), f32),
            pltpu.VMEM((2, 6) + line, f32),
            pltpu.VMEM((2,) + line, f32),
            pltpu.VMEM((2,) + line, f32),
            pltpu.VMEM((2, 2, 2) + line, f32),
            pltpu.VMEM((2,) + columns, f32),
            pltpu.VMEM(columns, f32),
            pltpu.VMEM(columns, f32),
            pltpu.VMEM((levels, groups + 2, FIRST + along + ROWS, LANES), f32),
            pltpu.VMEM((levels, groups, along, LANES), f32),
            pltpu.VMEM((levels, 5, along, LANES), f32),
            pltpu.VMEM((2, 2) + line, f32),
            pltpu.VMEM((2 * LANES, 4 * LANES), jnp.bfloat16),
            pltpu.VMEM((2,) + line, f32),
            pltpu.VMEM((2,) + line, f32),
            pltpu.SMEM(palatable.shape, f32),
            pltpu.SemaphoreType.DMA((8,)),
            pltpu.SemaphoreType.DMA((levels,)),
            pltpu.SemaphoreType.DMA((6,)),
            pltpu.SemaphoreType.DMA((6,)),
            pltpu.SemaphoreType.REGULAR((5,)),
        ],
        compiler_params=pltpu.CompilerParams(
            collective_id=0, has_side_effects=True, vmem_limit_bytes=32 * 2**20
        ),
        name="exchange",
    )(*[
        pltpu.with_memory_space_constraint(x, pltpu.HBM)
        for x in (tracers, velocity, land_mask, sunlight) + small
    ])
    return pl.pallas_call(
        functools.partial(across_kernel, (count, levels, along)),
        out_shape=jax.ShapeDtypeStruct(tracers.shape, f32),
        in_specs=[vmem] * len(outputs),
        out_specs=any_space,
        scratch_shapes=[
            pltpu.VMEM((2, levels, 2, count, LANES), f32),
            pltpu.SemaphoreType.DMA((2,)),
        ],
        compiler_params=pltpu.CompilerParams(vmem_limit_bytes=24 * 2**20),
        name="across",
    )(*prepared)


def solution(mesh):
    return jax.shard_map(
        shards,
        mesh=mesh,
        in_specs=(
            P("member", None, "tx", "ty"),
            P(None, None, "tx", "ty"),
            P(None, "tx", "ty"),
            P("tx", "ty"),
            P("member"),
            P("member", None),
            P("member"),
            P("member"),
            P("member"),
            P("member", None),
            P(),
        ),
        out_specs=P("member", None, "tx", "ty"),
        check_vma=False,
    )
```
